16 devices in a mesh: data: 2 (over y, z), expert: 8 (over x, core).
Axes of the slice: x: 4, y: 2, z: 1, core: 2. Of those that a mesh axis runs over, the one named last changes fastest.
The devices are a block of a 4x4x8 slice.
Arguments:
- tok_x: bfloat16 [12288, 4096], P(('data', 'expert')), parts along dimension 0
- route_idx: int32 [12288, 2], P(('data', 'expert')), parts along dimension 0
- route_gate: float32 [12288, 2], P(('data', 'expert')), parts along dimension 0
- grad_y: bfloat16 [12288, 4096], P(('data', 'expert')), parts along dimension 0
- w_gate: bfloat16 [8, 4096, 1024], P('expert')
- w_up: bfloat16 [8, 4096, 1024], P('expert')
- w_down: bfloat16 [8, 1024, 4096], P('expert')
Outputs:
- output 1: bfloat16 [12288, 4096], P(('data', 'expert')), parts along dimension 0
- output 2: bfloat16 [12288, 4096], P(('data', 'expert')), parts along dimension 0
- output 3: float32 [16, 4096, 1024], P(('data', 'expert')), parts along dimension 0
- output 4: float32 [16, 4096, 1024], P(('data', 'expert')), parts along dimension 0
- output 5: float32 [16, 1024, 4096], P(('data', 'expert')), parts along dimension 0
There are 2 independent parts. The reference program is written for one: setup_inputs(seed, part) draws one part's arguments, and reference() takes and returns one part's arrays. A program takes and returns all parts, laid end to end along the dimension named above; an argument that names none is the same for every part.
All inputs are finite; a program needn't handle non-finite values.
Results may differ from the reference program's by a relative error of at most 0.00366429.
Values are sent between devices in bfloat16 or wider.
A program may use at most 768 MiB of HBM per device.

```python
import jax
import jax.numpy as jnp
from jax import lax

GROUP_SIZE = 8
TOKENS = 768
MODEL_DIM = 4096
FFN_DIM = 1024
EXPERTS = 8
TOP_K = 2

HOT_COUNT = min(4, EXPERTS // 8)
HOT_STRIDE = EXPERTS // HOT_COUNT
COLD_COUNT = EXPERTS - HOT_COUNT
CAPACITY = max(4, 2 * TOKENS * TOP_K // EXPERTS)
FILL_ROWS = CAPACITY + 4
PART_ROWS = GROUP_SIZE * TOKENS
SLOT_COUNT = TOKENS * TOP_K


def draw_routing(route_key):
    key_list = jax.random.split(route_key, 5)
    row_ids = jnp.arange(PART_ROWS)
    slot_ids = jnp.arange(TOP_K)
    cold_first = jax.random.randint(key_list[0], (PART_ROWS,), 0, COLD_COUNT)
    cold_second = jax.random.randint(key_list[1], (PART_ROWS,), 0, 2 * COLD_COUNT)
    forced = jax.random.randint(key_list[2], (GROUP_SIZE,), 0, COLD_COUNT)
    is_fill = (row_ids % TOKENS) < FILL_ROWS
    cold_base = jnp.where(is_fill, (forced[row_ids // TOKENS] - (TOP_K - 1)) % COLD_COUNT, jnp.minimum(cold_first, cold_second))
    cold_rank = (cold_base[:, None] + slot_ids[None, :]) % COLD_COUNT
    cold_ids = (cold_rank // (HOT_STRIDE - 1)) * HOT_STRIDE + 1 + cold_rank % (HOT_STRIDE - 1)
    hot_roll = jax.random.randint(key_list[3], (PART_ROWS, TOP_K), 0, 10)
    hot_base = jax.random.randint(key_list[4], (PART_ROWS,), 0, HOT_COUNT)
    hot_ids = ((hot_base[:, None] + slot_ids[None, :]) % HOT_COUNT) * HOT_STRIDE
    use_hot = (hot_roll < 6) & (slot_ids[None, :] < min(HOT_COUNT, TOP_K)) & jnp.logical_not(is_fill)[:, None]
    return jnp.where(use_hot, hot_ids, cold_ids).astype(jnp.int32)


def setup_inputs(seed: int = 0, part: int = 0) -> dict:
    root_key = jax.random.key(seed)
    part_key = jax.random.fold_in(root_key, part)
    tok_keys = jax.random.split(part_key, 4)
    weight_keys = jax.random.split(root_key, 3)
    tok_x = jax.random.normal(tok_keys[0], (PART_ROWS, MODEL_DIM), jnp.float32).astype(jnp.bfloat16)
    route_idx = draw_routing(tok_keys[1])
    route_gate = jax.random.uniform(tok_keys[2], (PART_ROWS, TOP_K), jnp.float32, 0.2, 1.0)
    grad_y = jax.random.normal(tok_keys[3], (PART_ROWS, MODEL_DIM), jnp.float32).astype(jnp.bfloat16)
    in_scale = MODEL_DIM ** -0.5
    w_gate = (jax.random.normal(weight_keys[0], (EXPERTS, MODEL_DIM, FFN_DIM), jnp.float32) * in_scale).astype(jnp.bfloat16)
    w_up = (jax.random.normal(weight_keys[1], (EXPERTS, MODEL_DIM, FFN_DIM), jnp.float32) * in_scale).astype(jnp.bfloat16)
    w_down = (jax.random.normal(weight_keys[2], (EXPERTS, FFN_DIM, MODEL_DIM), jnp.float32) * FFN_DIM ** -0.5).astype(jnp.bfloat16)
    return {'tok_x': tok_x, 'route_idx': route_idx, 'route_gate': route_gate, 'grad_y': grad_y, 'w_gate': w_gate, 'w_up': w_up, 'w_down': w_down}


def silu_parts(pre_act):
    sigmoid_a = jax.nn.sigmoid(pre_act)
    return pre_act * sigmoid_a, sigmoid_a * (1.0 + pre_act * (1.0 - sigmoid_a))


def expert_rows(rows_x, row_gate, rows_dy, w_in, w_lin, w_out):
    pre_a = jnp.dot(rows_x, w_in, preferred_element_type=jnp.float32).astype(jnp.bfloat16)
    pre_b = jnp.dot(rows_x, w_lin, preferred_element_type=jnp.float32).astype(jnp.bfloat16)
    silu_a, silu_slope = silu_parts(pre_a.astype(jnp.float32))
    lin_b = pre_b.astype(jnp.float32)
    hidden = (silu_a * lin_b).astype(jnp.bfloat16)
    out_rows = jnp.dot(hidden, w_out, preferred_element_type=jnp.float32).astype(jnp.bfloat16)
    grad_out = (row_gate[:, None] * rows_dy.astype(jnp.float32)).astype(jnp.bfloat16)
    grad_h = jnp.dot(grad_out, w_out.T, preferred_element_type=jnp.float32).astype(jnp.bfloat16).astype(jnp.float32)
    grad_a = (grad_h * lin_b * silu_slope).astype(jnp.bfloat16)
    grad_b = (grad_h * silu_a).astype(jnp.bfloat16)
    grad_in = (jnp.dot(grad_a, w_in.T, preferred_element_type=jnp.float32) + jnp.dot(grad_b, w_lin.T, preferred_element_type=jnp.float32)).astype(jnp.bfloat16)
    grad_w_in = jnp.dot(rows_x.T, grad_a, preferred_element_type=jnp.float32)
    grad_w_lin = jnp.dot(rows_x.T, grad_b, preferred_element_type=jnp.float32)
    grad_w_out = jnp.dot(hidden.T, grad_out, preferred_element_type=jnp.float32)
    return out_rows, grad_in, grad_w_in, grad_w_lin, grad_w_out


def route_device(dev_idx):
    flat_ids = dev_idx.reshape(SLOT_COUNT)
    onehot = (flat_ids[:, None] == jnp.arange(EXPERTS, dtype=jnp.int32)[None, :]).astype(jnp.int32)
    position = jnp.sum(jnp.cumsum(onehot, axis=0) * onehot, axis=1) - 1
    is_kept = (flat_ids % HOT_STRIDE != 0) & (position < CAPACITY)
    dest_row = jnp.where(is_kept, flat_ids * CAPACITY + position, EXPERTS * CAPACITY)
    slot_src = jnp.full((EXPERTS * CAPACITY + 1,), SLOT_COUNT, jnp.int32).at[dest_row].set(jnp.arange(SLOT_COUNT, dtype=jnp.int32))
    return dest_row, slot_src[:EXPERTS * CAPACITY]


def take_rows(row_table, row_ids):
    return row_table[row_ids]


def reference(tok_x, route_idx, route_gate, grad_y, w_gate, w_up, w_down):
    dest_row, slot_src = jax.vmap(route_device)(route_idx.reshape(GROUP_SIZE, TOKENS, TOP_K))
    tok_src = slot_src // TOP_K
    zero_rows = jnp.zeros((GROUP_SIZE, 1, MODEL_DIM), jnp.bfloat16)
    x_pad = jnp.concatenate([tok_x.reshape(GROUP_SIZE, TOKENS, MODEL_DIM), zero_rows], axis=1)
    dy_pad = jnp.concatenate([grad_y.reshape(GROUP_SIZE, TOKENS, MODEL_DIM), zero_rows], axis=1)
    gate_pad = jnp.concatenate([route_gate.reshape(GROUP_SIZE, SLOT_COUNT), jnp.zeros((GROUP_SIZE, 1), jnp.float32)], axis=1)
    buf_x = jax.vmap(take_rows)(x_pad, tok_src).reshape(GROUP_SIZE, EXPERTS, CAPACITY, MODEL_DIM)
    buf_dy = jax.vmap(take_rows)(dy_pad, tok_src).reshape(GROUP_SIZE, EXPERTS, CAPACITY, MODEL_DIM)
    buf_gate = jax.vmap(take_rows)(gate_pad, slot_src).reshape(GROUP_SIZE, EXPERTS, CAPACITY)
    ex_x = jnp.swapaxes(buf_x, 0, 1).reshape(EXPERTS, GROUP_SIZE * CAPACITY, MODEL_DIM)
    ex_dy = jnp.swapaxes(buf_dy, 0, 1).reshape(EXPERTS, GROUP_SIZE * CAPACITY, MODEL_DIM)
    ex_gate = jnp.swapaxes(buf_gate, 0, 1).reshape(EXPERTS, GROUP_SIZE * CAPACITY)
    cold_out, cold_dx, cold_dwg, cold_dwu, cold_dwd = lax.map(lambda operands: expert_rows(*operands), (ex_x, ex_gate, ex_dy, w_gate, w_up, w_down))
    back_out = jnp.swapaxes(cold_out.reshape(EXPERTS, GROUP_SIZE, CAPACITY, MODEL_DIM), 0, 1).reshape(GROUP_SIZE, EXPERTS * CAPACITY, MODEL_DIM)
    back_dx = jnp.swapaxes(cold_dx.reshape(EXPERTS, GROUP_SIZE, CAPACITY, MODEL_DIM), 0, 1).reshape(GROUP_SIZE, EXPERTS * CAPACITY, MODEL_DIM)
    out_slots = jax.vmap(take_rows)(jnp.concatenate([back_out, zero_rows], axis=1), dest_row).reshape(PART_ROWS, TOP_K, MODEL_DIM)
    dx_slots = jax.vmap(take_rows)(jnp.concatenate([back_dx, zero_rows], axis=1), dest_row).reshape(PART_ROWS, TOP_K, MODEL_DIM)
    hot_ids = jnp.arange(HOT_COUNT, dtype=jnp.int32) * HOT_STRIDE
    hot_gate = jnp.sum(jnp.where(route_idx[:, :, None] == hot_ids[None, None, :], route_gate[:, :, None], 0.0), axis=1)
    hot_out, hot_dx, hot_dwg, hot_dwu, hot_dwd = lax.map(lambda operands: expert_rows(tok_x, operands[0], grad_y, operands[1], operands[2], operands[3]), (hot_gate.T, w_gate[::HOT_STRIDE], w_up[::HOT_STRIDE], w_down[::HOT_STRIDE]))
    out_y = jnp.sum(route_gate[:, :, None] * out_slots.astype(jnp.float32), axis=1) + jnp.sum(hot_gate.T[:, :, None] * hot_out.astype(jnp.float32), axis=0)
    grad_x = jnp.sum(dx_slots.astype(jnp.float32), axis=1) + jnp.sum(hot_dx.astype(jnp.float32), axis=0)
    grad_w_gate = cold_dwg.at[::HOT_STRIDE].add(hot_dwg)
    grad_w_up = cold_dwu.at[::HOT_STRIDE].add(hot_dwu)
    grad_w_down = cold_dwd.at[::HOT_STRIDE].add(hot_dwd)
    return (out_y.astype(jnp.bfloat16), grad_x.astype(jnp.bfloat16), grad_w_gate, grad_w_up, grad_w_down)
```

```python
import jax
import jax.numpy as jnp
from jax import lax
from jax.sharding import PartitionSpec as P

BF = jnp.bfloat16
F32 = jnp.float32


def dot(form, a, b):
    return jnp.einsum(form, a, b, preferred_element_type=F32)


def expert_rows(x, dy, gate, w1, w3, w2):
    pre_a = dot('cd,df->cf', x, w1).astype(BF)
    pre_b = dot('cd,df->cf', x, w3).astype(BF)
    a = pre_a.astype(F32)
    b = pre_b.astype(F32)
    sig = jax.nn.sigmoid(a)
    silu = a * sig
    slope = sig * (1.0 + a * (1.0 - sig))
    hid = (silu * b).astype(BF)
    out = dot('cf,fd->cd', hid, w2).astype(BF)
    live = (gate > 0.0)[:, None]
    g = (gate[:, None] * dy.astype(F32)).astype(BF)
    dh = dot('cd,fd->cf', g, w2).astype(BF).astype(F32)
    da = jnp.where(live, dh * b * slope, 0.0).astype(BF)
    db = jnp.where(live, dh * silu, 0.0).astype(BF)
    hid = jnp.where(live, hid, jnp.zeros_like(hid))
    dx = (dot('cf,df->cd', da, w1) + dot('cf,df->cd', db, w3)).astype(BF)
    dw1 = dot('cd,cf->df', x, da)
    dw3 = dot('cd,cf->df', x, db)
    dw2 = dot('cf,cd->fd', hid, g)
    return out, dx, dw1, dw3, dw2


def solution(mesh):
    group = mesh.shape['expert']
    tok_spec = P(('data', 'expert'))
    w_spec = P('expert')

    def body(tok_x, route_idx, route_gate, grad_y, w_gate, w_up, w_down):
        toks, dim = tok_x.shape
        tops = route_idx.shape[1]
        slots = toks * tops
        local = w_gate.shape[0]
        experts = local * group
        stride = experts // min(4, experts // 8)
        cap = max(4, 2 * slots // experts)
        w1, w3, w2 = w_gate[0], w_up[0], w_down[0]

        flat = route_idx.reshape(slots)
        onehot = (flat[:, None] == jnp.arange(experts, dtype=jnp.int32)[None, :]).astype(jnp.int32)
        pos = jnp.sum(jnp.cumsum(onehot, axis=0) * onehot, axis=1) - 1
        is_hot = flat % stride == 0
        slot_ids = jnp.arange(slots, dtype=jnp.int32)
        flat_gate = route_gate.reshape(slots)

        def tables(first):
            kept = (pos >= first) & (pos < first + cap)
            if first:
                kept = kept & is_hot
            dest = jnp.where(kept, flat * cap + pos - first, experts * cap)
            src = jnp.full((experts * cap + 1,), slots, jnp.int32).at[dest].set(slot_ids)[:experts * cap]
            live = src < slots
            src = jnp.where(live, src, 0)
            gate = jnp.where(live, flat_gate[src], 0.0)
            row = (src // tops).astype(F32)
            table = jnp.stack([row.reshape(experts, cap), gate.reshape(experts, cap)], axis=1)
            table = lax.all_to_all(table, 'expert', 0, 0)
            base = jnp.arange(group, dtype=jnp.int32)[:, None] * toks
            rows = (table[:, 0].astype(jnp.int32) + base).reshape(group * cap)
            return kept, jnp.where(kept, dest, 0), rows, table[:, 1].reshape(group * cap)

        def slot_sum(back, kept, dest, weight):
            rows = back.reshape(group * cap, dim)[dest].astype(F32)
            if weight is not None:
                rows = rows * weight[:, None]
            rows = jnp.where(kept[:, None], rows, 0.0).reshape(toks, tops, dim)
            return jnp.sum(rows, axis=1)

        all_x = lax.all_gather(tok_x, 'expert', tiled=True)
        all_dy = lax.all_gather(grad_y, 'expert', tiled=True)

        def run_pass(first):
            kept, dest, rows, gate = tables(first)
            out, dx, dw1, dw3, dw2 = expert_rows(all_x[rows], all_dy[rows], gate, w1, w3, w2)
            back_out = lax.all_to_all(out.reshape(group, cap, dim), 'expert', 0, 0)
            back_dx = lax.all_to_all(dx.reshape(group, cap, dim), 'expert', 0, 0)
            y = slot_sum(back_out, kept, dest, flat_gate)
            gx = slot_sum(back_dx, kept, dest, None)
            return y, gx, dw1, dw3, dw2

        first = run_pass(0)
        hot_most = jnp.max(jnp.where(is_hot, pos, 0))
        spill = lax.pmax(hot_most, ('data', 'expert')) >= cap
        y, gx, dw1, dw3, dw2 = first
        res = lax.cond(
            spill,
            lambda f: tuple(u + v for u, v in zip(f, run_pass(cap))),
            lambda f: f, first)
        y, gx, dw1, dw3, dw2 = res
        return y.astype(BF), gx.astype(BF), dw1[None], dw3[None], dw2[None]

    return jax.shard_map(body, mesh=mesh, in_specs=(tok_spec,) * 4 + (w_spec,) * 3, out_specs=(tok_spec,) * 5, check_vma=False)
```

```python
import jax
import jax.numpy as jnp
from jax import lax
from jax.sharding import PartitionSpec as P

BF = jnp.bfloat16
F32 = jnp.float32


def dot(form, a, b):
    return jnp.einsum(form, a, b, preferred_element_type=F32)


def count_before(mask):
    n = mask.shape[0]
    earlier = lax.broadcasted_iota(jnp.int32, (n, n), 1) < lax.broadcasted_iota(jnp.int32, (n, n), 0)
    return dot('ts,sc->tc', earlier.astype(BF), mask.astype(BF)).astype(jnp.int32)


def solution(mesh):
    group = mesh.shape['expert']
    tok_spec = P(('data', 'expert'))
    w_spec = P('expert')

    def body(tok_x, route_idx, route_gate, grad_y, w_gate, w_up, w_down):
        toks, dim = tok_x.shape
        tops = route_idx.shape[1]
        experts = w_gate.shape[0] * group
        stride = experts // min(4, experts // 8)
        cap = max(4, 2 * toks * tops // experts)
        rows = group * cap
        half = dim // 2
        me = lax.axis_index('expert')
        w1, w3, w2 = w_gate[0], w_up[0], w_down[0]

        route = jnp.concatenate([route_idx.astype(F32), route_gate], axis=1)
        all_route = lax.all_gather(route, 'expert')
        all_idx = all_route[:, :, :tops].astype(jnp.int32)
        all_gate = all_route[:, :, tops:]

        hit = all_idx == me
        mine = jnp.any(hit, axis=2)
        rank_in = count_before(mine.T).T
        gate_in = jnp.sum(jnp.where(hit, all_gate, 0.0), axis=2)
        taken = jnp.any(route_idx[:, :, None] == jnp.arange(experts, dtype=jnp.int32), axis=1)
        rank_all = count_before(taken)
        slot_hit = route_idx[:, :, None] == jnp.arange(experts, dtype=jnp.int32)
        rank_out = jnp.sum(jnp.where(slot_hit, rank_all[:, None, :], 0), axis=2)
        hot_out = route_idx % stride == 0
        spill = lax.pmax(jnp.max(jnp.where(hot_out, rank_out, 0)), ('data', 'expert')) >= cap

        def pick_in(first):
            ok = mine & (rank_in >= first) & (rank_in < first + cap)
            if first:
                ok = ok & (me % stride == 0)
            want = jnp.where(ok, rank_in - first, -1)
            onehot = want[:, None, :] == lax.broadcasted_iota(jnp.int32, (1, cap, 1), 1)
            gate = jnp.sum(jnp.where(onehot, gate_in[:, None, :], 0.0), axis=2)
            return onehot.astype(BF), gate.reshape(rows, 1)

        def pick_out(first):
            ok = (rank_out >= first) & (rank_out < first + cap)
            if first:
                ok = ok & hot_out
            want = jnp.where(ok, route_idx * cap + rank_out - first, -1)
            return (want.T[:, :, None] == lax.broadcasted_iota(jnp.int32, (1, 1, rows), 2)).astype(BF)

        def take(onehot, tok):
            return dot('gcs,gsd->gcd', onehot, tok).astype(BF).reshape(rows, dim)

        def forward(onehot, all_x):
            x = take(onehot, all_x)
            pre_a = dot('cd,df->cf', x, w1).astype(BF)
            pre_b = dot('cd,df->cf', x, w3).astype(BF)
            a = pre_a.astype(F32)
            hid = (a * jax.nn.sigmoid(a) * pre_b.astype(F32)).astype(BF)
            out = dot('cf,fd->cd', hid, w2).astype(BF)
            return x, pre_a, pre_b, hid, out

        def backward(onehot, gate, all_dy, pre_a, pre_b):
            dy = take(onehot, all_dy)
            g = (gate * dy.astype(F32)).astype(BF)
            dh = dot('cd,fd->cf', g, w2).astype(BF).astype(F32)
            a = pre_a.astype(F32)
            sig = jax.nn.sigmoid(a)
            da = (dh * pre_b.astype(F32) * (sig * (1.0 + a * (1.0 - sig)))).astype(BF)
            db = (dh * (a * sig)).astype(BF)
            return g, da, db

        def input_grad(da, db, lo):
            return (dot('cf,df->cd', da, w1[lo:lo + half]) + dot('cf,df->cd', db, w3[lo:lo + half])).astype(BF)

        def swap(r):
            return lax.all_to_all(r.reshape(group, cap, r.shape[1]), 'expert', 0, 0).reshape(rows, r.shape[1])

        def weight_grads(x, hid, g, da, db):
            return dot('cd,cf->df', x, da), dot('cd,cf->df', x, db), dot('cf,cd->fd', hid, g)

        def gated(onehot, back):
            slots = dot('jtr,rd->jtd', onehot, back).astype(BF).astype(F32)
            return jnp.sum(route_gate.T[:, :, None] * slots, axis=0)

        def summed(onehot, back):
            return dot('tr,rd->td', jnp.sum(onehot, axis=0), back)

        def after(value, *others):
            return lax.optimization_barrier((value,) + others)[0]

        all_x = lax.all_gather(tok_x, 'expert')
        all_dy = lax.all_gather(grad_y, 'expert')
        onehot_in, gate = pick_in(0)
        onehot_out = pick_out(0)
        all_x, spill, onehot_in, gate = lax.optimization_barrier((all_x, spill, onehot_in, gate))

        x, pre_a, pre_b, hid, out = forward(onehot_in, all_x)
        pre_a, pre_b, hid = lax.optimization_barrier((pre_a, pre_b, hid))
        back_out = swap(out)
        g, da, db = backward(onehot_in, gate, after(all_dy, out), pre_a, pre_b)
        g, da, db = lax.optimization_barrier((g, da, db))
        dx = [input_grad(da, db, lo) for lo in (0, half)]
        back_dx = []
        for d in dx:
            back_dx.append(swap(after(d, back_out, *back_dx)))
        y = gated(after(onehot_out, *dx), back_out)
        dw = weight_grads(x, hid, g, *lax.optimization_barrier((da, db) + tuple(dx))[:2])
        gx = [summed(onehot_out, b).astype(BF) for b in back_dx]
        done = (y.astype(BF), jnp.concatenate(gx, axis=1)) + dw

        def more(done):
            onehot_in, gate = pick_in(cap)
            onehot_late = pick_out(cap)
            x, pre_a, pre_b, hid, out = forward(onehot_in, all_x)
            g, da, db = backward(onehot_in, gate, all_dy, pre_a, pre_b)
            y2 = y + gated(onehot_late, swap(out))
            gx2 = [summed(onehot_out, b) + summed(onehot_late, swap(input_grad(da, db, lo))) for b, lo in zip(back_dx, (0, half))]
            dw2 = weight_grads(x, hid, g, da, db)
            return (y2.astype(BF), jnp.concatenate(gx2, axis=1).astype(BF)) + tuple(u + v for u, v in zip(dw, dw2))

        y, gx, dw1, dw3, dw2 = lax.cond(spill, more, lambda done: done, done)
        return y, gx, dw1[None], dw3[None], dw2[None]

    return jax.shard_map(body, mesh=mesh, in_specs=(tok_spec,) * 4 + (w_spec,) * 3, out_specs=(tok_spec,) * 5, check_vma=False)
```

```python
import functools

import jax
import jax.numpy as jnp
from jax import lax
from jax.experimental import pallas as pl
from jax.experimental.layout import Layout, with_layout_constraint
from jax.experimental.pallas import tpu as pltpu
from jax.sharding import PartitionSpec as P

BF = jnp.bfloat16
F32 = jnp.float32
I32 = jnp.int32
PIECE = 16
TILE = 128
WINDOW = 144
SPAN = 256
VMEM_LIMIT = 50 * 2 ** 20


def dot(form, a, b):
    return jnp.einsum(form, a, b, preferred_element_type=F32)


def iota(shape, axis):
    return lax.broadcasted_iota(I32, shape, axis)


def count_before(mask):
    n = mask.shape[-1]
    earlier = iota((n, n), 0) < iota((n, n), 1)
    return dot('...u,us->...s', mask.astype(BF), earlier.astype(BF)).astype(I32)


def pick(table, index):
    sel = iota(table.shape, 0) == index
    return jnp.sum(jnp.where(sel, table, jnp.zeros_like(table)), axis=0)


def row_major(v):
    return with_layout_constraint(v, Layout(major_to_minor=tuple(range(v.ndim))))


def after(value, *others):
    return lax.optimization_barrier((value,) + others)[0]


def pack_kernel(scaled, dev_ref, seg_ref, low_ref, tab0, tab1, info, *refs):
    outs, (buf, pend, sem) = (refs[4:6], refs[6:8]), refs[8:]
    g = pl.program_id(0)
    toks = info.shape[2]
    length, start, extra, stage = [seg_ref[g, k] for k in range(4)]

    @pl.when(g == 0)
    def _():
        pend[0] = 0
        pend[1] = 0

    def drain(slot):
        def one(_, carry):
            pltpu.make_async_copy(buf.at[0, pl.ds(0, PIECE)], outs[0][0].at[pl.ds(0, PIECE)], sem.at[slot]).wait()
            return carry

        lax.fori_loop(0, pend[slot], one, 0)
        pend[slot] = 0

    def put(slot, p, side, at):
        for late, ref in enumerate(outs[side]):
            @pl.when((at >= stage) == bool(late))
            def _(ref=ref, late=late):
                spot = jnp.minimum(at - stage if late else at, ref.shape[0] - PIECE)
                src = buf.at[slot, pl.ds(pl.multiple_of(p * PIECE, PIECE), PIECE)]
                pltpu.make_async_copy(src, ref.at[pl.ds(pl.multiple_of(spot, PIECE), PIECE)], sem.at[slot]).start()
        pend[slot] = pend[slot] + 1

    def tile(i, carry):
        @pl.when(i * TILE < length)
        def _():
            slot = lax.rem(i, 2)
            drain(slot)
            vals = info[0]
            match = vals[0:1, :] == (iota((TILE, toks), 0) + i * TILE).astype(F32)

            def column(k, off):
                return jnp.sum(jnp.where(match, vals[k:k + 1, :] + off, 0.0), axis=1, keepdims=True)

            lows = [low_ref[g, 2 * i + k] for k in range(2)]

            def part(k, tab):
                at = column(1 + k, 1.0) - (lows[k] + 1).astype(F32)
                onehot = (at == iota((TILE, SPAN), 1).astype(F32)).astype(BF)
                got = jnp.dot(onehot, tab[0, pl.ds(pl.multiple_of(lows[k], PIECE), SPAN)], preferred_element_type=F32)
                return got * column(3 + k, 0.0) if scaled else got

            @pl.when((lows[0] >= 0) & (lows[1] < 0))
            def _():
                buf[slot] = part(0, tab0).astype(BF)

            @pl.when((lows[0] < 0) & (lows[1] >= 0))
            def _():
                buf[slot] = part(1, tab1).astype(BF)

            @pl.when((lows[0] >= 0) & (lows[1] >= 0))
            def _():
                buf[slot] = (part(0, tab0) + part(1, tab1)).astype(BF)

            def piece(p, carry):
                q = i * TILE + p * PIECE
                at = start + q
                near = jnp.where(at >= stage, at + extra, at)

                @pl.when((q < length) & (g < 2) & (at < extra))
                def _():
                    put(slot, p, 0, at)

                @pl.when((q < length) & (g < 2) & (at >= extra))
                def _():
                    put(slot, p, 1, at - extra)

                @pl.when((q < length) & (g >= 2) & (g < 4))
                def _():
                    put(slot, p, 0, near)

                @pl.when((q < length) & (g >= 4))
                def _():
                    put(slot, p, 1, near)

                return carry

            lax.fori_loop(0, TILE // PIECE, piece, 0)

        return carry

    lax.fori_loop(0, toks // TILE, tile, 0)

    @pl.when(g == pl.num_programs(0) - 1)
    def _():
        drain(0)
        drain(1)


def arrive_kernel(scaled, second, home_ref, win_ref, tab0, tab1, info, up1, up2, down1, down2, out, acc, wbuf, sem):
    t, last = pl.program_id(0), pl.num_programs(0) - 1
    windows = (up1, up2, up2, down1, down2, down2)

    def copies(step, do):
        slot = lax.rem(step, 2)
        for w, ref in enumerate(windows):
            begin = win_ref[step, w]

            @pl.when(begin >= 0)
            def _(ref=ref, w=w, begin=begin):
                src = ref.at[pl.ds(pl.multiple_of(jnp.maximum(begin, 0), PIECE), WINDOW)]
                do(pltpu.make_async_copy(src, wbuf.at[slot, w, pl.ds(0, WINDOW)], sem.at[slot, w]))

    @pl.when(t == 0)
    def _():
        wbuf[:, :, WINDOW:] = jnp.zeros((2, len(windows), SPAN - WINDOW, wbuf.shape[3]), BF)
        copies(0, lambda c: c.start())

    @pl.when(t < last)
    def _():
        copies(t + 1, lambda c: c.start())

    vals = info[0]
    eye = iota((TILE, TILE), 0) == iota((TILE, TILE), 1)

    def column(k):
        return jnp.sum(jnp.where(eye, vals[k:k + 1, :], 0.0), axis=1, keepdims=True)

    def add(begin, base, spot, weight, rows):
        @pl.when(begin >= 0)
        def _():
            at = column(spot) - (begin + base).astype(F32)
            onehot = (at == iota((TILE, SPAN), 1).astype(F32)).astype(BF)
            part = jnp.dot(onehot, rows(), preferred_element_type=F32)
            acc[...] = acc[...] + (part * column(weight) if scaled else part)

    acc[...] = jnp.zeros_like(acc)
    for k, tab in enumerate((tab0, tab1)):
        low = win_ref[t, len(windows) + k]
        add(low, 0, k, 2 + k, lambda tab=tab, low=low: tab[0, pl.ds(pl.multiple_of(low, PIECE), SPAN)])
    copies(t, lambda c: c.wait())
    slot = lax.rem(t, 2)
    for w, (spot, weight, base) in enumerate(((4, 8, 0), (4, 8, second), (6, 10, 0), (5, 9, 0), (5, 9, second), (7, 10, 0))):
        add(win_ref[t, w], base, spot, weight, lambda w=w: wbuf[slot, w])
    out[0] = acc[...].astype(BF)


def by_count(count, cap, run):
    for n in range(0, cap + 1, TILE):
        @pl.when((count > n - TILE) & (count <= n))
        def _(n=n):
            run(n)


def inner_kernel(count_ref, info, dy, w2t, a_ref, b_ref, g_ref, da_ref, db_ref):
    cap, dim = g_ref.shape[1:]
    step = dim // 4

    def run(n):
        if n:
            vals = info[0]
            match = vals[0:1, :] == iota((n, vals.shape[1]), 0).astype(F32)
            gate = jnp.sum(jnp.where(match, vals[1:2, :], 0.0), axis=1, keepdims=True)
            onehot = match.astype(BF)
            for c in range(0, dim, step):
                got = jnp.dot(onehot, dy[0, :, c:c + step], preferred_element_type=F32)
                g_ref[0, :n, c:c + step] = (gate * got).astype(BF)
            dh = jnp.dot(g_ref[0, :n], w2t[...], preferred_element_type=F32).astype(BF).astype(F32)
            a, b = a_ref[0, :n].astype(F32), b_ref[0, :n].astype(F32)
            sig = jax.nn.sigmoid(a)
            da_ref[0, :n] = (dh * b * (sig * (1.0 + a * (1.0 - sig)))).astype(BF)
            db_ref[0, :n] = (dh * (a * sig)).astype(BF)
        if n < cap:
            for ref in (g_ref, da_ref, db_ref):
                ref[0, n:] = jnp.zeros((cap - n, ref.shape[2]), BF)

    by_count(count_ref[pl.program_id(0)], cap, run)


def input_kernel(count_ref, da, db, w1t, w3t, out):
    cap, width = out.shape[1:]
    step = width // 2

    def run(n):
        if n:
            for c in range(0, width, step):
                got = jnp.dot(da[0, :n], w1t[:, c:c + step], preferred_element_type=F32)
                got = got + jnp.dot(db[0, :n], w3t[:, c:c + step], preferred_element_type=F32)
                out[0, :n, c:c + step] = got.astype(BF)
        if n < cap:
            out[0, n:] = jnp.zeros((cap - n, width), BF)

    by_count(count_ref[pl.program_id(0)], cap, run)


def solution(mesh):
    group = mesh.shape['expert']
    chips = group // 2
    tok_spec = P(('data', 'expert'))
    w_spec = P('expert')
    to_mate = [(i, i ^ 1) for i in range(group)]
    to_next = [(i, (i + 2) % group) for i in range(group)]
    to_prev = [(i, (i - 2) % group) for i in range(group)]

    def layer(tok_x, route_idx, route_gate, grad_y, w_gate, w_up, w_down):
        toks, dim = tok_x.shape
        tops = route_idx.shape[1]
        experts = w_gate.shape[0] * group
        stride = experts // min(4, experts // 8)
        cap = max(4, 2 * toks * tops // experts)
        rows = group * cap
        half = dim // 2
        tiles = toks // TILE
        small = toks * 13 // 12 // PIECE * PIECE
        stage = toks * 71 // 48 // PIECE * PIECE
        place = 2 * stage
        me = lax.axis_index('expert')
        chip, core = me // 2, me % 2
        up, down, far = (chip + 1) % chips, (chip + chips - 1) % chips, (chip + 2) % chips
        w1, w3, w2 = w_gate[0], w_up[0], w_down[0]

        def mate(v):
            return lax.ppermute(v, 'expert', to_mate)

        all_x = lax.all_gather(tok_x, 'expert')
        all_dy = lax.all_gather(grad_y, 'expert')

        route = jnp.concatenate([route_idx.astype(F32).T, route_gate.T], axis=0)
        every = lax.all_gather(route, 'expert').swapaxes(0, 1)
        idx, gates = every[:tops].astype(I32), every[tops:]
        expert_id = iota((experts, 1, 1), 0)
        taken = jnp.any(idx[None] == expert_id[:, None], axis=1)
        rank = count_before(taken)
        hot_id = expert_id % stride == 0
        kept = taken & (hot_id | (rank < cap))
        spot = jnp.where(kept, rank, -1)
        need = jnp.any(kept.reshape(chips, 2, group, toks), axis=1)
        single = jnp.sum(need.astype(I32), axis=0) == 1
        listed = jnp.where(need, count_before(need), -1)
        sizes = (jnp.sum(need.astype(I32), axis=2) + PIECE - 1) // PIECE * PIECE
        total = jnp.sum(sizes.reshape(chips, chips, 2), axis=2)

        def turn(table, by):
            return jnp.roll(table, -by, axis=-1)

        def hop(by):
            sel = (iota((chips, chips), 0) + by) % chips == iota((chips, chips), 1)
            return jnp.sum(jnp.where(sel, total, 0), axis=1)

        tries = 5 ** chips
        share = (iota((tries, chips), 0) // (5 ** iota((tries, chips), 1))) % 5
        go_up = hop(2)[None] * share // (4 * PIECE) * PIECE
        go_down = hop(2)[None] - go_up
        on_up = hop(1)[None] + go_up + turn(go_up, -1)
        on_down = hop(chips - 1)[None] + go_down + turn(go_down, 1)
        two_hop = jnp.max(jnp.maximum(go_up, go_down), axis=1)
        load = jnp.max(jnp.maximum(on_up, on_down), axis=1) + jnp.where(two_hop > small, 2 * place, 0)
        best = jnp.min(load)
        first_best = jnp.min(jnp.where(load == best, jnp.arange(tries, dtype=I32), tries))
        chosen = jnp.sum(jnp.where(iota((tries, 1), 0) == first_best, go_up, 0), axis=0)
        other = hop(2) - chosen
        full = jnp.any(taken & hot_id & (rank >= cap)) | (best > place)
        state = jnp.where(full, 2, jnp.where(best > 2 * small, 1, 0))
        state = lax.pmax(state.astype(I32), ('data', 'expert'))

        def gate_of(eid):
            return jnp.sum(jnp.where(idx == eid, gates, 0.0), axis=0)

        own_spot, mate_spot = pick(spot, me), pick(spot, me ^ 1)
        own_gate, mate_gate = gate_of(me), gate_of(me ^ 1)
        pad = jnp.zeros((group, toks), F32)
        send_info = jnp.stack([pick(listed, chip).astype(F32), own_spot.astype(F32), mate_spot.astype(F32),
                               jnp.where(single, own_gate, 1.0), jnp.where(single, mate_gate, 1.0), pad, pad, pad], axis=1)
        f_up, f_down = pick(chosen, chip), pick(other, chip)
        pass_up, pass_down = pick(chosen, down), pick(other, up)
        my_sizes = pick(sizes, chip)
        devs = jnp.stack([2 * to + k for to in (far, up, down) for k in range(2)])

        def lowest(at, ok):
            low = jnp.min(jnp.where(ok & (at >= 0), at, cap), axis=-1)
            return jnp.where(low < cap, jnp.minimum(low // PIECE * PIECE, cap - SPAN), -1)

        list_tile = (pick(listed, chip) // TILE)[None] == iota((tiles, 1, 1), 0)
        list_tile = list_tile & (pick(listed, chip) >= 0)[None]
        lows = jnp.stack([lowest(v[None], list_tile) for v in (own_spot, mate_spot)], axis=2)
        lows = lows.swapaxes(0, 1).reshape(group, 2 * tiles)
        low_rows = jnp.concatenate([lax.dynamic_slice_in_dim(lows, 2 * to, 2, 0) for to in (far, up, down)])

        def segments(size_of_stage):
            segs = []
            for to, lead, extra in ((far, 0, f_up), (up, f_up, pass_up), (down, f_down, pass_down)):
                for k in range(2):
                    size = pick(my_sizes, 2 * to + k)
                    segs.append(jnp.stack([size, jnp.asarray(lead, I32), extra, jnp.asarray(size_of_stage, I32)]))
                    lead = lead + size
            return jnp.stack(segs)

        tier_stage = jnp.where(state == 0, small, stage)
        segs = segments(tier_stage)

        def home(v):
            return lax.dynamic_slice_in_dim(v, 2 * chip, 2, 0)

        home_idx = [home(idx[j]) for j in range(tops)]
        home_gates = [home(gates[j]) for j in range(tops)]
        home_kept = home(jnp.sum(kept.astype(I32) * (1 << expert_id), axis=0))
        home_single = home(single.astype(I32)) > 0

        def listed_at(c):
            at = home(pick(listed, c))
            first = pick(pick(sizes, c), 2 * chip)
            return at >= 0, at + jnp.where(iota((2, 1), 0) == 1, first, 0)

        def weight_of(c):
            w = 0.0
            for j in range(tops):
                held = (home_kept >> home_idx[j]) % 2 == 1
                w = w + jnp.where((home_idx[j] // 2 == c) & held, home_gates[j], 0.0)
            return jnp.where(home_single, 1.0, w)

        far_ok, far_at = listed_at(far)
        far_cut = pick(chosen, far)
        far_by_up = jnp.where(far_ok & (far_at < far_cut), far_at, -1)
        far_by_down = jnp.where(far_ok & (far_at >= far_cut), far_at - far_cut, -1)
        home_spots = [home(own_spot), home(mate_spot)]
        weights = [weight_of(c) for c in (down, up, far)]
        own_lows = [lowest(v.reshape(2 * tiles, TILE), True) for v in home_spots]

        def arrival(size_of_stage):
            def near_spot(c, lead, passed):
                ok, at = listed_at(c)
                at = at + lead
                return jnp.where(ok, jnp.where(at >= size_of_stage, stage + at + passed - size_of_stage, at), -1)

            from_down = near_spot(down, pick(chosen, down), pick(chosen, far))
            from_up = near_spot(up, pick(other, up), pick(other, far))
            info = [v.astype(F32) for v in home_spots] + [home(own_gate), home(mate_gate)]
            info += [v.astype(F32) for v in (from_down, from_up, far_by_up, far_by_down)] + weights
            info = jnp.stack(info + [jnp.zeros((2, toks), F32)] * 5, axis=1)
            begins = []
            for near, by in ((from_down, far_by_up), (from_up, far_by_down)):
                begins.append(jnp.where((near >= 0) & (near < stage), near, place))
                begins.append(jnp.where(near >= stage, near - stage, place))
                begins.append(jnp.where(by >= 0, by, place))
            low = jnp.min(jnp.stack(begins).reshape(6, 2 * tiles, TILE), axis=2)
            low = jnp.where(low < place, jnp.minimum(low // PIECE * PIECE, size_of_stage - WINDOW), -1)
            return info, jnp.concatenate([low, jnp.stack(own_lows)]).T

        home_info, win = arrival(tier_stage)
        homes = jnp.stack([2 * chip, 2 * chip + 1])

        onehot_in = (own_spot[:, None, :] == iota((1, cap, 1), 1)).astype(BF)

        def columns(w, axis, mine):
            parts = jnp.split(w, 2, axis=axis)
            return jnp.where((core == 0) == mine, parts[0], parts[1])

        w2_halves = [columns(w2, 1, m) for m in (True, False)]
        w2t = row_major(w2.T)
        w13t_halves = [[row_major(columns(w, 0, m).T) for w in (w1, w3)] for m in (True, False)]
        counts = jnp.sum((own_spot >= 0).astype(I32), axis=1)
        pad = jnp.zeros((group, toks), F32)
        own_info = jnp.stack([own_spot.astype(F32), own_gate] + [pad] * 6, axis=1)
        rooms = [jnp.full((stage, half), jnp.where(state > 3 + k, 1.0, 0.0), BF) for k in range(8)]
        plan = (state, send_info, devs, segs, low_rows, home_info, win, homes, onehot_in, counts, own_info, w2_halves, w2t, w13t_halves, rooms)
        plan = lax.optimization_barrier(plan)
        all_x, plan = lax.optimization_barrier((all_x, plan))
        (state, send_info, devs, segs, low_rows, home_info, win, homes, onehot_in, counts, own_info, w2_halves, w2t, w13t_halves,
         rooms) = plan

        def take(onehot, tok, gate=None):
            got = dot('gcs,gsd->gcd', onehot, tok)
            return (got if gate is None else gate.reshape(group, cap, 1) * got).astype(BF).reshape(rows, dim)

        def up_front(x):
            pre_a = dot('cd,df->cf', x, w1).astype(BF)
            pre_b = dot('cd,df->cf', x, w3).astype(BF)
            pre_a, pre_b = lax.optimization_barrier((pre_a, pre_b))
            a = pre_a.astype(F32)
            hid = (a * jax.nn.sigmoid(a) * pre_b.astype(F32)).astype(BF)
            return pre_a, pre_b, hid

        def inner_grads(pre_a, pre_b, dh):
            dh = dh.astype(BF).astype(F32)
            a = pre_a.astype(F32)
            sig = jax.nn.sigmoid(a)
            da = (dh * pre_b.astype(F32) * (sig * (1.0 + a * (1.0 - sig)))).astype(BF)
            db = (dh * (a * sig)).astype(BF)
            return da, db

        any_spec = pl.BlockSpec(memory_space=pl.ANY)

        def packed(tables, segs, rooms, scaled):
            table_spec = pl.BlockSpec((1, cap, half), lambda g, dev, seg, low: (dev[g], 0, 0))
            res = pl.pallas_call(
                functools.partial(pack_kernel, scaled),
                grid_spec=pltpu.PrefetchScalarGridSpec(
                    num_scalar_prefetch=3, grid=(6,),
                    in_specs=[table_spec, table_spec, pl.BlockSpec((1, 8, toks), lambda g, dev, seg, low: (dev[g], 0, 0))] + [any_spec] * 4,
                    out_specs=[any_spec] * 4,
                    scratch_shapes=[pltpu.VMEM((2, TILE, half), BF), pltpu.SMEM((2,), I32),
                                    pltpu.SemaphoreType.DMA((2,))]),
                out_shape=[jax.ShapeDtypeStruct((stage, half), BF)] * 4,
                input_output_aliases={6 + k: k for k in range(4)},
                compiler_params=pltpu.CompilerParams(vmem_limit_bytes=VMEM_LIMIT),
                cost_estimate=pl.CostEstimate(flops=2 * rows * cap * half, bytes_accessed=12 * rows * half, transcendentals=0),
                name='pack',
            )(devs, segs, low_rows, *tables, send_info, *rooms)
            return res[:2], res[2:]

        def arrived(tables, info, win, got_up, got_down, scaled):
            table_spec = pl.BlockSpec((1, cap, half), lambda t, homes, win: (homes[t // tiles], 0, 0))
            info_spec = pl.BlockSpec((1, 16, TILE), lambda t, homes, win: (t // tiles, 0, t % tiles))
            return pl.pallas_call(
                functools.partial(arrive_kernel, scaled, stage),
                grid_spec=pltpu.PrefetchScalarGridSpec(
                    num_scalar_prefetch=2, grid=(2 * tiles,),
                    in_specs=[table_spec, table_spec, info_spec] + [any_spec] * 4,
                    out_specs=pl.BlockSpec((1, TILE, half), lambda t, homes, win: (t // tiles, t % tiles, 0)),
                    scratch_shapes=[pltpu.VMEM((TILE, half), F32), pltpu.VMEM((2, 6, SPAN, half), BF), pltpu.SemaphoreType.DMA((2, 6))]),
                out_shape=jax.ShapeDtypeStruct((2, toks, half), BF),
                compiler_params=pltpu.CompilerParams(vmem_limit_bytes=VMEM_LIMIT),
                cost_estimate=pl.CostEstimate(flops=2 * rows * cap * half, bytes_accessed=12 * rows * half, transcendentals=0),
                name='arrive',
            )(homes, win, *tables, info, *got_up, *got_down)

        def shift(up_rows, down_rows):
            got_up = lax.ppermute(up_rows, 'expert', to_next)
            got_down = lax.ppermute(down_rows, 'expert', to_prev)
            return got_up, got_down

        def second_rows(got, up_rows, down_rows):
            row = iota((up_rows.shape[0], 1), 0)
            return jnp.where(row < pass_up, got[0], up_rows), jnp.where(row < pass_down, got[1], down_rows)

        def whole(total):
            mine = jnp.where(core == 0, total[0], total[1])
            theirs = mate(jnp.where(core == 0, total[1], total[0]))
            return jnp.where(core == 0, jnp.concatenate([mine, theirs], axis=1), jnp.concatenate([theirs, mine], axis=1))

        def table(v):
            return v.reshape(group, cap, half)

        x = take(onehot_in, all_x)
        pre_a, pre_b, hid = up_front(x)
        theirs = dot('cf,fd->cd', hid, w2_halves[1]).astype(BF)
        out_got = mate(theirs)
        ours = dot('cf,fd->cd', after(hid, theirs), w2_halves[0]).astype(BF)
        out_tables = (table(ours), table(out_got))
        out_up, out_down = packed(out_tables, segs, rooms[:4], True)
        all_dy = after(all_dy, out_up, out_down)

        def block_spec(rows, width):
            return pl.BlockSpec((1, rows, width), lambda e, count: (e, 0, 0))

        def fixed_spec(w):
            return pl.BlockSpec(w.shape, lambda e, count: (0, 0), pipeline_mode=pl.Buffered(1))

        def inner_grads_of(dy):
            f = pre_a.shape[1]
            return pl.pallas_call(
                inner_kernel,
                grid_spec=pltpu.PrefetchScalarGridSpec(
                    num_scalar_prefetch=1, grid=(group,),
                    in_specs=[block_spec(8, toks), block_spec(toks, dim), fixed_spec(w2t), block_spec(cap, f), block_spec(cap, f)],
                    out_specs=[block_spec(cap, dim), block_spec(cap, f), block_spec(cap, f)]),
                out_shape=[jax.ShapeDtypeStruct((group, cap, n), BF) for n in (dim, f, f)],
                compiler_params=pltpu.CompilerParams(vmem_limit_bytes=VMEM_LIMIT),
                cost_estimate=pl.CostEstimate(flops=2 * rows * dim * (toks + f), bytes_accessed=2 * rows * dim * 4, transcendentals=rows * f),
                name='inner',
            )(counts, own_info, dy, w2t, pre_a.reshape(group, cap, f), pre_b.reshape(group, cap, f))

        def input_grad(da, db, k):
            w1t, w3t = w13t_halves[k]
            f = da.shape[2]
            return pl.pallas_call(
                input_kernel,
                grid_spec=pltpu.PrefetchScalarGridSpec(
                    num_scalar_prefetch=1, grid=(group,),
                    in_specs=[block_spec(cap, f), block_spec(cap, f), fixed_spec(w1t), fixed_spec(w3t)],
                    out_specs=block_spec(cap, half)),
                out_shape=jax.ShapeDtypeStruct((group, cap, half), BF),
                compiler_params=pltpu.CompilerParams(vmem_limit_bytes=VMEM_LIMIT),
                cost_estimate=pl.CostEstimate(flops=4 * rows * f * half, bytes_accessed=4 * rows * half, transcendentals=0),
                name='input_grad',
            )(counts, da, db, w1t, w3t)

        def rest(size):
            out_first = shift(out_up[0][:size], out_down[0][:size])
            g, da, db = inner_grads_of(all_dy)
            out_second = second_rows(after(out_first, da), out_up[1][:size], out_down[1][:size])
            out_last = shift(*out_second)
            da, db = after((da, db), *out_second)
            theirs = input_grad(da, db, 1)
            dx_got = mate(theirs)
            ours = input_grad(after(da, theirs), db, 0)
            dx_tables = (ours, dx_got)
            dx_up, dx_down = packed(dx_tables, segs, rooms[4:], False)
            dx_first = shift(dx_up[0][:size], dx_down[0][:size])
            out_first, out_last, da, db, g = after((out_first, out_last, da, db, g), dx_up, dx_down)
            f = da.shape[2]
            da, db, g = da.reshape(rows, f), db.reshape(rows, f), g.reshape(rows, dim)
            dw1 = dot('cd,cf->df', x, da)
            out_first, out_last = after((out_first, out_last), dw1[:8, :TILE])
            y = arrived(out_tables, home_info, win, (out_first[0], out_last[0]), (out_first[1], out_last[1]), True)
            y = whole(y)
            dx_second = second_rows(after(dx_first, y), dx_up[1][:size], dx_down[1][:size])
            dx_last = shift(*dx_second)
            db, hid_late = after((db, hid), *dx_second)
            dw3 = dot('cd,cf->df', x, db)
            dw2 = dot('cf,cd->fd', hid_late, g)
            gx = whole(arrived(dx_tables, home_info, win, (dx_first[0], dx_last[0]), (dx_first[1], dx_last[1]), False))
            return y, gx, row_major(dw1)[None], row_major(dw3)[None], row_major(dw2)[None]

        def general():
            my_rank, my_taken = pick(rank, me), pick(taken.astype(I32), me) > 0
            my_idx = route_idx.T
            home_rank = pick(jnp.moveaxis(rank, 1, 0), me)
            out_rank = jnp.stack([jnp.sum(jnp.where(my_idx[j] == expert_id[:, 0], home_rank, 0), axis=0) for j in range(tops)])
            out_hot = my_idx % stride == 0

            def one_pass(first):
                ok = my_taken & (my_rank >= first) & (my_rank < first + cap)
                ok_out = (out_rank >= first) & (out_rank < first + cap)
                if first:
                    ok = ok & (me % stride == 0)
                    ok_out = ok_out & out_hot
                onehot = jnp.where(ok, my_rank - first, -1)[:, None, :] == iota((1, cap, 1), 1)
                gate = jnp.sum(jnp.where(onehot, own_gate[:, None, :], 0.0), axis=2)
                onehot = onehot.astype(BF)
                goal = jnp.where(ok_out, my_idx * cap + out_rank - first, -1)
                onehot_out = (goal[:, :, None] == iota((1, 1, rows), 2)).astype(BF)

                def swap(r):
                    return lax.all_to_all(r.reshape(group, cap, dim), 'expert', 0, 0).reshape(rows, dim)

                x = take(onehot, all_x)
                pre_a, pre_b, hid = up_front(x)
                back = swap(dot('cf,fd->cd', hid, w2).astype(BF))
                g = lax.optimization_barrier(take(onehot, all_dy, gate))
                da, db = lax.optimization_barrier(inner_grads(pre_a, pre_b, dot('cd,fd->cf', g, w2)))
                dx = (dot('cf,df->cd', da, w1) + dot('cf,df->cd', db, w3)).astype(BF)
                back_dx = swap(after(dx, back))
                slots = dot('jtr,rd->jtd', onehot_out, back)
                y = jnp.sum(route_gate.T[:, :, None] * slots, axis=0)
                gx = dot('tr,rd->td', jnp.sum(onehot_out, axis=0), back_dx)
                return y, gx, dot('cd,cf->df', x, da), dot('cd,cf->df', x, db), dot('cf,cd->fd', hid, g)

            first = one_pass(0)
            second = one_pass(cap)
            sums = [u + v for u, v in zip(first, second)]
            return (sums[0].astype(BF), sums[1].astype(BF)) + tuple(v[None] for v in sums[2:])

        return lax.switch(state, [lambda: rest(small), lambda: rest(stage), general])

    return jax.shard_map(layer, mesh=mesh, in_specs=(tok_spec,) * 4 + (w_spec,) * 3, out_specs=(tok_spec,) * 5, check_vma=False)
```

```python
import functools

import jax
import jax.numpy as jnp
from jax import lax
from jax.experimental import pallas as pl
from jax.experimental.layout import Layout, with_layout_constraint
from jax.experimental.pallas import tpu as pltpu
from jax.sharding import PartitionSpec as P

BF = jnp.bfloat16
F32 = jnp.float32
I32 = jnp.int32
PIECE = 16
TILE = 128
WINDOW = 144
SPAN = 256
VMEM_LIMIT = 50 * 2 ** 20


def dot(form, a, b):
    return jnp.einsum(form, a, b, preferred_element_type=F32)


def iota(shape, axis):
    return lax.broadcasted_iota(I32, shape, axis)


def count_before(mask):
    n = mask.shape[-1]
    earlier = iota((n, n), 0) < iota((n, n), 1)
    return dot('...u,us->...s', mask.astype(BF), earlier.astype(BF)).astype(I32)


def pick(table, index):
    sel = iota(table.shape, 0) == index
    return jnp.sum(jnp.where(sel, table, jnp.zeros_like(table)), axis=0)


def row_major(v):
    return with_layout_constraint(v, Layout(major_to_minor=tuple(range(v.ndim))))


def after(value, *others):
    return lax.optimization_barrier((value,) + others)[0]


def pack_kernel(scaled, dev_ref, seg_ref, low_ref, tab0, tab1, info, *refs):
    outs, (buf, pend, sem) = (refs[0:2], refs[2:4]), refs[4:]
    g = pl.program_id(0)
    toks = info.shape[2]
    length, start, extra, stage = [seg_ref[g, k] for k in range(4)]

    @pl.when(g == 0)
    def _():
        pend[0] = 0
        pend[1] = 0

    def drain(slot):
        def one(_, carry):
            pltpu.make_async_copy(buf.at[0, pl.ds(0, PIECE)], outs[0][0].at[pl.ds(0, PIECE)], sem.at[slot]).wait()
            return carry

        lax.fori_loop(0, pend[slot], one, 0)
        pend[slot] = 0

    def put(slot, p, side, at):
        for late, ref in enumerate(outs[side]):
            @pl.when((at >= stage) == bool(late))
            def _(ref=ref, late=late):
                spot = jnp.minimum(at - stage if late else at, ref.shape[0] - PIECE)
                src = buf.at[slot, pl.ds(pl.multiple_of(p * PIECE, PIECE), PIECE)]
                pltpu.make_async_copy(src, ref.at[pl.ds(pl.multiple_of(spot, PIECE), PIECE)], sem.at[slot]).start()
        pend[slot] = pend[slot] + 1

    def tile(i, carry):
        @pl.when(i * TILE < length)
        def _():
            slot = lax.rem(i, 2)
            drain(slot)
            vals = info[0]
            match = vals[0:1, :] == (iota((TILE, toks), 0) + i * TILE).astype(F32)

            def column(k, off):
                return jnp.sum(jnp.where(match, vals[k:k + 1, :] + off, 0.0), axis=1, keepdims=True)

            lows = [low_ref[g, 2 * i + k] for k in range(2)]

            def part(k, tab):
                at = column(1 + k, 1.0) - (lows[k] + 1).astype(F32)
                onehot = (at == iota((TILE, SPAN), 1).astype(F32)).astype(BF)
                got = jnp.dot(onehot, tab[0, pl.ds(pl.multiple_of(lows[k], PIECE), SPAN)], preferred_element_type=F32)
                return got * column(3 + k, 0.0) if scaled else got

            @pl.when((lows[0] >= 0) & (lows[1] < 0))
            def _():
                buf[slot] = part(0, tab0).astype(BF)

            @pl.when((lows[0] < 0) & (lows[1] >= 0))
            def _():
                buf[slot] = part(1, tab1).astype(BF)

            @pl.when((lows[0] >= 0) & (lows[1] >= 0))
            def _():
                buf[slot] = (part(0, tab0) + part(1, tab1)).astype(BF)

            def piece(p, carry):
                q = i * TILE + p * PIECE
                at = start + q
                near = jnp.where(at >= stage, at + extra, at)

                @pl.when((q < length) & (g < 2) & (at < extra))
                def _():
                    put(slot, p, 0, at)

                @pl.when((q < length) & (g < 2) & (at >= extra))
                def _():
                    put(slot, p, 1, at - extra)

                @pl.when((q < length) & (g >= 2) & (g < 4))
                def _():
                    put(slot, p, 0, near)

                @pl.when((q < length) & (g >= 4))
                def _():
                    put(slot, p, 1, near)

                return carry

            lax.fori_loop(0, TILE // PIECE, piece, 0)

        return carry

    lax.fori_loop(0, toks // TILE, tile, 0)

    @pl.when(g == pl.num_programs(0) - 1)
    def _():
        drain(0)
        drain(1)


def arrive_kernel(scaled, second, home_ref, win_ref, tab0, tab1, info, up1, up2, down1, down2, out, acc, wbuf, sem):
    t, last = pl.program_id(0), pl.num_programs(0) - 1
    windows = (up1, up2, up2, down1, down2, down2)

    def copies(step, do):
        slot = lax.rem(step, 2)
        for w, ref in enumerate(windows):
            begin = win_ref[step, w]

            @pl.when(begin >= 0)
            def _(ref=ref, w=w, begin=begin):
                src = ref.at[pl.ds(pl.multiple_of(jnp.maximum(begin, 0), PIECE), WINDOW)]
                do(pltpu.make_async_copy(src, wbuf.at[slot, w, pl.ds(0, WINDOW)], sem.at[slot, w]))

    @pl.when(t == 0)
    def _():
        wbuf[:, :, WINDOW:] = jnp.zeros((2, len(windows), SPAN - WINDOW, wbuf.shape[3]), BF)
        copies(0, lambda c: c.start())

    @pl.when(t < last)
    def _():
        copies(t + 1, lambda c: c.start())

    vals = info[0]
    eye = iota((TILE, TILE), 0) == iota((TILE, TILE), 1)

    def column(k):
        return jnp.sum(jnp.where(eye, vals[k:k + 1, :], 0.0), axis=1, keepdims=True)

    def add(begin, base, spot, weight, rows):
        @pl.when(begin >= 0)
        def _():
            at = column(spot) - (begin + base).astype(F32)
            onehot = (at == iota((TILE, SPAN), 1).astype(F32)).astype(BF)
            part = jnp.dot(onehot, rows(), preferred_element_type=F32)
            acc[...] = acc[...] + (part * column(weight) if scaled else part)

    acc[...] = jnp.zeros_like(acc)
    count = len(windows)
    for k, tab in enumerate((tab0, tab1)):
        low = win_ref[t, count + k]
        add(low, 0, k, 2 + k, lambda tab=tab, low=low: tab[0, pl.ds(pl.multiple_of(low, PIECE), SPAN)])
    copies(t, lambda c: c.wait())
    slot = lax.rem(t, 2)

    def arrived_rows(w):
        used = (win_ref[t, count + 2 + w] - win_ref[t, w] + PIECE - 1) // PIECE

        def clear(p, carry):
            wbuf[slot, w, pl.ds(pl.multiple_of(p * PIECE, PIECE), PIECE)] = jnp.zeros((PIECE, wbuf.shape[3]), BF)
            return carry

        lax.fori_loop(used, WINDOW // PIECE, clear, 0)
        return wbuf[slot, w]

    for w, (spot, weight, base) in enumerate(((4, 8, 0), (4, 8, second), (6, 10, 0), (5, 9, 0), (5, 9, second), (7, 10, 0))):
        add(win_ref[t, w], base, spot, weight, lambda w=w: arrived_rows(w))
    out[0] = acc[...].astype(BF)


def by_count(count, cap, run):
    for n in range(0, cap + 1, TILE):
        @pl.when((count > n - TILE) & (count <= n))
        def _(n=n):
            run(n)


def inner_kernel(count_ref, info, dy, w2t, a_ref, b_ref, g_ref, da_ref, db_ref):
    cap, dim = g_ref.shape[1:]
    step = dim // 4

    def run(n):
        if n:
            vals = info[0]
            match = vals[0:1, :] == iota((n, vals.shape[1]), 0).astype(F32)
            gate = jnp.sum(jnp.where(match, vals[1:2, :], 0.0), axis=1, keepdims=True)
            onehot = match.astype(BF)
            for c in range(0, dim, step):
                got = jnp.dot(onehot, dy[0, :, c:c + step], preferred_element_type=F32)
                g_ref[0, :n, c:c + step] = (gate * got).astype(BF)
            dh = jnp.dot(g_ref[0, :n], w2t[...], preferred_element_type=F32).astype(BF).astype(F32)
            a, b = a_ref[0, :n].astype(F32), b_ref[0, :n].astype(F32)
            sig = jax.nn.sigmoid(a)
            da_ref[0, :n] = (dh * b * (sig * (1.0 + a * (1.0 - sig)))).astype(BF)
            db_ref[0, :n] = (dh * (a * sig)).astype(BF)
        if n < cap:
            for ref in (g_ref, da_ref, db_ref):
                ref[0, n:] = jnp.zeros((cap - n, ref.shape[2]), BF)

    by_count(count_ref[pl.program_id(0)], cap, run)


def input_kernel(count_ref, da, db, w1t, w3t, out):
    cap, width = out.shape[1:]
    step = width // 2

    def run(n):
        if n:
            for c in range(0, width, step):
                got = jnp.dot(da[0, :n], w1t[:, c:c + step], preferred_element_type=F32)
                got = got + jnp.dot(db[0, :n], w3t[:, c:c + step], preferred_element_type=F32)
                out[0, :n, c:c + step] = got.astype(BF)
        if n < cap:
            out[0, n:] = jnp.zeros((cap - n, width), BF)

    by_count(count_ref[pl.program_id(0)], cap, run)


def solution(mesh):
    group = mesh.shape['expert']
    chips = group // 2
    tok_spec = P(('data', 'expert'))
    w_spec = P('expert')
    to_mate = [(i, i ^ 1) for i in range(group)]
    to_next = [(i, (i + 2) % group) for i in range(group)]
    to_prev = [(i, (i - 2) % group) for i in range(group)]

    def layer(tok_x, route_idx, route_gate, grad_y, w_gate, w_up, w_down):
        toks, dim = tok_x.shape
        tops = route_idx.shape[1]
        experts = w_gate.shape[0] * group
        stride = experts // min(4, experts // 8)
        cap = max(4, 2 * toks * tops // experts)
        rows = group * cap
        half = dim // 2
        tiles = toks // TILE
        tiers = [toks * n // 48 for n in (44, 49, 55, 71)]
        stage = tiers[-1]
        place = 2 * stage
        me = lax.axis_index('expert')
        chip, core = me // 2, me % 2
        up, down, far = (chip + 1) % chips, (chip + chips - 1) % chips, (chip + 2) % chips
        w1, w3, w2 = w_gate[0], w_up[0], w_down[0]

        def mate(v):
            return lax.ppermute(v, 'expert', to_mate)

        all_x = lax.all_gather(tok_x, 'expert')
        all_dy = lax.all_gather(grad_y, 'expert')

        route = jnp.concatenate([route_idx.astype(F32).T, route_gate.T], axis=0)
        every = lax.all_gather(route, 'expert').swapaxes(0, 1)
        idx, gates = every[:tops].astype(I32), every[tops:]
        expert_id = iota((experts, 1, 1), 0)
        taken = jnp.any(idx[None] == expert_id[:, None], axis=1)
        rank = count_before(taken)
        hot_id = expert_id % stride == 0
        kept = taken & (hot_id | (rank < cap))
        spot = jnp.where(kept, rank, -1)
        need = jnp.any(kept.reshape(chips, 2, group, toks), axis=1)
        single = jnp.sum(need.astype(I32), axis=0) == 1
        listed = jnp.where(need, count_before(need), -1)
        sizes = (jnp.sum(need.astype(I32), axis=2) + PIECE - 1) // PIECE * PIECE
        total = jnp.sum(sizes.reshape(chips, chips, 2), axis=2)

        def turn(table, by):
            return jnp.roll(table, -by, axis=0)

        def hop(by):
            sel = (iota((chips, chips), 0) + by) % chips == iota((chips, chips), 1)
            return jnp.sum(jnp.where(sel, total, 0), axis=1)

        parts = 8
        tries = (parts + 1) ** chips
        share = (iota((chips, tries), 1) // ((parts + 1) ** iota((chips, tries), 0))) % (parts + 1)
        two_hops = hop(2)[:, None]
        go_up = two_hops * share // (parts * PIECE) * PIECE
        go_down = two_hops - go_up
        on_up = hop(1)[:, None] + go_up + turn(go_up, -1)
        on_down = hop(chips - 1)[:, None] + go_down + turn(go_down, 1)
        load = jnp.max(jnp.maximum(jnp.maximum(on_up, on_down), 2 * jnp.maximum(go_up, go_down)), axis=0)
        best = jnp.min(load)
        first_best = jnp.min(jnp.where(load == best, jnp.arange(tries, dtype=I32), tries))
        chosen = jnp.sum(jnp.where(iota((1, tries), 1) == first_best, go_up, 0), axis=1)
        other = hop(2) - chosen
        full = jnp.any(taken & hot_id & (rank >= cap))
        state = sum([(best > 2 * size).astype(I32) for size in tiers])
        state = lax.pmax(jnp.where(full, len(tiers), state), ('data', 'expert'))

        def gate_of(eid):
            return jnp.sum(jnp.where(idx == eid, gates, 0.0), axis=0)

        own_spot, mate_spot = pick(spot, me), pick(spot, me ^ 1)
        own_gate, mate_gate = gate_of(me), gate_of(me ^ 1)
        pad = jnp.zeros((group, toks), F32)
        send_info = jnp.stack([pick(listed, chip).astype(F32), own_spot.astype(F32), mate_spot.astype(F32),
                               jnp.where(single, own_gate, 1.0), jnp.where(single, mate_gate, 1.0), pad, pad, pad], axis=1)
        f_up, f_down = pick(chosen, chip), pick(other, chip)
        pass_up, pass_down = pick(chosen, down), pick(other, up)
        my_sizes = pick(sizes, chip)
        devs = jnp.stack([2 * to + k for to in (far, up, down) for k in range(2)])

        def lowest(at, ok):
            low = jnp.min(jnp.where(ok & (at >= 0), at, cap), axis=-1)
            return jnp.where(low < cap, jnp.minimum(low // PIECE * PIECE, cap - SPAN), -1)

        list_tile = (pick(listed, chip) // TILE)[None] == iota((tiles, 1, 1), 0)
        list_tile = list_tile & (pick(listed, chip) >= 0)[None]
        lows = jnp.stack([lowest(v[None], list_tile) for v in (own_spot, mate_spot)], axis=2)
        lows = lows.swapaxes(0, 1).reshape(group, 2 * tiles)
        low_rows = jnp.concatenate([lax.dynamic_slice_in_dim(lows, 2 * to, 2, 0) for to in (far, up, down)])

        def segments(size_of_stage):
            segs = []
            for to, lead, extra in ((far, 0, f_up), (up, f_up, pass_up), (down, f_down, pass_down)):
                for k in range(2):
                    size = pick(my_sizes, 2 * to + k)
                    segs.append(jnp.stack([size, jnp.asarray(lead, I32), extra, jnp.asarray(size_of_stage, I32)]))
                    lead = lead + size
            return jnp.stack(segs)

        tier_stage = sum([jnp.where(state == k, size, 0) for k, size in enumerate(tiers)]) + jnp.where(state == len(tiers), stage, 0)
        segs = segments(tier_stage)

        def home(v):
            return lax.dynamic_slice_in_dim(v, 2 * chip, 2, 0)

        home_idx = [home(idx[j]) for j in range(tops)]
        home_gates = [home(gates[j]) for j in range(tops)]
        home_kept = home(jnp.sum(kept.astype(I32) * (1 << expert_id), axis=0))
        home_single = home(single.astype(I32)) > 0

        def listed_at(c):
            at = home(pick(listed, c))
            first = pick(pick(sizes, c), 2 * chip)
            return at >= 0, at + jnp.where(iota((2, 1), 0) == 1, first, 0)

        def weight_of(c):
            w = 0.0
            for j in range(tops):
                held = (home_kept >> home_idx[j]) % 2 == 1
                w = w + jnp.where((home_idx[j] // 2 == c) & held, home_gates[j], 0.0)
            return jnp.where(home_single, 1.0, w)

        far_ok, far_at = listed_at(far)
        far_cut = pick(chosen, far)
        far_by_up = jnp.where(far_ok & (far_at < far_cut), far_at, -1)
        far_by_down = jnp.where(far_ok & (far_at >= far_cut), far_at - far_cut, -1)
        home_spots = [home(own_spot), home(mate_spot)]
        weights = [weight_of(c) for c in (down, up, far)]
        own_lows = [lowest(v.reshape(2 * tiles, TILE), True) for v in home_spots]

        def arrival(size_of_stage):
            def near_spot(c, lead, passed):
                ok, at = listed_at(c)
                at = at + lead
                return jnp.where(ok, jnp.where(at >= size_of_stage, stage + at + passed - size_of_stage, at), -1)

            from_down = near_spot(down, pick(chosen, down), pick(chosen, far))
            from_up = near_spot(up, pick(other, up), pick(other, far))
            info = [v.astype(F32) for v in home_spots] + [home(own_gate), home(mate_gate)]
            info += [v.astype(F32) for v in (from_down, from_up, far_by_up, far_by_down)] + weights
            info = jnp.stack(info + [jnp.zeros((2, toks), F32)] * 5, axis=1)
            begins = []
            for near, by in ((from_down, far_by_up), (from_up, far_by_down)):
                begins.append(jnp.where((near >= 0) & (near < stage), near, place))
                begins.append(jnp.where(near >= stage, near - stage, place))
                begins.append(jnp.where(by >= 0, by, place))
            begins = jnp.stack(begins).reshape(6, 2 * tiles, TILE)
            low = jnp.min(begins, axis=2)
            end = jnp.max(jnp.where(begins < place, begins, -1), axis=2) + 1
            low = jnp.where(low < place, jnp.minimum(low // PIECE * PIECE, size_of_stage - WINDOW), -1)
            return info, jnp.concatenate([low, jnp.stack(own_lows), end]).T

        home_info, win = arrival(tier_stage)
        homes = jnp.stack([2 * chip, 2 * chip + 1])

        onehot_in = (own_spot[:, None, :] == iota((1, cap, 1), 1)).astype(BF)

        def columns(w, axis, mine):
            parts = jnp.split(w, 2, axis=axis)
            return jnp.where((core == 0) == mine, parts[0], parts[1])

        w2_halves = [columns(w2, 1, m) for m in (True, False)]
        w2t = row_major(w2.T)
        w13t_halves = [[row_major(columns(w, 0, m).T) for w in (w1, w3)] for m in (True, False)]
        counts = jnp.sum((own_spot >= 0).astype(I32), axis=1)
        pad = jnp.zeros((group, toks), F32)
        own_info = jnp.stack([own_spot.astype(F32), own_gate] + [pad] * 6, axis=1)
        plan = (state, send_info, devs, segs, low_rows, home_info, win, homes, onehot_in, counts, own_info, w2_halves, w2t, w13t_halves)
        plan = lax.optimization_barrier(plan)
        all_x, plan = lax.optimization_barrier((all_x, plan))
        (state, send_info, devs, segs, low_rows, home_info, win, homes, onehot_in, counts, own_info, w2_halves, w2t, w13t_halves) = plan

        def take(onehot, tok, gate=None):
            got = dot('gcs,gsd->gcd', onehot, tok)
            return (got if gate is None else gate.reshape(group, cap, 1) * got).astype(BF).reshape(rows, dim)

        def up_front(x):
            pre_a = dot('cd,df->cf', x, w1).astype(BF)
            pre_b = dot('cd,df->cf', x, w3).astype(BF)
            pre_a, pre_b = lax.optimization_barrier((pre_a, pre_b))
            a = pre_a.astype(F32)
            hid = (a * jax.nn.sigmoid(a) * pre_b.astype(F32)).astype(BF)
            return pre_a, pre_b, hid

        def inner_grads(pre_a, pre_b, dh):
            dh = dh.astype(BF).astype(F32)
            a = pre_a.astype(F32)
            sig = jax.nn.sigmoid(a)
            da = (dh * pre_b.astype(F32) * (sig * (1.0 + a * (1.0 - sig)))).astype(BF)
            db = (dh * (a * sig)).astype(BF)
            return da, db

        any_spec = pl.BlockSpec(memory_space=pl.ANY)

        def packed(tables, size, scaled):
            table_spec = pl.BlockSpec((1, cap, half), lambda g, dev, seg, low: (dev[g], 0, 0))
            res = pl.pallas_call(
                functools.partial(pack_kernel, scaled),
                grid_spec=pltpu.PrefetchScalarGridSpec(
                    num_scalar_prefetch=3, grid=(6,),
                    in_specs=[table_spec, table_spec, pl.BlockSpec((1, 8, toks), lambda g, dev, seg, low: (dev[g], 0, 0))],
                    out_specs=[any_spec] * 4,
                    scratch_shapes=[pltpu.VMEM((2, TILE, half), BF), pltpu.SMEM((2,), I32),
                                    pltpu.SemaphoreType.DMA((2,))]),
                out_shape=[jax.ShapeDtypeStruct((size, half), BF)] * 4,
                compiler_params=pltpu.CompilerParams(vmem_limit_bytes=VMEM_LIMIT),
                cost_estimate=pl.CostEstimate(flops=2 * rows * cap * half, bytes_accessed=12 * rows * half, transcendentals=0),
                name='pack',
            )(devs, segs, low_rows, *tables, send_info)
            return res[:2], res[2:]

        def arrived(tables, info, win, got_up, got_down, scaled):
            table_spec = pl.BlockSpec((1, cap, half), lambda t, homes, win: (homes[t // tiles], 0, 0))
            info_spec = pl.BlockSpec((1, 16, TILE), lambda t, homes, win: (t // tiles, 0, t % tiles))
            return pl.pallas_call(
                functools.partial(arrive_kernel, scaled, stage),
                grid_spec=pltpu.PrefetchScalarGridSpec(
                    num_scalar_prefetch=2, grid=(2 * tiles,),
                    in_specs=[table_spec, table_spec, info_spec] + [any_spec] * 4,
                    out_specs=pl.BlockSpec((1, TILE, half), lambda t, homes, win: (t // tiles, t % tiles, 0)),
                    scratch_shapes=[pltpu.VMEM((TILE, half), F32), pltpu.VMEM((2, 6, SPAN, half), BF), pltpu.SemaphoreType.DMA((2, 6))]),
                out_shape=jax.ShapeDtypeStruct((2, toks, half), BF),
                compiler_params=pltpu.CompilerParams(vmem_limit_bytes=VMEM_LIMIT),
                cost_estimate=pl.CostEstimate(flops=2 * rows * cap * half, bytes_accessed=12 * rows * half, transcendentals=0),
                name='arrive',
            )(homes, win, *tables, info, *got_up, *got_down)

        def shift(up_rows, down_rows):
            got_up = lax.ppermute(up_rows, 'expert', to_next)
            got_down = lax.ppermute(down_rows, 'expert', to_prev)
            return got_up, got_down

        def second_rows(got, up_rows, down_rows):
            row = iota((up_rows.shape[0], 1), 0)
            return jnp.where(row < pass_up, got[0], up_rows), jnp.where(row < pass_down, got[1], down_rows)

        def parts_of(total):
            mine = jnp.where(core == 0, total[0], total[1])
            return mine, mate(jnp.where(core == 0, total[1], total[0]))

        def join(mine, theirs):
            return jnp.where(core == 0, jnp.concatenate([mine, theirs], axis=1), jnp.concatenate([theirs, mine], axis=1))

        def table(v):
            return v.reshape(group, cap, half)

        x = take(onehot_in, all_x)
        pre_a, pre_b, hid = up_front(x)
        theirs = dot('cf,fd->cd', hid, w2_halves[1]).astype(BF)
        out_got = mate(theirs)
        ours = dot('cf,fd->cd', after(hid, theirs), w2_halves[0]).astype(BF)
        out_tables = (table(ours), table(out_got))
        out_up, out_down = packed(out_tables, stage, True)
        cut = [(out_up[0][:size], out_down[0][:size]) for size in tiers[:-1]] + [(out_up[0], out_down[0])]
        all_dy = after(all_dy, out_up, out_down, cut)

        def block_spec(rows, width):
            return pl.BlockSpec((1, rows, width), lambda e, count: (e, 0, 0))

        def fixed_spec(w):
            return pl.BlockSpec(w.shape, lambda e, count: (0, 0), pipeline_mode=pl.Buffered(1))

        def inner_grads_of(dy):
            f = pre_a.shape[1]
            return pl.pallas_call(
                inner_kernel,
                grid_spec=pltpu.PrefetchScalarGridSpec(
                    num_scalar_prefetch=1, grid=(group,),
                    in_specs=[block_spec(8, toks), block_spec(toks, dim), fixed_spec(w2t), block_spec(cap, f), block_spec(cap, f)],
                    out_specs=[block_spec(cap, dim), block_spec(cap, f), block_spec(cap, f)]),
                out_shape=[jax.ShapeDtypeStruct((group, cap, n), BF) for n in (dim, f, f)],
                compiler_params=pltpu.CompilerParams(vmem_limit_bytes=VMEM_LIMIT),
                cost_estimate=pl.CostEstimate(flops=2 * rows * dim * (toks + f), bytes_accessed=2 * rows * dim * 4, transcendentals=rows * f),
                name='inner',
            )(counts, own_info, dy, w2t, pre_a.reshape(group, cap, f), pre_b.reshape(group, cap, f))

        def input_grad(da, db, k):
            w1t, w3t = w13t_halves[k]
            f = da.shape[2]
            return pl.pallas_call(
                input_kernel,
                grid_spec=pltpu.PrefetchScalarGridSpec(
                    num_scalar_prefetch=1, grid=(group,),
                    in_specs=[block_spec(cap, f), block_spec(cap, f), fixed_spec(w1t), fixed_spec(w3t)],
                    out_specs=block_spec(cap, half)),
                out_shape=jax.ShapeDtypeStruct((group, cap, half), BF),
                compiler_params=pltpu.CompilerParams(vmem_limit_bytes=VMEM_LIMIT),
                cost_estimate=pl.CostEstimate(flops=4 * rows * f * half, bytes_accessed=4 * rows * half, transcendentals=0),
                name='input_grad',
            )(counts, da, db, w1t, w3t)

        def rest(tier):
            size = tiers[tier]
            out_first = shift(*cut[tier])
            g, da, db = inner_grads_of(all_dy)
            theirs = input_grad(da, db, 1)
            dx_got = mate(theirs)
            out_second = second_rows(after(out_first, theirs), out_up[1][:size], out_down[1][:size])
            out_last = shift(*out_second)
            ours = input_grad(*after((da, db), *out_second), 0)
            dx_tables = (ours, dx_got)
            dx_up, dx_down = packed(dx_tables, size, False)
            dx_first = shift(dx_up[0], dx_down[0])
            out_first, out_last, da, db, g = after((out_first, out_last, da, db, g), dx_up, dx_down)
            f = da.shape[2]
            da, db, g = da.reshape(rows, f), db.reshape(rows, f), g.reshape(rows, dim)
            dw1 = dot('cd,cf->df', x, da)
            out_first, out_last = after((out_first, out_last), dw1[:8, :TILE])
            y = arrived(out_tables, home_info, win, (out_first[0], out_last[0]), (out_first[1], out_last[1]), True)
            y = join(*parts_of(y))
            dx_second = second_rows(after(dx_first, y), dx_up[1], dx_down[1])
            dx_last = shift(*dx_second)
            db, hid_late = after((db, hid), *dx_second)
            dw3 = dot('cd,cf->df', x, db)
            dw2 = dot('cf,cd->fd', hid_late, g)
            gx = parts_of(arrived(dx_tables, home_info, win, (dx_first[0], dx_last[0]), (dx_first[1], dx_last[1]), False))
            return y, *gx, row_major(dw1)[None], row_major(dw3)[None], row_major(dw2)[None]

        def general():
            my_rank, my_taken = pick(rank, me), pick(taken.astype(I32), me) > 0
            my_idx = route_idx.T
            home_rank = pick(jnp.moveaxis(rank, 1, 0), me)
            out_rank = jnp.stack([jnp.sum(jnp.where(my_idx[j] == expert_id[:, 0], home_rank, 0), axis=0) for j in range(tops)])
            out_hot = my_idx % stride == 0

            def one_pass(first):
                ok = my_taken & (my_rank >= first) & (my_rank < first + cap)
                ok_out = (out_rank >= first) & (out_rank < first + cap)
                if first:
                    ok = ok & (me % stride == 0)
                    ok_out = ok_out & out_hot
                onehot = jnp.where(ok, my_rank - first, -1)[:, None, :] == iota((1, cap, 1), 1)
                gate = jnp.sum(jnp.where(onehot, own_gate[:, None, :], 0.0), axis=2)
                onehot = onehot.astype(BF)
                goal = jnp.where(ok_out, my_idx * cap + out_rank - first, -1)
                onehot_out = (goal[:, :, None] == iota((1, 1, rows), 2)).astype(BF)

                def swap(r):
                    return lax.all_to_all(r.reshape(group, cap, dim), 'expert', 0, 0).reshape(rows, dim)

                x = take(onehot, all_x)
                pre_a, pre_b, hid = up_front(x)
                back = swap(dot('cf,fd->cd', hid, w2).astype(BF))
                g = lax.optimization_barrier(take(onehot, all_dy, gate))
                da, db = lax.optimization_barrier(inner_grads(pre_a, pre_b, dot('cd,fd->cf', g, w2)))
                dx = (dot('cf,df->cd', da, w1) + dot('cf,df->cd', db, w3)).astype(BF)
                back_dx = swap(after(dx, back))
                slots = dot('jtr,rd->jtd', onehot_out, back)
                y = jnp.sum(route_gate.T[:, :, None] * slots, axis=0)
                gx = dot('tr,rd->td', jnp.sum(onehot_out, axis=0), back_dx)
                return y, gx, dot('cd,cf->df', x, da), dot('cd,cf->df', x, db), dot('cf,cd->fd', hid, g)

            first = one_pass(0)
            second = one_pass(cap)
            sums = [u + v for u, v in zip(first, second)]
            gx = jnp.split(sums[1].astype(BF), 2, axis=1)
            gx = [jnp.where(core == k, gx[0], gx[1]) for k in range(2)]
            return sums[0].astype(BF), *gx, *[v[None] for v in sums[2:]]

        branches = [functools.partial(rest, tier) for tier in range(len(tiers))] + [general]
        y, mine, theirs, dw1, dw3, dw2 = lax.switch(state, branches)
        return y, join(mine, theirs), dw1, dw3, dw2

    return jax.shard_map(layer, mesh=mesh, in_specs=(tok_spec,) * 4 + (w_spec,) * 3, out_specs=(tok_spec,) * 5, check_vma=False)
```

```python
import functools

import jax
import jax.numpy as jnp
from jax import lax
from jax.experimental import pallas as pl
from jax.experimental.layout import Layout, with_layout_constraint
from jax.experimental.pallas import tpu as pltpu
from jax.sharding import PartitionSpec as P

BF = jnp.bfloat16
F32 = jnp.float32
I32 = jnp.int32
PIECE = 16
TILE = 128
SPAN = 256
ROOM = 512
VMEM_LIMIT = 50 * 2 ** 20


def dot(form, a, b):
    return jnp.einsum(form, a, b, preferred_element_type=F32)


def iota(shape, axis):
    return lax.broadcasted_iota(I32, shape, axis)


def count_before(mask):
    n = mask.shape[-1]
    earlier = iota((n, n), 0) < iota((n, n), 1)
    return dot('...u,us->...s', mask.astype(BF), earlier.astype(BF)).astype(I32)


def pick(table, index):
    sel = iota(table.shape, 0) == index
    return jnp.sum(jnp.where(sel, table, jnp.zeros_like(table)), axis=0)


def row_major(v):
    return with_layout_constraint(v, Layout(major_to_minor=tuple(range(v.ndim))))


def after(value, *others):
    return lax.optimization_barrier((value,) + others)[0]


def pack_kernel(scaled, dev_ref, seg_ref, low_ref, tab0, tab1, cols, *refs):
    outs, (buf, pend, sem) = (refs[0:2], refs[2:4]), refs[4:]
    g = pl.program_id(0)
    toks = cols.shape[1]
    length, start, extra, stage = [seg_ref[g, k] for k in range(4)]

    @pl.when(g == 0)
    def _():
        pend[0] = 0
        pend[1] = 0

    def drain(slot):
        def one(_, carry):
            pltpu.make_async_copy(buf.at[0, pl.ds(0, PIECE)], outs[0][0].at[pl.ds(0, PIECE)], sem.at[slot]).wait()
            return carry

        lax.fori_loop(0, pend[slot], one, 0)
        pend[slot] = 0

    def put(slot, p, side, at):
        for late, ref in enumerate(outs[side]):
            @pl.when((at >= stage) == bool(late))
            def _(ref=ref, late=late):
                spot = jnp.minimum(at - stage if late else at, ref.shape[0] - PIECE)
                src = buf.at[slot, pl.ds(pl.multiple_of(p * PIECE, PIECE), PIECE)]
                pltpu.make_async_copy(src, ref.at[pl.ds(pl.multiple_of(spot, PIECE), PIECE)], sem.at[slot]).start()
        pend[slot] = pend[slot] + 1

    def tile(i, carry):
        @pl.when(i * TILE < length)
        def _():
            slot = lax.rem(i, 2)
            drain(slot)
            vals = cols[0, pl.ds(pl.multiple_of(i * TILE, TILE), TILE)]
            lows = [low_ref[g, 2 * i + k] for k in range(2)]

            def part(k, tab):
                at = vals[:, k:k + 1] - lows[k].astype(F32)
                onehot = (at == iota((TILE, SPAN), 1).astype(F32)).astype(BF)
                got = jnp.dot(onehot, tab[0, pl.ds(pl.multiple_of(lows[k], PIECE), SPAN)], preferred_element_type=F32)
                return got * vals[:, 2 + k:3 + k] if scaled else got

            @pl.when((lows[0] >= 0) & (lows[1] < 0))
            def _():
                buf[slot] = part(0, tab0).astype(BF)

            @pl.when((lows[0] < 0) & (lows[1] >= 0))
            def _():
                buf[slot] = part(1, tab1).astype(BF)

            @pl.when((lows[0] >= 0) & (lows[1] >= 0))
            def _():
                buf[slot] = (part(0, tab0) + part(1, tab1)).astype(BF)

            def piece(p, carry):
                q = i * TILE + p * PIECE
                at = start + q
                near = jnp.where(at >= stage, at + extra, at)

                @pl.when((q < length) & (g < 2) & (at < extra))
                def _():
                    put(slot, p, 0, at)

                @pl.when((q < length) & (g < 2) & (at >= extra))
                def _():
                    put(slot, p, 1, at - extra)

                @pl.when((q < length) & (g >= 2) & (g < 4))
                def _():
                    put(slot, p, 0, near)

                @pl.when((q < length) & (g >= 4))
                def _():
                    put(slot, p, 1, near)

                return carry

            lax.fori_loop(0, TILE // PIECE, piece, 0)

        return carry

    lax.fori_loop(0, toks // TILE, tile, 0)

    @pl.when(g == pl.num_programs(0) - 1)
    def _():
        drain(0)
        drain(1)


def arrive_kernel(scaled, home_ref, plan_ref, info, tab0, tab1, up1, up2, down1, down2, out, wbuf, sem):
    t, last = pl.program_id(0), pl.num_programs(0) - 1
    sources = (tab0.at[home_ref[0]], tab1.at[home_ref[0]], up1, up2, up2, down1, down2, down2)

    def pieces(step, do):
        slot = lax.rem(step, 2)
        for w, ref in enumerate(sources):
            begin, count, to = [plan_ref[step, 3 * w + k] for k in range(3)]

            def one(p, carry, ref=ref, begin=begin, to=to):
                src = ref.at[pl.ds(pl.multiple_of(begin + p * PIECE, PIECE), PIECE)]
                do(pltpu.make_async_copy(src, wbuf.at[slot, pl.ds(pl.multiple_of(to + p * PIECE, PIECE), PIECE)], sem.at[slot]))
                return carry

            lax.fori_loop(0, count, one, 0)

    @pl.when(t == 0)
    def _():
        wbuf[...] = jnp.zeros_like(wbuf)
        pieces(0, lambda c: c.start())

    @pl.when(t < last)
    def _():
        pieces(t + 1, lambda c: c.start())

    vals = info[0]
    eye = iota((TILE, TILE), 0) == iota((TILE, TILE), 1)
    lane = iota((TILE, wbuf.shape[1]), 1).astype(F32)

    def column(k):
        return jnp.sum(jnp.where(eye, vals[k:k + 1, :], 0.0), axis=1, keepdims=True)

    first, second = column(0) == lane, column(1) == lane
    pieces(t, lambda c: c.wait())
    rows = wbuf.at[lax.rem(t, 2)]
    if scaled:
        total = column(2) * jnp.dot(first.astype(BF), rows[...], preferred_element_type=F32)
        total = total + column(3) * jnp.dot(second.astype(BF), rows[...], preferred_element_type=F32)
    else:
        total = jnp.dot((first | second).astype(BF), rows[...], preferred_element_type=F32)
    out[...] = total.astype(BF)


def by_count(count, cap, run):
    for n in range(0, cap + 1, TILE):
        @pl.when((count > n - TILE) & (count <= n))
        def _(n=n):
            run(n)


def inner_kernel(count_ref, from_ref, info, dy, w2t, a_ref, b_ref, g_ref, da_ref, db_ref):
    e = pl.program_id(0)
    cap, dim = g_ref.shape[1:]
    toks = dy.shape[1]
    step = dim // 4
    count, begin = count_ref[e], from_ref[e]

    def fill(n, begin, span):
        if n:
            vals = info[0, :, pl.ds(begin, span)]
            match = vals[0:1, :] == iota((n, span), 0).astype(F32)
            gate = jnp.sum(jnp.where(match, vals[1:2, :], 0.0), axis=1, keepdims=True)
            onehot = match.astype(BF)
            for c in range(0, dim, step):
                got = jnp.dot(onehot, dy[0, pl.ds(begin, span), c:c + step], preferred_element_type=F32)
                g_ref[0, :n, c:c + step] = (gate * got).astype(BF)
            dh = jnp.dot(g_ref[0, :n], w2t[...], preferred_element_type=F32).astype(BF).astype(F32)
            a, b = a_ref[0, :n].astype(F32), b_ref[0, :n].astype(F32)
            sig = jax.nn.sigmoid(a)
            da_ref[0, :n] = (dh * b * (sig * (1.0 + a * (1.0 - sig)))).astype(BF)
            db_ref[0, :n] = (dh * (a * sig)).astype(BF)
        if n < cap:
            for ref in (g_ref, da_ref, db_ref):
                ref[0, n:] = jnp.zeros((cap - n, ref.shape[2]), BF)

    @pl.when(begin >= 0)
    def _():
        by_count(count, cap, lambda n: fill(n, pl.multiple_of(begin, TILE), toks * 2 // 3))

    @pl.when(begin < 0)
    def _():
        fill(cap, 0, toks)


def input_kernel(count_ref, da, db, w1t, w3t, out):
    cap, width = out.shape[1:]
    step = width // 2

    def run(n):
        if n:
            for c in range(0, width, step):
                got = jnp.dot(da[0, :n], w1t[:, c:c + step], preferred_element_type=F32)
                got = got + jnp.dot(db[0, :n], w3t[:, c:c + step], preferred_element_type=F32)
                out[0, :n, c:c + step] = got.astype(BF)
        if n < cap:
            out[0, n:] = jnp.zeros((cap - n, width), BF)

    by_count(count_ref[pl.program_id(0)], cap, run)


def solution(mesh):
    group = mesh.shape['expert']
    chips = group // 2
    tok_spec = P(('data', 'expert'))
    w_spec = P('expert')
    to_mate = [(i, i ^ 1) for i in range(group)]
    to_next = [(i, (i + 2) % group) for i in range(group)]
    to_prev = [(i, (i - 2) % group) for i in range(group)]

    def layer(tok_x, route_idx, route_gate, grad_y, w_gate, w_up, w_down):
        toks, dim = tok_x.shape
        tops = route_idx.shape[1]
        experts = w_gate.shape[0] * group
        stride = experts // min(4, experts // 8)
        cap = max(4, 2 * toks * tops // experts)
        rows = group * cap
        half = dim // 2
        tiles = toks // TILE
        tiers = [toks * n // 48 for n in (44, 49, 55, 71)]
        stage = tiers[-1]
        place = 2 * stage
        me = lax.axis_index('expert')
        chip, core = me // 2, me % 2
        up, down, far = (chip + 1) % chips, (chip + chips - 1) % chips, (chip + 2) % chips
        w1, w3, w2 = w_gate[0], w_up[0], w_down[0]

        def mate(v):
            return lax.ppermute(v, 'expert', to_mate)

        all_x = lax.all_gather(tok_x, 'expert')
        all_dy = lax.all_gather(grad_y, 'expert')

        route = jnp.concatenate([route_idx.astype(F32).T, route_gate.T], axis=0)
        every = lax.all_gather(route, 'expert').swapaxes(0, 1)
        idx, gates = every[:tops].astype(I32), every[tops:]
        expert_id = iota((experts, 1, 1), 0)
        taken = jnp.any(idx[None] == expert_id[:, None], axis=1)
        rank = count_before(taken)
        hot_id = expert_id % stride == 0
        kept = taken & (hot_id | (rank < cap))
        spot = jnp.where(kept, rank, -1)
        need = jnp.any(kept.reshape(chips, 2, group, toks), axis=1)
        single = jnp.sum(need.astype(I32), axis=0) == 1
        listed = jnp.where(need, count_before(need), -1)
        sizes = (jnp.sum(need.astype(I32), axis=2) + PIECE - 1) // PIECE * PIECE
        total = jnp.sum(sizes.reshape(chips, chips, 2), axis=2)

        def turn(table, by):
            return jnp.roll(table, -by, axis=0)

        def hop(by):
            sel = (iota((chips, chips), 0) + by) % chips == iota((chips, chips), 1)
            return jnp.sum(jnp.where(sel, total, 0), axis=1)

        parts = 8
        tries = (parts + 1) ** chips
        share = (iota((chips, tries), 1) // ((parts + 1) ** iota((chips, tries), 0))) % (parts + 1)
        two_hops = hop(2)[:, None]
        go_up = two_hops * share // (parts * PIECE) * PIECE
        go_down = two_hops - go_up
        on_up = hop(1)[:, None] + go_up + turn(go_up, -1)
        on_down = hop(chips - 1)[:, None] + go_down + turn(go_down, 1)
        load = jnp.max(jnp.maximum(jnp.maximum(on_up, on_down), 2 * jnp.maximum(go_up, go_down)), axis=0)
        best = jnp.min(load)
        first_best = jnp.min(jnp.where(load == best, jnp.arange(tries, dtype=I32), tries))
        chosen = jnp.sum(jnp.where(iota((1, tries), 1) == first_best, go_up, 0), axis=1)
        other = hop(2) - chosen
        full = jnp.any(taken & hot_id & (rank >= cap))
        state = sum([(best > 2 * size).astype(I32) for size in tiers])
        state = lax.pmax(jnp.where(full, len(tiers), state), ('data', 'expert'))

        def gate_of(eid):
            return jnp.sum(jnp.where(idx == eid, gates, 0.0), axis=0)

        own_spot, mate_spot = pick(spot, me), pick(spot, me ^ 1)
        own_gate, mate_gate = gate_of(me), gate_of(me ^ 1)
        f_up, f_down = pick(chosen, chip), pick(other, chip)
        pass_up, pass_down = pick(chosen, down), pick(other, up)
        my_sizes = pick(sizes, chip)
        devs = jnp.stack([2 * to + k for to in (far, up, down) for k in range(2)])

        def lowest(at, ok):
            low = jnp.min(jnp.where(ok & (at >= 0), at, cap), axis=-1)
            return jnp.where(low < cap, jnp.minimum(low // PIECE * PIECE, cap - SPAN), -1)

        list_tile = (pick(listed, chip) // TILE)[None] == iota((tiles, 1, 1), 0)
        list_tile = list_tile & (pick(listed, chip) >= 0)[None]
        lows = jnp.stack([lowest(v[None], list_tile) for v in (own_spot, mate_spot)], axis=2)
        lows = lows.swapaxes(0, 1).reshape(group, 2 * tiles)
        low_rows = jnp.concatenate([lax.dynamic_slice_in_dim(lows, 2 * to, 2, 0) for to in (far, up, down)])

        def segments(size_of_stage):
            segs = []
            for to, lead, extra in ((far, 0, f_up), (up, f_up, pass_up), (down, f_down, pass_down)):
                for k in range(2):
                    size = pick(my_sizes, 2 * to + k)
                    segs.append(jnp.stack([size, jnp.asarray(lead, I32), extra, jnp.asarray(size_of_stage, I32)]))
                    lead = lead + size
            return jnp.stack(segs)

        def of_chips(v):
            return jnp.concatenate([lax.dynamic_slice_in_dim(v, 2 * to, 2, 0) for to in (far, up, down)])

        def thirds(v):
            high = v.astype(BF)
            middle = (v - high.astype(F32)).astype(BF)
            return [high, middle, (v - high.astype(F32) - middle.astype(F32)).astype(BF)]

        values = []
        for v in (own_spot, mate_spot):
            v = of_chips(v) + 1
            values += [(v // 256).astype(BF), (v % 256).astype(BF)]
        for v in (own_gate, mate_gate):
            values += thirds(of_chips(jnp.where(single, v, 1.0)))
        in_list = of_chips(pick(listed, chip))[:, None, :] == iota((1, toks, 1), 1)
        got = dot('gqs,gsk->gqk', in_list.astype(BF), jnp.stack(values, axis=2))
        list_cols = [got[:, :, 2 * k] * 256.0 + got[:, :, 2 * k + 1] - 1.0 for k in range(2)]
        list_cols += [got[:, :, 4 + 3 * k] + got[:, :, 5 + 3 * k] + got[:, :, 6 + 3 * k] for k in range(2)]
        list_cols = jnp.stack(list_cols + [jnp.zeros_like(list_cols[0])] * 4, axis=2)

        tier_stage = sum([jnp.where(state == k, size, 0) for k, size in enumerate(tiers)]) + jnp.where(state == len(tiers), stage, 0)
        segs = segments(tier_stage)

        def home(v):
            v = lax.dynamic_slice_in_dim(v, 2 * chip, 2, 0)
            return jnp.where(core == 0, v[::-1], v)

        home_core = jnp.where((core == 0) == (iota((2, 1), 0) == 0), 1, 0)
        home_idx = [home(idx[j]) for j in range(tops)]
        home_gates = [home(gates[j]) for j in range(tops)]
        home_kept = home(jnp.sum(kept.astype(I32) * (1 << expert_id), axis=0))
        home_single = home(single.astype(I32)) > 0

        def listed_at(c):
            at = home(pick(listed, c))
            first = pick(pick(sizes, c), 2 * chip)
            return at >= 0, at + jnp.where(home_core == 1, first, 0)

        def weight_of(c):
            w = 0.0
            for j in range(tops):
                held = (home_kept >> home_idx[j]) % 2 == 1
                w = w + jnp.where((home_idx[j] // 2 == c) & held, home_gates[j], 0.0)
            return jnp.where(home_single, 1.0, w)

        def near_spots(c, lead, passed):
            ok, at = listed_at(c)
            at = at + lead
            late = at >= tier_stage
            return [jnp.where(ok & jnp.logical_not(late), at, -1), jnp.where(ok & late, at + passed - tier_stage, -1)]

        far_ok, far_at = listed_at(far)
        far_cut = pick(chosen, far)
        spots = [home(own_spot), home(mate_spot)]
        spots += near_spots(down, pick(chosen, down), pick(chosen, far)) + [jnp.where(far_ok & (far_at < far_cut), far_at, -1)]
        spots += near_spots(up, pick(other, up), pick(other, far)) + [jnp.where(far_ok & (far_at >= far_cut), far_at - far_cut, -1)]
        w_down, w_up, w_far = [weight_of(c) for c in (down, up, far)]
        weights = [home(own_gate), home(mate_gate), w_down, w_down, w_far, w_up, w_up, w_far]
        spots = jnp.stack(spots).reshape(8, 2 * tiles, TILE)
        weights = jnp.stack(weights).reshape(8, 2 * tiles, TILE)
        there = spots >= 0
        begin = jnp.min(jnp.where(there, spots, place), axis=2) // PIECE * PIECE
        count = jnp.maximum(jnp.max(spots, axis=2) - begin + PIECE, 0) // PIECE
        to = jnp.cumsum(count, axis=0) * PIECE - count * PIECE
        at = jnp.where(there, spots + (to - begin)[:, :, None], -1)
        first = jnp.max(at, axis=0)
        second = jnp.sum(at + 1, axis=0) - first - 2
        w_first = jnp.sum(jnp.where(there & (at == first[None]), weights, 0.0), axis=0)
        w_second = jnp.sum(jnp.where(there & (at == second[None]), weights, 0.0), axis=0)
        home_info = [first.astype(F32), second.astype(F32), w_first, w_second]
        home_info = jnp.stack(home_info + [jnp.zeros_like(w_first)] * 4, axis=1).reshape(2, tiles, 8, TILE)
        home_plan = jnp.stack([begin, count, to], axis=1).reshape(24, 2 * tiles).T.reshape(2, tiles, 24)
        homes = 2 * chip + home_core

        onehot_in = (own_spot[:, None, :] == iota((1, cap, 1), 1)).astype(BF)

        def columns(w, axis, mine):
            parts = jnp.split(w, 2, axis=axis)
            return jnp.where((core == 0) == mine, parts[0], parts[1])

        w2_halves = [columns(w2, 1, m) for m in (True, False)]
        w2t = row_major(w2.T)
        w13t_halves = [[row_major(columns(w, 0, m).T) for w in (w1, w3)] for m in (True, False)]
        counts = jnp.sum((own_spot >= 0).astype(I32), axis=1)
        pad = jnp.zeros((group, toks), F32)
        own_info = jnp.stack([own_spot.astype(F32), own_gate] + [pad] * 6, axis=1)
        span = toks * 2 // 3
        s_first = jnp.min(jnp.where(own_spot >= 0, iota(own_spot.shape, 1), toks), axis=1)
        s_last = jnp.max(jnp.where(own_spot >= 0, iota(own_spot.shape, 1), 0), axis=1)
        froms = jnp.minimum(s_first // TILE * TILE, toks - span)
        froms = jnp.where(s_last < froms + span, froms, -1)
        plan = (state, list_cols, devs, segs, low_rows, home_info, home_plan, homes, onehot_in, counts, froms, own_info, w2_halves, w2t, w13t_halves)
        plan = lax.optimization_barrier(plan)
        all_x, plan = lax.optimization_barrier((all_x, plan))
        (state, list_cols, devs, segs, low_rows, home_info, home_plan, homes, onehot_in, counts, froms, own_info, w2_halves, w2t,
         w13t_halves) = plan

        def take(onehot, tok, gate=None):
            got = dot('gcs,gsd->gcd', onehot, tok)
            return (got if gate is None else gate.reshape(group, cap, 1) * got).astype(BF).reshape(rows, dim)

        def up_front(x):
            pre_a = dot('cd,df->cf', x, w1).astype(BF)
            pre_b = dot('cd,df->cf', x, w3).astype(BF)
            pre_a, pre_b = lax.optimization_barrier((pre_a, pre_b))
            a = pre_a.astype(F32)
            hid = (a * jax.nn.sigmoid(a) * pre_b.astype(F32)).astype(BF)
            return pre_a, pre_b, hid

        def inner_grads(pre_a, pre_b, dh):
            dh = dh.astype(BF).astype(F32)
            a = pre_a.astype(F32)
            sig = jax.nn.sigmoid(a)
            da = (dh * pre_b.astype(F32) * (sig * (1.0 + a * (1.0 - sig)))).astype(BF)
            db = (dh * (a * sig)).astype(BF)
            return da, db

        any_spec = pl.BlockSpec(memory_space=pl.ANY)

        def packed(tables, size, scaled):
            table_spec = pl.BlockSpec((1, cap, half), lambda g, dev, seg, low: (dev[g], 0, 0))
            res = pl.pallas_call(
                functools.partial(pack_kernel, scaled),
                grid_spec=pltpu.PrefetchScalarGridSpec(
                    num_scalar_prefetch=3, grid=(6,),
                    in_specs=[table_spec, table_spec, pl.BlockSpec((1, toks, 8), lambda g, dev, seg, low: (g, 0, 0))],
                    out_specs=[any_spec] * 4,
                    scratch_shapes=[pltpu.VMEM((2, TILE, half), BF), pltpu.SMEM((2,), I32),
                                    pltpu.SemaphoreType.DMA((2,))]),
                out_shape=[jax.ShapeDtypeStruct((size, half), BF)] * 4,
                compiler_params=pltpu.CompilerParams(vmem_limit_bytes=VMEM_LIMIT),
                cost_estimate=pl.CostEstimate(flops=2 * rows * cap * half, bytes_accessed=12 * rows * half, transcendentals=0),
                name='pack',
            )(devs, segs, low_rows, *tables, list_cols)
            return res[:2], res[2:]

        def arrived(which, tables, got_up, got_down, scaled):
            return pl.pallas_call(
                functools.partial(arrive_kernel, scaled),
                grid_spec=pltpu.PrefetchScalarGridSpec(
                    num_scalar_prefetch=2, grid=(tiles,),
                    in_specs=[pl.BlockSpec((1, 8, TILE), lambda t, homes, plan: (t, 0, 0))] + [any_spec] * 6,
                    out_specs=pl.BlockSpec((TILE, half), lambda t, homes, plan: (t, 0)),
                    scratch_shapes=[pltpu.VMEM((2, ROOM, half), BF), pltpu.SemaphoreType.DMA((2,))]),
                out_shape=jax.ShapeDtypeStruct((toks, half), BF),
                compiler_params=pltpu.CompilerParams(vmem_limit_bytes=VMEM_LIMIT),
                cost_estimate=pl.CostEstimate(flops=2 * rows * cap * half, bytes_accessed=6 * rows * half, transcendentals=0),
                name='arrive',
            )(homes[which], home_plan[which], home_info[which], *tables, *got_up, *got_down)

        def all_arrived(tables, got_up, got_down, scaled):
            theirs = arrived(0, tables, got_up, got_down, scaled)
            mine = arrived(1, after(tables, theirs), got_up, got_down, scaled)
            theirs = mate(theirs)
            return jnp.where(core == 0, jnp.concatenate([mine, theirs], axis=1), jnp.concatenate([theirs, mine], axis=1))

        def shift(up_rows, down_rows):
            got_up = lax.ppermute(up_rows, 'expert', to_next)
            got_down = lax.ppermute(down_rows, 'expert', to_prev)
            return got_up, got_down

        def second_rows(got, up_rows, down_rows):
            row = iota((up_rows.shape[0], 1), 0)
            return jnp.where(row < pass_up, got[0], up_rows), jnp.where(row < pass_down, got[1], down_rows)

        def table(v):
            return v.reshape(group, cap, half)

        x = take(onehot_in, all_x)
        pre_a, pre_b, hid = up_front(x)
        theirs = dot('cf,fd->cd', hid, w2_halves[1]).astype(BF)
        out_got = mate(theirs)
        ours = dot('cf,fd->cd', after(hid, theirs), w2_halves[0]).astype(BF)
        out_tables = (table(ours), table(out_got))
        out_up, out_down = packed(out_tables, stage, True)
        cut = [(out_up[0][:size], out_down[0][:size]) for size in tiers[:-1]] + [(out_up[0], out_down[0])]
        all_dy = after(all_dy, out_up, out_down, cut)

        def block_spec(rows, width):
            return pl.BlockSpec((1, rows, width), lambda e, *tables: (e, 0, 0))

        def fixed_spec(w):
            return pl.BlockSpec(w.shape, lambda e, *tables: (0, 0), pipeline_mode=pl.Buffered(1))

        def inner_grads_of(dy):
            f = pre_a.shape[1]
            return pl.pallas_call(
                inner_kernel,
                grid_spec=pltpu.PrefetchScalarGridSpec(
                    num_scalar_prefetch=2, grid=(group,),
                    in_specs=[block_spec(8, toks), block_spec(toks, dim), fixed_spec(w2t), block_spec(cap, f), block_spec(cap, f)],
                    out_specs=[block_spec(cap, dim), block_spec(cap, f), block_spec(cap, f)]),
                out_shape=[jax.ShapeDtypeStruct((group, cap, n), BF) for n in (dim, f, f)],
                compiler_params=pltpu.CompilerParams(vmem_limit_bytes=VMEM_LIMIT),
                cost_estimate=pl.CostEstimate(flops=2 * rows * dim * (toks + f), bytes_accessed=2 * rows * dim * 4, transcendentals=rows * f),
                name='inner',
            )(counts, froms, own_info, dy, w2t, pre_a.reshape(group, cap, f), pre_b.reshape(group, cap, f))

        def input_grad(da, db, k):
            w1t, w3t = w13t_halves[k]
            f = da.shape[2]
            return pl.pallas_call(
                input_kernel,
                grid_spec=pltpu.PrefetchScalarGridSpec(
                    num_scalar_prefetch=1, grid=(group,),
                    in_specs=[block_spec(cap, f), block_spec(cap, f), fixed_spec(w1t), fixed_spec(w3t)],
                    out_specs=block_spec(cap, half)),
                out_shape=jax.ShapeDtypeStruct((group, cap, half), BF),
                compiler_params=pltpu.CompilerParams(vmem_limit_bytes=VMEM_LIMIT),
                cost_estimate=pl.CostEstimate(flops=4 * rows * f * half, bytes_accessed=4 * rows * half, transcendentals=0),
                name='input_grad',
            )(counts, da, db, w1t, w3t)

        def rest(tier):
            size = tiers[tier]
            out_first = shift(*cut[tier])
            g, da, db = inner_grads_of(all_dy)
            theirs = input_grad(da, db, 1)
            dx_got = mate(theirs)
            out_second = second_rows(after(out_first, theirs), out_up[1][:size], out_down[1][:size])
            out_last = shift(*out_second)
            ours = input_grad(*after((da, db), *out_second), 0)
            dx_tables = (ours, dx_got)
            dx_up, dx_down = packed(dx_tables, size, False)
            dx_first = shift(dx_up[0], dx_down[0])
            out_first, out_last, da, db, g = after((out_first, out_last, da, db, g), dx_up, dx_down)
            f = da.shape[2]
            da, db, g = da.reshape(rows, f), db.reshape(rows, f), g.reshape(rows, dim)
            dw1 = dot('cd,cf->df', x, da)
            out_first, out_last = after((out_first, out_last), dw1[:8, :TILE])
            y = all_arrived(out_tables, (out_first[0], out_last[0]), (out_first[1], out_last[1]), True)
            dx_second = second_rows(after(dx_first, y), dx_up[1], dx_down[1])
            dx_last = shift(*dx_second)
            db, hid_late = after((db, hid), *dx_second)
            dw3 = dot('cd,cf->df', x, db)
            dw2 = dot('cf,cd->fd', hid_late, g)
            gx = all_arrived(dx_tables, (dx_first[0], dx_last[0]), (dx_first[1], dx_last[1]), False)
            return y, gx, row_major(dw1)[None], row_major(dw3)[None], row_major(dw2)[None]

        def general():
            my_rank, my_taken = pick(rank, me), pick(taken.astype(I32), me) > 0
            my_idx = route_idx.T
            home_rank = pick(jnp.moveaxis(rank, 1, 0), me)
            out_rank = jnp.stack([jnp.sum(jnp.where(my_idx[j] == expert_id[:, 0], home_rank, 0), axis=0) for j in range(tops)])
            out_hot = my_idx % stride == 0

            def one_pass(first):
                ok = my_taken & (my_rank >= first) & (my_rank < first + cap)
                ok_out = (out_rank >= first) & (out_rank < first + cap)
                if first:
                    ok = ok & (me % stride == 0)
                    ok_out = ok_out & out_hot
                onehot = jnp.where(ok, my_rank - first, -1)[:, None, :] == iota((1, cap, 1), 1)
                gate = jnp.sum(jnp.where(onehot, own_gate[:, None, :], 0.0), axis=2)
                onehot = onehot.astype(BF)
                goal = jnp.where(ok_out, my_idx * cap + out_rank - first, -1)
                onehot_out = (goal[:, :, None] == iota((1, 1, rows), 2)).astype(BF)

                def swap(r):
                    return lax.all_to_all(r.reshape(group, cap, dim), 'expert', 0, 0).reshape(rows, dim)

                x = take(onehot, all_x)
                pre_a, pre_b, hid = up_front(x)
                back = swap(dot('cf,fd->cd', hid, w2).astype(BF))
                g = lax.optimization_barrier(take(onehot, all_dy, gate))
                da, db = lax.optimization_barrier(inner_grads(pre_a, pre_b, dot('cd,fd->cf', g, w2)))
                dx = (dot('cf,df->cd', da, w1) + dot('cf,df->cd', db, w3)).astype(BF)
                back_dx = swap(after(dx, back))
                slots = dot('jtr,rd->jtd', onehot_out, back)
                y = jnp.sum(route_gate.T[:, :, None] * slots, axis=0)
                gx = dot('tr,rd->td', jnp.sum(onehot_out, axis=0), back_dx)
                return y, gx, dot('cd,cf->df', x, da), dot('cd,cf->df', x, db), dot('cf,cd->fd', hid, g)

            first = one_pass(0)
            second = one_pass(cap)
            sums = [u + v for u, v in zip(first, second)]
            return sums[0].astype(BF), sums[1].astype(BF), *[v[None] for v in sums[2:]]

        branches = [functools.partial(rest, tier) for tier in range(len(tiers))] + [general]
        return lax.switch(state, branches)

    return jax.shard_map(layer, mesh=mesh, in_specs=(tok_spec,) * 4 + (w_spec,) * 3, out_specs=(tok_spec,) * 5, check_vma=False)
```

```python
import functools

import jax
import jax.numpy as jnp
from jax import lax
from jax.experimental import pallas as pl
from jax.experimental.layout import Layout, with_layout_constraint
from jax.experimental.pallas import tpu as pltpu
from jax.sharding import PartitionSpec as P

BF = jnp.bfloat16
F32 = jnp.float32
I32 = jnp.int32
PIECE = 16
TILE = 128
SPAN = 256
ROOM = 512
VMEM_LIMIT = 50 * 2 ** 20


def dot(form, a, b):
    return jnp.einsum(form, a, b, preferred_element_type=F32)


def iota(shape, axis):
    return lax.broadcasted_iota(I32, shape, axis)


def count_before(mask):
    n = mask.shape[-1]
    earlier = iota((n, n), 0) < iota((n, n), 1)
    return dot('...u,us->...s', mask.astype(BF), earlier.astype(BF)).astype(I32)


def pick(table, index):
    sel = iota(table.shape, 0) == index
    return jnp.sum(jnp.where(sel, table, jnp.zeros_like(table)), axis=0)


def row_major(v):
    return with_layout_constraint(v, Layout(major_to_minor=tuple(range(v.ndim))))


def after(value, *others):
    return lax.optimization_barrier((value,) + others)[0]


def pack_kernel(scaled, dev_ref, seg_ref, low_ref, tab0, tab1, cols, *refs):
    outs, (buf, pend, sem) = (refs[0:2], refs[2:4]), refs[4:]
    g = pl.program_id(0)
    toks = cols.shape[1]
    length, start, extra, stage = [seg_ref[g, k] for k in range(4)]

    @pl.when(g == 0)
    def _():
        pend[0] = 0
        pend[1] = 0

    def drain(slot):
        def one(_, carry):
            pltpu.make_async_copy(buf.at[0, pl.ds(0, PIECE)], outs[0][0].at[pl.ds(0, PIECE)], sem.at[slot]).wait()
            return carry

        lax.fori_loop(0, pend[slot], one, 0)
        pend[slot] = 0

    def put(slot, p, side, at):
        for late, ref in enumerate(outs[side]):
            @pl.when((at >= stage) == bool(late))
            def _(ref=ref, late=late):
                spot = jnp.minimum(at - stage if late else at, ref.shape[0] - PIECE)
                src = buf.at[slot, pl.ds(pl.multiple_of(p * PIECE, PIECE), PIECE)]
                pltpu.make_async_copy(src, ref.at[pl.ds(pl.multiple_of(spot, PIECE), PIECE)], sem.at[slot]).start()
        pend[slot] = pend[slot] + 1

    def tile(i, carry):
        @pl.when(i * TILE < length)
        def _():
            slot = lax.rem(i, 2)
            drain(slot)
            vals = cols[0, pl.ds(pl.multiple_of(i * TILE, TILE), TILE)]
            lows = [low_ref[g, 2 * i + k] for k in range(2)]

            def part(k, tab):
                at = vals[:, k:k + 1] - lows[k].astype(F32)
                onehot = (at == iota((TILE, SPAN), 1).astype(F32)).astype(BF)
                got = jnp.dot(onehot, tab[0, pl.ds(pl.multiple_of(lows[k], PIECE), SPAN)], preferred_element_type=F32)
                return got * vals[:, 2 + k:3 + k] if scaled else got

            @pl.when((lows[0] >= 0) & (lows[1] < 0))
            def _():
                buf[slot] = part(0, tab0).astype(BF)

            @pl.when((lows[0] < 0) & (lows[1] >= 0))
            def _():
                buf[slot] = part(1, tab1).astype(BF)

            @pl.when((lows[0] >= 0) & (lows[1] >= 0))
            def _():
                buf[slot] = (part(0, tab0) + part(1, tab1)).astype(BF)

            def piece(p, carry):
                q = i * TILE + p * PIECE
                at = start + q
                near = jnp.where(at >= stage, at + extra, at)

                @pl.when((q < length) & (g < 2) & (at < extra))
                def _():
                    put(slot, p, 0, at)

                @pl.when((q < length) & (g < 2) & (at >= extra))
                def _():
                    put(slot, p, 1, at - extra)

                @pl.when((q < length) & (g >= 2) & (g < 4))
                def _():
                    put(slot, p, 0, near)

                @pl.when((q < length) & (g >= 4))
                def _():
                    put(slot, p, 1, near)

                return carry

            lax.fori_loop(0, TILE // PIECE, piece, 0)

        return carry

    lax.fori_loop(0, toks // TILE, tile, 0)

    @pl.when(g == pl.num_programs(0) - 1)
    def _():
        drain(0)
        drain(1)


def arrive_kernel(scaled, home_ref, plan_ref, info, tab0, tab1, up1, up2, down1, down2, out, wbuf, sem):
    t, last = pl.program_id(0), pl.num_programs(0) - 1
    sources = (tab0.at[home_ref[0]], tab1.at[home_ref[0]], up1, up2, up2, down1, down2, down2)

    def pieces(step, do):
        slot = lax.rem(step, 2)
        for w, ref in enumerate(sources):
            begin, count, to = [plan_ref[step, 3 * w + k] for k in range(3)]

            def one(p, carry, ref=ref, begin=begin, to=to):
                src = ref.at[pl.ds(pl.multiple_of(begin + p * PIECE, PIECE), PIECE)]
                do(pltpu.make_async_copy(src, wbuf.at[slot, pl.ds(pl.multiple_of(to + p * PIECE, PIECE), PIECE)], sem.at[slot]))
                return carry

            lax.fori_loop(0, count, one, 0)

    @pl.when(t == 0)
    def _():
        wbuf[...] = jnp.zeros_like(wbuf)
        pieces(0, lambda c: c.start())

    @pl.when(t < last)
    def _():
        pieces(t + 1, lambda c: c.start())

    vals = info[0]
    eye = iota((TILE, TILE), 0) == iota((TILE, TILE), 1)
    lane = iota((TILE, wbuf.shape[1]), 1).astype(F32)

    def column(k):
        return jnp.sum(jnp.where(eye, vals[k:k + 1, :], 0.0), axis=1, keepdims=True)

    first, second = column(0) == lane, column(1) == lane
    pieces(t, lambda c: c.wait())
    rows = wbuf.at[lax.rem(t, 2)]
    if scaled:
        total = column(2) * jnp.dot(first.astype(BF), rows[...], preferred_element_type=F32)
        total = total + column(3) * jnp.dot(second.astype(BF), rows[...], preferred_element_type=F32)
    else:
        total = jnp.dot((first | second).astype(BF), rows[...], preferred_element_type=F32)
    out[...] = total.astype(BF)


def by_count(count, cap, run):
    for n in range(0, cap + 1, TILE):
        @pl.when((count > n - TILE) & (count <= n))
        def _(n=n):
            run(n)


def inner_kernel(count_ref, from_ref, info, dy, w2t, a_ref, b_ref, g_ref, da_ref, db_ref):
    e = pl.program_id(0)
    cap, dim = g_ref.shape[1:]
    toks = dy.shape[1]
    step, narrow = dim // 4, da_ref.shape[2] // 4
    count, begin = count_ref[e], from_ref[e]

    def fill(n, begin, span):
        if n:
            vals = info[0, :, pl.ds(begin, span)]
            match = vals[0:1, :] == iota((n, span), 0).astype(F32)
            gate = jnp.sum(jnp.where(match, vals[1:2, :], 0.0), axis=1, keepdims=True)
            onehot = match.astype(BF)

            def outer(k, carry):
                at = pl.ds(pl.multiple_of(k * step, step), step)
                got = jnp.dot(onehot, dy[0, pl.ds(begin, span), at], preferred_element_type=F32)
                g_ref[0, :n, at] = (gate * got).astype(BF)
                return carry

            lax.fori_loop(0, dim // step, outer, 0)

            def hidden(k, carry):
                at = pl.ds(pl.multiple_of(k * narrow, narrow), narrow)
                dh = jnp.dot(g_ref[0, :n], w2t[:, at], preferred_element_type=F32).astype(BF).astype(F32)
                a, b = a_ref[0, :n, at].astype(F32), b_ref[0, :n, at].astype(F32)
                sig = jax.nn.sigmoid(a)
                da_ref[0, :n, at] = (dh * b * (sig * (1.0 + a * (1.0 - sig)))).astype(BF)
                db_ref[0, :n, at] = (dh * (a * sig)).astype(BF)
                return carry

            lax.fori_loop(0, da_ref.shape[2] // narrow, hidden, 0)
        if n < cap:
            for ref in (g_ref, da_ref, db_ref):
                ref[0, n:] = jnp.zeros((cap - n, ref.shape[2]), BF)

    @pl.when(begin >= 0)
    def _():
        by_count(count, cap, lambda n: fill(n, pl.multiple_of(begin, TILE), toks * 2 // 3))

    @pl.when(begin < 0)
    def _():
        fill(cap, 0, toks)


def input_kernel(count_ref, da, db, w1t, w3t, out):
    cap, width = out.shape[1:]
    step = width // 2

    def run(n):
        if n:
            for c in range(0, width, step):
                got = jnp.dot(da[0, :n], w1t[:, c:c + step], preferred_element_type=F32)
                got = got + jnp.dot(db[0, :n], w3t[:, c:c + step], preferred_element_type=F32)
                out[0, :n, c:c + step] = got.astype(BF)
        if n < cap:
            out[0, n:] = jnp.zeros((cap - n, width), BF)

    by_count(count_ref[pl.program_id(0)], cap, run)


def solution(mesh):
    group = mesh.shape['expert']
    chips = group // 2
    tok_spec = P(('data', 'expert'))
    w_spec = P('expert')
    to_mate = [(i, i ^ 1) for i in range(group)]
    to_next = [(i, (i + 2) % group) for i in range(group)]
    to_prev = [(i, (i - 2) % group) for i in range(group)]

    def layer(tok_x, route_idx, route_gate, grad_y, w_gate, w_up, w_down):
        toks, dim = tok_x.shape
        tops = route_idx.shape[1]
        experts = w_gate.shape[0] * group
        stride = experts // min(4, experts // 8)
        cap = max(4, 2 * toks * tops // experts)
        rows = group * cap
        half = dim // 2
        tiles = toks // TILE
        tiers = [toks * n // 48 for n in (49, 54, 60, 71)]
        stage = tiers[-1]
        place = 2 * stage
        me = lax.axis_index('expert')
        chip, core = me // 2, me % 2
        up, down, far = (chip + 1) % chips, (chip + chips - 1) % chips, (chip + 2) % chips
        w1, w3, w2 = w_gate[0], w_up[0], w_down[0]

        def mate(v):
            return lax.ppermute(v, 'expert', to_mate)

        all_x = lax.all_gather(tok_x, 'expert')
        all_dy = lax.all_gather(grad_y, 'expert')

        route = jnp.concatenate([route_idx.astype(F32).T, route_gate.T], axis=0)
        every = lax.all_gather(route, 'expert').swapaxes(0, 1)
        idx, gates = every[:tops].astype(I32), every[tops:]
        expert_id = iota((experts, 1, 1), 0)
        taken = jnp.any(idx[None] == expert_id[:, None], axis=1)
        rank = count_before(taken)
        hot_id = expert_id % stride == 0
        kept = taken & (hot_id | (rank < cap))
        spot = jnp.where(kept, rank, -1)
        need = jnp.any(kept.reshape(chips, 2, group, toks), axis=1)
        single = jnp.sum(need.astype(I32), axis=0) == 1
        listed = jnp.where(need, count_before(need), -1)
        sizes = (jnp.sum(need.astype(I32), axis=2) + PIECE - 1) // PIECE * PIECE
        total = jnp.sum(sizes.reshape(chips, chips, 2), axis=2)

        def turn(table, by):
            return jnp.roll(table, -by, axis=0)

        def hop(by):
            sel = (iota((chips, chips), 0) + by) % chips == iota((chips, chips), 1)
            return jnp.sum(jnp.where(sel, total, 0), axis=1)

        parts = 8
        tries = (parts + 1) ** chips
        share = (iota((chips, tries), 1) // ((parts + 1) ** iota((chips, tries), 0))) % (parts + 1)
        two_hops = hop(2)[:, None]
        go_up = two_hops * share // (parts * PIECE) * PIECE
        go_down = two_hops - go_up
        on_up = hop(1)[:, None] + go_up + turn(go_up, -1)
        on_down = hop(chips - 1)[:, None] + go_down + turn(go_down, 1)
        load = jnp.max(jnp.maximum(jnp.maximum(on_up, on_down), 2 * jnp.maximum(go_up, go_down)), axis=0)
        best = jnp.min(load)
        first_best = jnp.min(jnp.where(load == best, jnp.arange(tries, dtype=I32), tries))
        chosen = jnp.sum(jnp.where(iota((1, tries), 1) == first_best, go_up, 0), axis=1)
        other = hop(2) - chosen
        full = jnp.any(taken & hot_id & (rank >= cap))
        state = sum([(best > 2 * size).astype(I32) for size in tiers])
        state = lax.pmax(jnp.where(full, len(tiers), state), ('data', 'expert'))

        def gate_of(eid):
            return jnp.sum(jnp.where(idx == eid, gates, 0.0), axis=0)

        own_spot, mate_spot = pick(spot, me), pick(spot, me ^ 1)
        own_gate, mate_gate = gate_of(me), gate_of(me ^ 1)
        f_up, f_down = pick(chosen, chip), pick(other, chip)
        pass_up, pass_down = pick(chosen, down), pick(other, up)
        my_sizes = pick(sizes, chip)
        devs = jnp.stack([2 * to + k for to in (far, up, down) for k in range(2)])

        def lowest(at, ok):
            low = jnp.min(jnp.where(ok & (at >= 0), at, cap), axis=-1)
            return jnp.where(low < cap, jnp.minimum(low // PIECE * PIECE, cap - SPAN), -1)

        list_tile = (pick(listed, chip) // TILE)[None] == iota((tiles, 1, 1), 0)
        list_tile = list_tile & (pick(listed, chip) >= 0)[None]
        lows = jnp.stack([lowest(v[None], list_tile) for v in (own_spot, mate_spot)], axis=2)
        lows = lows.swapaxes(0, 1).reshape(group, 2 * tiles)
        low_rows = jnp.concatenate([lax.dynamic_slice_in_dim(lows, 2 * to, 2, 0) for to in (far, up, down)])

        def segments(size_of_stage):
            segs = []
            for to, lead, extra in ((far, 0, f_up), (up, f_up, pass_up), (down, f_down, pass_down)):
                for k in range(2):
                    size = pick(my_sizes, 2 * to + k)
                    segs.append(jnp.stack([size, jnp.asarray(lead, I32), extra, jnp.asarray(size_of_stage, I32)]))
                    lead = lead + size
            return jnp.stack(segs)

        def of_chips(v):
            return jnp.concatenate([lax.dynamic_slice_in_dim(v, 2 * to, 2, 0) for to in (far, up, down)])

        def thirds(v):
            high = v.astype(BF)
            middle = (v - high.astype(F32)).astype(BF)
            return [high, middle, (v - high.astype(F32) - middle.astype(F32)).astype(BF)]

        values = []
        for v in (own_spot, mate_spot):
            v = of_chips(v) + 1
            values += [(v // 256).astype(BF), (v % 256).astype(BF)]
        for v in (own_gate, mate_gate):
            values += thirds(of_chips(jnp.where(single, v, 1.0)))
        in_list = of_chips(pick(listed, chip))[:, None, :] == iota((1, toks, 1), 1)
        got = dot('gqs,gsk->gqk', in_list.astype(BF), jnp.stack(values, axis=2))
        list_cols = [got[:, :, 2 * k] * 256.0 + got[:, :, 2 * k + 1] - 1.0 for k in range(2)]
        list_cols += [got[:, :, 4 + 3 * k] + got[:, :, 5 + 3 * k] + got[:, :, 6 + 3 * k] for k in range(2)]
        list_cols = jnp.stack(list_cols + [jnp.zeros_like(list_cols[0])] * 4, axis=2)

        tier_stage = sum([jnp.where(state == k, size, 0) for k, size in enumerate(tiers)]) + jnp.where(state == len(tiers), stage, 0)
        segs = segments(tier_stage)

        def home(v):
            v = lax.dynamic_slice_in_dim(v, 2 * chip, 2, 0)
            return jnp.where(core == 0, v[::-1], v)

        home_core = jnp.where((core == 0) == (iota((2, 1), 0) == 0), 1, 0)
        home_idx = [home(idx[j]) for j in range(tops)]
        home_gates = [home(gates[j]) for j in range(tops)]
        home_kept = home(jnp.sum(kept.astype(I32) * (1 << expert_id), axis=0))
        home_single = home(single.astype(I32)) > 0

        def listed_at(c):
            at = home(pick(listed, c))
            first = pick(pick(sizes, c), 2 * chip)
            return at >= 0, at + jnp.where(home_core == 1, first, 0)

        def weight_of(c):
            w = 0.0
            for j in range(tops):
                held = (home_kept >> home_idx[j]) % 2 == 1
                w = w + jnp.where((home_idx[j] // 2 == c) & held, home_gates[j], 0.0)
            return jnp.where(home_single, 1.0, w)

        def near_spots(c, lead, passed):
            ok, at = listed_at(c)
            at = at + lead
            late = at >= tier_stage
            return [jnp.where(ok & jnp.logical_not(late), at, -1), jnp.where(ok & late, at + passed - tier_stage, -1)]

        far_ok, far_at = listed_at(far)
        far_cut = pick(chosen, far)
        spots = [home(own_spot), home(mate_spot)]
        spots += near_spots(down, pick(chosen, down), pick(chosen, far)) + [jnp.where(far_ok & (far_at < far_cut), far_at, -1)]
        spots += near_spots(up, pick(other, up), pick(other, far)) + [jnp.where(far_ok & (far_at >= far_cut), far_at - far_cut, -1)]
        w_down, w_up, w_far = [weight_of(c) for c in (down, up, far)]
        weights = [home(own_gate), home(mate_gate), w_down, w_down, w_far, w_up, w_up, w_far]
        spots = jnp.stack(spots).reshape(8, 2 * tiles, TILE)
        weights = jnp.stack(weights).reshape(8, 2 * tiles, TILE)
        there = spots >= 0
        begin = jnp.min(jnp.where(there, spots, place), axis=2) // PIECE * PIECE
        count = jnp.maximum(jnp.max(spots, axis=2) - begin + PIECE, 0) // PIECE
        to = jnp.cumsum(count, axis=0) * PIECE - count * PIECE
        at = jnp.where(there, spots + (to - begin)[:, :, None], -1)
        first = jnp.max(at, axis=0)
        second = jnp.sum(at + 1, axis=0) - first - 2
        w_first = jnp.sum(jnp.where(there & (at == first[None]), weights, 0.0), axis=0)
        w_second = jnp.sum(jnp.where(there & (at == second[None]), weights, 0.0), axis=0)
        home_info = [first.astype(F32), second.astype(F32), w_first, w_second]
        home_info = jnp.stack(home_info + [jnp.zeros_like(w_first)] * 4, axis=1).reshape(2, tiles, 8, TILE)
        home_plan = jnp.stack([begin, count, to], axis=1).reshape(24, 2 * tiles).T.reshape(2, tiles, 24)
        homes = 2 * chip + home_core

        onehot_in = (own_spot[:, None, :] == iota((1, cap, 1), 1)).astype(BF)

        def columns(w, axis, mine):
            parts = jnp.split(w, 2, axis=axis)
            return jnp.where((core == 0) == mine, parts[0], parts[1])

        w2_halves = [columns(w2, 1, m) for m in (True, False)]
        w2t = row_major(w2.T)
        w13t_halves = [[row_major(columns(w, 0, m).T) for w in (w1, w3)] for m in (True, False)]
        counts = jnp.sum((own_spot >= 0).astype(I32), axis=1)
        pad = jnp.zeros((group, toks), F32)
        own_info = jnp.stack([own_spot.astype(F32), own_gate] + [pad] * 6, axis=1)
        span = toks * 2 // 3
        s_first = jnp.min(jnp.where(own_spot >= 0, iota(own_spot.shape, 1), toks), axis=1)
        s_last = jnp.max(jnp.where(own_spot >= 0, iota(own_spot.shape, 1), 0), axis=1)
        froms = jnp.minimum(s_first // TILE * TILE, toks - span)
        froms = jnp.where(s_last < froms + span, froms, -1)
        plan = (state, list_cols, devs, segs, low_rows, home_info, home_plan, homes, onehot_in, counts, froms, own_info, w2_halves, w2t, w13t_halves)
        plan = lax.optimization_barrier(plan)
        all_x, plan = lax.optimization_barrier((all_x, plan))
        (state, list_cols, devs, segs, low_rows, home_info, home_plan, homes, onehot_in, counts, froms, own_info, w2_halves, w2t,
         w13t_halves) = plan

        def take(onehot, tok, gate=None):
            got = dot('gcs,gsd->gcd', onehot, tok)
            return (got if gate is None else gate.reshape(group, cap, 1) * got).astype(BF).reshape(rows, dim)

        def up_front(x):
            pre_a = dot('cd,df->cf', x, w1).astype(BF)
            pre_b = dot('cd,df->cf', x, w3).astype(BF)
            pre_a, pre_b = lax.optimization_barrier((pre_a, pre_b))
            a = pre_a.astype(F32)
            hid = (a * jax.nn.sigmoid(a) * pre_b.astype(F32)).astype(BF)
            return pre_a, pre_b, hid

        def inner_grads(pre_a, pre_b, dh):
            dh = dh.astype(BF).astype(F32)
            a = pre_a.astype(F32)
            sig = jax.nn.sigmoid(a)
            da = (dh * pre_b.astype(F32) * (sig * (1.0 + a * (1.0 - sig)))).astype(BF)
            db = (dh * (a * sig)).astype(BF)
            return da, db

        any_spec = pl.BlockSpec(memory_space=pl.ANY)

        def packed(tables, size, scaled):
            table_spec = pl.BlockSpec((1, cap, half), lambda g, dev, seg, low: (dev[g], 0, 0))
            res = pl.pallas_call(
                functools.partial(pack_kernel, scaled),
                grid_spec=pltpu.PrefetchScalarGridSpec(
                    num_scalar_prefetch=3, grid=(6,),
                    in_specs=[table_spec, table_spec, pl.BlockSpec((1, toks, 8), lambda g, dev, seg, low: (g, 0, 0))],
                    out_specs=[any_spec] * 4,
                    scratch_shapes=[pltpu.VMEM((2, TILE, half), BF), pltpu.SMEM((2,), I32),
                                    pltpu.SemaphoreType.DMA((2,))]),
                out_shape=[jax.ShapeDtypeStruct((size, half), BF)] * 4,
                compiler_params=pltpu.CompilerParams(vmem_limit_bytes=VMEM_LIMIT),
                cost_estimate=pl.CostEstimate(flops=2 * rows * cap * half, bytes_accessed=12 * rows * half, transcendentals=0),
                name='pack',
            )(devs, segs, low_rows, *tables, list_cols)
            return res[:2], res[2:]

        def arrived(which, tables, got_up, got_down, scaled):
            return pl.pallas_call(
                functools.partial(arrive_kernel, scaled),
                grid_spec=pltpu.PrefetchScalarGridSpec(
                    num_scalar_prefetch=2, grid=(tiles,),
                    in_specs=[pl.BlockSpec((1, 8, TILE), lambda t, homes, plan: (t, 0, 0))] + [any_spec] * 6,
                    out_specs=pl.BlockSpec((TILE, half), lambda t, homes, plan: (t, 0)),
                    scratch_shapes=[pltpu.VMEM((2, ROOM, half), BF), pltpu.SemaphoreType.DMA((2,))]),
                out_shape=jax.ShapeDtypeStruct((toks, half), BF),
                compiler_params=pltpu.CompilerParams(vmem_limit_bytes=VMEM_LIMIT),
                cost_estimate=pl.CostEstimate(flops=2 * rows * cap * half, bytes_accessed=6 * rows * half, transcendentals=0),
                name='arrive',
            )(homes[which], home_plan[which], home_info[which], *tables, *got_up, *got_down)

        def all_arrived(tables, got_up, got_down, scaled):
            theirs = arrived(0, tables, got_up, got_down, scaled)
            mine = arrived(1, after(tables, theirs), got_up, got_down, scaled)
            theirs = mate(theirs)
            return jnp.where(core == 0, jnp.concatenate([mine, theirs], axis=1), jnp.concatenate([theirs, mine], axis=1))

        def shift(up_rows, down_rows):
            got_up = lax.ppermute(up_rows, 'expert', to_next)
            got_down = lax.ppermute(down_rows, 'expert', to_prev)
            return got_up, got_down

        def second_rows(got, up_rows, down_rows):
            row = iota((up_rows.shape[0], 1), 0)
            return jnp.where(row < pass_up, got[0], up_rows), jnp.where(row < pass_down, got[1], down_rows)

        def table(v):
            return v.reshape(group, cap, half)

        x = take(onehot_in, all_x)
        pre_a, pre_b, hid = up_front(x)
        theirs = dot('cf,fd->cd', hid, w2_halves[1]).astype(BF)
        out_got = mate(theirs)
        ours = dot('cf,fd->cd', after(hid, theirs), w2_halves[0]).astype(BF)
        out_tables = (table(ours), table(out_got))
        out_up, out_down = packed(out_tables, stage, True)
        cut = [(out_up[0][:size], out_down[0][:size]) for size in tiers[:-1]] + [(out_up[0], out_down[0])]
        all_dy = after(all_dy, out_up, out_down, cut)

        def block_spec(rows, width):
            return pl.BlockSpec((1, rows, width), lambda e, *tables: (e, 0, 0))

        def fixed_spec(w):
            return pl.BlockSpec(w.shape, lambda e, *tables: (0, 0), pipeline_mode=pl.Buffered(1))

        def inner_grads_of(dy):
            f = pre_a.shape[1]
            return pl.pallas_call(
                inner_kernel,
                grid_spec=pltpu.PrefetchScalarGridSpec(
                    num_scalar_prefetch=2, grid=(group,),
                    in_specs=[block_spec(8, toks), block_spec(toks, dim), fixed_spec(w2t), block_spec(cap, f), block_spec(cap, f)],
                    out_specs=[block_spec(cap, dim), block_spec(cap, f), block_spec(cap, f)]),
                out_shape=[jax.ShapeDtypeStruct((group, cap, n), BF) for n in (dim, f, f)],
                compiler_params=pltpu.CompilerParams(vmem_limit_bytes=VMEM_LIMIT),
                cost_estimate=pl.CostEstimate(flops=2 * rows * dim * (toks + f), bytes_accessed=2 * rows * dim * 4, transcendentals=rows * f),
                name='inner',
            )(counts, froms, own_info, dy, w2t, pre_a.reshape(group, cap, f), pre_b.reshape(group, cap, f))

        def input_grad(da, db, k):
            w1t, w3t = w13t_halves[k]
            f = da.shape[2]
            return pl.pallas_call(
                input_kernel,
                grid_spec=pltpu.PrefetchScalarGridSpec(
                    num_scalar_prefetch=1, grid=(group,),
                    in_specs=[block_spec(cap, f), block_spec(cap, f), fixed_spec(w1t), fixed_spec(w3t)],
                    out_specs=block_spec(cap, half)),
                out_shape=jax.ShapeDtypeStruct((group, cap, half), BF),
                compiler_params=pltpu.CompilerParams(vmem_limit_bytes=VMEM_LIMIT),
                cost_estimate=pl.CostEstimate(flops=4 * rows * f * half, bytes_accessed=4 * rows * half, transcendentals=0),
                name='input_grad',
            )(counts, da, db, w1t, w3t)

        def rest(tier):
            size = tiers[tier]
            out_first = shift(*cut[tier])
            g, da, db = inner_grads_of(all_dy)
            out_second = second_rows(after(out_first, da), out_up[1][:size], out_down[1][:size])
            out_last = shift(*out_second)
            da, db = after((da, db), *out_second)
            theirs = input_grad(da, db, 1)
            dx_got = mate(theirs)
            ours = input_grad(after(da, theirs), db, 0)
            dx_tables = (ours, dx_got)
            dx_up, dx_down = packed(dx_tables, size, False)
            dx_first = shift(dx_up[0], dx_down[0])
            out_first, out_last, da, db, g = after((out_first, out_last, da, db, g), dx_up, dx_down)
            f = da.shape[2]
            da, db, g = da.reshape(rows, f), db.reshape(rows, f), g.reshape(rows, dim)
            dw1 = dot('cd,cf->df', x, da)
            out_first, out_last = after((out_first, out_last), dw1[:8, :TILE])
            y = all_arrived(out_tables, (out_first[0], out_last[0]), (out_first[1], out_last[1]), True)
            dx_second = second_rows(after(dx_first, y), dx_up[1], dx_down[1])
            dx_last = shift(*dx_second)
            db, hid_late = after((db, hid), *dx_second)
            dw3 = dot('cd,cf->df', x, db)
            dw2 = dot('cf,cd->fd', hid_late, g)
            gx = all_arrived(dx_tables, (dx_first[0], dx_last[0]), (dx_first[1], dx_last[1]), False)
            return y, gx, row_major(dw1)[None], row_major(dw3)[None], row_major(dw2)[None]

        def general():
            my_rank, my_taken = pick(rank, me), pick(taken.astype(I32), me) > 0
            my_idx = route_idx.T
            home_rank = pick(jnp.moveaxis(rank, 1, 0), me)
            out_rank = jnp.stack([jnp.sum(jnp.where(my_idx[j] == expert_id[:, 0], home_rank, 0), axis=0) for j in range(tops)])
            out_hot = my_idx % stride == 0

            def one_pass(first):
                ok = my_taken & (my_rank >= first) & (my_rank < first + cap)
                ok_out = (out_rank >= first) & (out_rank < first + cap)
                if first:
                    ok = ok & (me % stride == 0)
                    ok_out = ok_out & out_hot
                onehot = jnp.where(ok, my_rank - first, -1)[:, None, :] == iota((1, cap, 1), 1)
                gate = jnp.sum(jnp.where(onehot, own_gate[:, None, :], 0.0), axis=2)
                onehot = onehot.astype(BF)
                goal = jnp.where(ok_out, my_idx * cap + out_rank - first, -1)
                onehot_out = (goal[:, :, None] == iota((1, 1, rows), 2)).astype(BF)

                def swap(r):
                    return lax.all_to_all(r.reshape(group, cap, dim), 'expert', 0, 0).reshape(rows, dim)

                x = take(onehot, all_x)
                pre_a, pre_b, hid = up_front(x)
                back = swap(dot('cf,fd->cd', hid, w2).astype(BF))
                g = lax.optimization_barrier(take(onehot, all_dy, gate))
                da, db = lax.optimization_barrier(inner_grads(pre_a, pre_b, dot('cd,fd->cf', g, w2)))
                dx = (dot('cf,df->cd', da, w1) + dot('cf,df->cd', db, w3)).astype(BF)
                back_dx = swap(after(dx, back))
                slots = dot('jtr,rd->jtd', onehot_out, back)
                y = jnp.sum(route_gate.T[:, :, None] * slots, axis=0)
                gx = dot('tr,rd->td', jnp.sum(onehot_out, axis=0), back_dx)
                return y, gx, dot('cd,cf->df', x, da), dot('cd,cf->df', x, db), dot('cf,cd->fd', hid, g)

            first = one_pass(0)
            second = one_pass(cap)
            sums = [u + v for u, v in zip(first, second)]
            return sums[0].astype(BF), sums[1].astype(BF), *[v[None] for v in sums[2:]]

        branches = [functools.partial(rest, tier) for tier in range(len(tiers))] + [general]
        return lax.switch(state, branches)

    return jax.shard_map(layer, mesh=mesh, in_specs=(tok_spec,) * 4 + (w_spec,) * 3, out_specs=(tok_spec,) * 5, check_vma=False)
```

```python
import functools

import jax
import jax.numpy as jnp
from jax import lax
from jax.experimental import pallas as pl
from jax.experimental.layout import Layout, with_layout_constraint
from jax.experimental.pallas import tpu as pltpu
from jax.sharding import PartitionSpec as P

BF = jnp.bfloat16
F32 = jnp.float32
I32 = jnp.int32
PIECE = 16
TILE = 128
SPAN = 256
ROOM = 512
VMEM_LIMIT = 50 * 2 ** 20


def dot(form, a, b):
    return jnp.einsum(form, a, b, preferred_element_type=F32)


def iota(shape, axis):
    return lax.broadcasted_iota(I32, shape, axis)


def count_before(mask):
    n = mask.shape[-1]
    earlier = iota((n, n), 0) < iota((n, n), 1)
    return dot('...u,us->...s', mask.astype(BF), earlier.astype(BF)).astype(I32)


def pick(table, index):
    sel = iota(table.shape, 0) == index
    return jnp.sum(jnp.where(sel, table, jnp.zeros_like(table)), axis=0)


def row_major(v):
    return with_layout_constraint(v, Layout(major_to_minor=tuple(range(v.ndim))))


def after(value, *others):
    return lax.optimization_barrier((value,) + others)[0]


def pack_kernel(scaled, dev_ref, seg_ref, low_ref, tab0, tab1, cols, *refs):
    outs, (buf, pend, sem) = (refs[0:2], refs[2:4]), refs[4:]
    g = pl.program_id(0)
    toks = cols.shape[1]
    length, start, extra, stage = [seg_ref[g, k] for k in range(4)]

    @pl.when(g == 0)
    def _():
        pend[0] = 0
        pend[1] = 0

    def drain(slot):
        def one(_, carry):
            pltpu.make_async_copy(buf.at[0, pl.ds(0, PIECE)], outs[0][0].at[pl.ds(0, PIECE)], sem.at[slot]).wait()
            return carry

        lax.fori_loop(0, pend[slot], one, 0)
        pend[slot] = 0

    def put(slot, p, side, at):
        for late, ref in enumerate(outs[side]):
            @pl.when((at >= stage) == bool(late))
            def _(ref=ref, late=late):
                spot = jnp.minimum(at - stage if late else at, ref.shape[0] - PIECE)
                src = buf.at[slot, pl.ds(pl.multiple_of(p * PIECE, PIECE), PIECE)]
                pltpu.make_async_copy(src, ref.at[pl.ds(pl.multiple_of(spot, PIECE), PIECE)], sem.at[slot]).start()
        pend[slot] = pend[slot] + 1

    def tile(i, carry):
        @pl.when(i * TILE < length)
        def _():
            slot = lax.rem(i, 2)
            drain(slot)
            vals = cols[0, pl.ds(pl.multiple_of(i * TILE, TILE), TILE)]
            lows = [low_ref[g, 2 * i + k] for k in range(2)]

            def part(k, tab):
                at = vals[:, k:k + 1] - lows[k].astype(F32)
                onehot = (at == iota((TILE, SPAN), 1).astype(F32)).astype(BF)
                got = jnp.dot(onehot, tab[0, pl.ds(pl.multiple_of(lows[k], PIECE), SPAN)], preferred_element_type=F32)
                return got * vals[:, 2 + k:3 + k] if scaled else got

            @pl.when((lows[0] >= 0) & (lows[1] < 0))
            def _():
                buf[slot] = part(0, tab0).astype(BF)

            @pl.when((lows[0] < 0) & (lows[1] >= 0))
            def _():
                buf[slot] = part(1, tab1).astype(BF)

            @pl.when((lows[0] >= 0) & (lows[1] >= 0))
            def _():
                buf[slot] = (part(0, tab0) + part(1, tab1)).astype(BF)

            def piece(p, carry):
                q = i * TILE + p * PIECE
                at = start + q
                near = jnp.where(at >= stage, at + extra, at)

                @pl.when((q < length) & (g < 2) & (at < extra))
                def _():
                    put(slot, p, 0, at)

                @pl.when((q < length) & (g < 2) & (at >= extra))
                def _():
                    put(slot, p, 1, at - extra)

                @pl.when((q < length) & (g >= 2) & (g < 4))
                def _():
                    put(slot, p, 0, near)

                @pl.when((q < length) & (g >= 4))
                def _():
                    put(slot, p, 1, near)

                return carry

            lax.fori_loop(0, TILE // PIECE, piece, 0)

        return carry

    lax.fori_loop(0, toks // TILE, tile, 0)

    @pl.when(g == pl.num_programs(0) - 1)
    def _():
        drain(0)
        drain(1)


def arrive_kernel(scaled, home_ref, plan_ref, info, tab0, tab1, up1, up2, down1, down2, out, wbuf, sem):
    t, last = pl.program_id(0), pl.num_programs(0) - 1
    sources = (tab0.at[home_ref[0]], tab1.at[home_ref[0]], up1, up2, up2, down1, down2, down2)

    def pieces(step, do):
        slot = lax.rem(step, 2)
        for w, ref in enumerate(sources):
            begin, count, to = [plan_ref[step, 3 * w + k] for k in range(3)]

            def one(p, carry, ref=ref, begin=begin, to=to):
                src = ref.at[pl.ds(pl.multiple_of(begin + p * PIECE, PIECE), PIECE)]
                do(pltpu.make_async_copy(src, wbuf.at[slot, pl.ds(pl.multiple_of(to + p * PIECE, PIECE), PIECE)], sem.at[slot]))
                return carry

            lax.fori_loop(0, count, one, 0)

    @pl.when(t == 0)
    def _():
        wbuf[...] = jnp.zeros_like(wbuf)
        pieces(0, lambda c: c.start())

    @pl.when(t < last)
    def _():
        pieces(t + 1, lambda c: c.start())

    vals = info[0]
    eye = iota((TILE, TILE), 0) == iota((TILE, TILE), 1)
    lane = iota((TILE, wbuf.shape[1]), 1).astype(F32)

    def column(k):
        return jnp.sum(jnp.where(eye, vals[k:k + 1, :], 0.0), axis=1, keepdims=True)

    first, second = column(0) == lane, column(1) == lane
    pieces(t, lambda c: c.wait())
    rows = wbuf.at[lax.rem(t, 2)]
    if scaled:
        total = column(2) * jnp.dot(first.astype(BF), rows[...], preferred_element_type=F32)
        total = total + column(3) * jnp.dot(second.astype(BF), rows[...], preferred_element_type=F32)
    else:
        total = jnp.dot((first | second).astype(BF), rows[...], preferred_element_type=F32)
    out[...] = total.astype(BF)


def by_count(count, cap, run):
    for n in range(0, cap + 1, TILE):
        @pl.when((count > n - TILE) & (count <= n))
        def _(n=n):
            run(n)


def inner_kernel(count_ref, from_ref, info, dy, w2t, a_ref, b_ref, g_ref, da_ref, db_ref):
    e = pl.program_id(0)
    cap, dim = g_ref.shape[1:]
    toks = dy.shape[1]
    step, narrow = dim // 4, da_ref.shape[2] // 4
    count, begin = count_ref[e], from_ref[e]

    def fill(n, begin, span):
        if n:
            vals = info[0, :, pl.ds(begin, span)]
            match = vals[0:1, :] == iota((n, span), 0).astype(F32)
            gate = jnp.sum(jnp.where(match, vals[1:2, :], 0.0), axis=1, keepdims=True)
            onehot = match.astype(BF)

            def outer(k, carry):
                at = pl.ds(pl.multiple_of(k * step, step), step)
                got = jnp.dot(onehot, dy[0, pl.ds(begin, span), at], preferred_element_type=F32)
                g_ref[0, :n, at] = (gate * got).astype(BF)
                return carry

            lax.fori_loop(0, dim // step, outer, 0)

            def hidden(k, carry):
                at = pl.ds(pl.multiple_of(k * narrow, narrow), narrow)
                dh = jnp.dot(g_ref[0, :n], w2t[:, at], preferred_element_type=F32).astype(BF).astype(F32)
                a, b = a_ref[0, :n, at].astype(F32), b_ref[0, :n, at].astype(F32)
                sig = jax.nn.sigmoid(a)
                da_ref[0, :n, at] = (dh * b * (sig * (1.0 + a * (1.0 - sig)))).astype(BF)
                db_ref[0, :n, at] = (dh * (a * sig)).astype(BF)
                return carry

            lax.fori_loop(0, da_ref.shape[2] // narrow, hidden, 0)
        if n < cap:
            for ref in (g_ref, da_ref, db_ref):
                ref[0, n:] = jnp.zeros((cap - n, ref.shape[2]), BF)

    @pl.when(begin >= 0)
    def _():
        by_count(count, cap, lambda n: fill(n, pl.multiple_of(begin, TILE), toks * 2 // 3))

    @pl.when(begin < 0)
    def _():
        fill(cap, 0, toks)


def input_kernel(count_ref, da, db, w1t, w3t, out):
    cap, width = out.shape[1:]
    step = width // 2

    def run(n):
        if n:
            for c in range(0, width, step):
                got = jnp.dot(da[0, :n], w1t[:, c:c + step], preferred_element_type=F32)
                got = got + jnp.dot(db[0, :n], w3t[:, c:c + step], preferred_element_type=F32)
                out[0, :n, c:c + step] = got.astype(BF)
        if n < cap:
            out[0, n:] = jnp.zeros((cap - n, width), BF)

    by_count(count_ref[pl.program_id(0)], cap, run)


def solution(mesh):
    group = mesh.shape['expert']
    chips = group // 2
    tok_spec = P(('data', 'expert'))
    w_spec = P('expert')
    to_mate = [(i, i ^ 1) for i in range(group)]
    to_next = [(i, (i + 2) % group) for i in range(group)]
    to_prev = [(i, (i - 2) % group) for i in range(group)]

    def layer(tok_x, route_idx, route_gate, grad_y, w_gate, w_up, w_down):
        toks, dim = tok_x.shape
        tops = route_idx.shape[1]
        experts = w_gate.shape[0] * group
        stride = experts // min(4, experts // 8)
        cap = max(4, 2 * toks * tops // experts)
        rows = group * cap
        half = dim // 2
        tiles = toks // TILE
        tiers = [toks * n // 48 for n in (49, 57, 71)]
        stage = tiers[-1]
        place = 2 * stage
        me = lax.axis_index('expert')
        chip, core = me // 2, me % 2
        up, down, far = (chip + 1) % chips, (chip + chips - 1) % chips, (chip + 2) % chips
        w1, w3, w2 = w_gate[0], w_up[0], w_down[0]

        def mate(v):
            return lax.ppermute(v, 'expert', to_mate)

        all_x = lax.all_gather(tok_x, 'expert')
        all_dy = lax.all_gather(grad_y, 'expert')

        route = jnp.concatenate([route_idx.astype(F32).T, route_gate.T], axis=0)
        every = lax.all_gather(route, 'expert').swapaxes(0, 1)
        idx, gates = every[:tops].astype(I32), every[tops:]
        expert_id = iota((experts, 1, 1), 0)
        taken = jnp.any(idx[None] == expert_id[:, None], axis=1)
        rank = count_before(taken)
        hot_id = expert_id % stride == 0
        kept = taken & (hot_id | (rank < cap))
        spot = jnp.where(kept, rank, -1)
        need = jnp.any(kept.reshape(chips, 2, group, toks), axis=1)
        single = jnp.sum(need.astype(I32), axis=0) == 1
        listed = jnp.where(need, count_before(need), -1)
        sizes = (jnp.sum(need.astype(I32), axis=2) + PIECE - 1) // PIECE * PIECE
        total = jnp.sum(sizes.reshape(chips, chips, 2), axis=2)

        def turn(table, by):
            return jnp.roll(table, -by, axis=0)

        def hop(by):
            sel = (iota((chips, chips), 0) + by) % chips == iota((chips, chips), 1)
            return jnp.sum(jnp.where(sel, total, 0), axis=1)

        parts = 8
        tries = (parts + 1) ** chips
        share = (iota((chips, tries), 1) // ((parts + 1) ** iota((chips, tries), 0))) % (parts + 1)
        two_hops = hop(2)[:, None]
        go_up = two_hops * share // (parts * PIECE) * PIECE
        go_down = two_hops - go_up
        on_up = hop(1)[:, None] + go_up + turn(go_up, -1)
        on_down = hop(chips - 1)[:, None] + go_down + turn(go_down, 1)
        load = jnp.max(jnp.maximum(jnp.maximum(on_up, on_down), 2 * jnp.maximum(go_up, go_down)), axis=0)
        best = jnp.min(load)
        first_best = jnp.min(jnp.where(load == best, jnp.arange(tries, dtype=I32), tries))
        chosen = jnp.sum(jnp.where(iota((1, tries), 1) == first_best, go_up, 0), axis=1)
        other = hop(2) - chosen
        full = jnp.any(taken & hot_id & (rank >= cap))
        state = sum([(best > 2 * size).astype(I32) for size in tiers])
        state = lax.pmax(jnp.where(full, len(tiers), state), ('data', 'expert'))

        def gate_of(eid):
            return jnp.sum(jnp.where(idx == eid, gates, 0.0), axis=0)

        own_spot, mate_spot = pick(spot, me), pick(spot, me ^ 1)
        own_gate, mate_gate = gate_of(me), gate_of(me ^ 1)
        f_up, f_down = pick(chosen, chip), pick(other, chip)
        pass_up, pass_down = pick(chosen, down), pick(other, up)
        my_sizes = pick(sizes, chip)
        devs = jnp.stack([2 * to + k for to in (far, up, down) for k in range(2)])

        def lowest(at, ok):
            low = jnp.min(jnp.where(ok & (at >= 0), at, cap), axis=-1)
            return jnp.where(low < cap, jnp.minimum(low // PIECE * PIECE, cap - SPAN), -1)

        list_tile = (pick(listed, chip) // TILE)[None] == iota((tiles, 1, 1), 0)
        list_tile = list_tile & (pick(listed, chip) >= 0)[None]
        lows = jnp.stack([lowest(v[None], list_tile) for v in (own_spot, mate_spot)], axis=2)
        lows = lows.swapaxes(0, 1).reshape(group, 2 * tiles)
        low_rows = jnp.concatenate([lax.dynamic_slice_in_dim(lows, 2 * to, 2, 0) for to in (far, up, down)])

        def segments(size_of_stage):
            segs = []
            for to, lead, extra in ((far, 0, f_up), (up, f_up, pass_up), (down, f_down, pass_down)):
                for k in range(2):
                    size = pick(my_sizes, 2 * to + k)
                    segs.append(jnp.stack([size, jnp.asarray(lead, I32), extra, jnp.asarray(size_of_stage, I32)]))
                    lead = lead + size
            return jnp.stack(segs)

        def of_chips(v):
            return jnp.concatenate([lax.dynamic_slice_in_dim(v, 2 * to, 2, 0) for to in (far, up, down)])

        def thirds(v):
            high = v.astype(BF)
            middle = (v - high.astype(F32)).astype(BF)
            return [high, middle, (v - high.astype(F32) - middle.astype(F32)).astype(BF)]

        values = []
        for v in (own_spot, mate_spot):
            v = of_chips(v) + 1
            values += [(v // 256).astype(BF), (v % 256).astype(BF)]
        for v in (own_gate, mate_gate):
            values += thirds(of_chips(jnp.where(single, v, 1.0)))
        in_list = of_chips(pick(listed, chip))[:, None, :] == iota((1, toks, 1), 1)
        got = dot('gqs,gsk->gqk', in_list.astype(BF), jnp.stack(values, axis=2))
        list_cols = [got[:, :, 2 * k] * 256.0 + got[:, :, 2 * k + 1] - 1.0 for k in range(2)]
        list_cols += [got[:, :, 4 + 3 * k] + got[:, :, 5 + 3 * k] + got[:, :, 6 + 3 * k] for k in range(2)]
        list_cols = jnp.stack(list_cols + [jnp.zeros_like(list_cols[0])] * 4, axis=2)

        tier_stage = sum([jnp.where(state == k, size, 0) for k, size in enumerate(tiers)]) + jnp.where(state == len(tiers), stage, 0)
        segs = segments(tier_stage)

        def home(v):
            v = lax.dynamic_slice_in_dim(v, 2 * chip, 2, 0)
            return jnp.where(core == 0, v[::-1], v)

        home_core = jnp.where((core == 0) == (iota((2, 1), 0) == 0), 1, 0)
        home_idx = [home(idx[j]) for j in range(tops)]
        home_gates = [home(gates[j]) for j in range(tops)]
        home_kept = home(jnp.sum(kept.astype(I32) * (1 << expert_id), axis=0))
        home_single = home(single.astype(I32)) > 0

        def listed_at(c):
            at = home(pick(listed, c))
            first = pick(pick(sizes, c), 2 * chip)
            return at >= 0, at + jnp.where(home_core == 1, first, 0)

        def weight_of(c):
            w = 0.0
            for j in range(tops):
                held = (home_kept >> home_idx[j]) % 2 == 1
                w = w + jnp.where((home_idx[j] // 2 == c) & held, home_gates[j], 0.0)
            return jnp.where(home_single, 1.0, w)

        def near_spots(c, lead, passed):
            ok, at = listed_at(c)
            at = at + lead
            late = at >= tier_stage
            return [jnp.where(ok & jnp.logical_not(late), at, -1), jnp.where(ok & late, at + passed - tier_stage, -1)]

        far_ok, far_at = listed_at(far)
        far_cut = pick(chosen, far)
        spots = [home(own_spot), home(mate_spot)]
        spots += near_spots(down, pick(chosen, down), pick(chosen, far)) + [jnp.where(far_ok & (far_at < far_cut), far_at, -1)]
        spots += near_spots(up, pick(other, up), pick(other, far)) + [jnp.where(far_ok & (far_at >= far_cut), far_at - far_cut, -1)]
        w_down, w_up, w_far = [weight_of(c) for c in (down, up, far)]
        weights = [home(own_gate), home(mate_gate), w_down, w_down, w_far, w_up, w_up, w_far]
        spots = jnp.stack(spots).reshape(8, 2 * tiles, TILE)
        weights = jnp.stack(weights).reshape(8, 2 * tiles, TILE)
        there = spots >= 0
        begin = jnp.min(jnp.where(there, spots, place), axis=2) // PIECE * PIECE
        count = jnp.maximum(jnp.max(spots, axis=2) - begin + PIECE, 0) // PIECE
        count = jnp.where(state == len(tiers), 0, count)
        to = jnp.cumsum(count, axis=0) * PIECE - count * PIECE
        at = jnp.where(there, spots + (to - begin)[:, :, None], -1)
        first = jnp.max(at, axis=0)
        second = jnp.sum(at + 1, axis=0) - first - 2
        w_first = jnp.sum(jnp.where(there & (at == first[None]), weights, 0.0), axis=0)
        w_second = jnp.sum(jnp.where(there & (at == second[None]), weights, 0.0), axis=0)
        home_info = [first.astype(F32), second.astype(F32), w_first, w_second]
        home_info = jnp.stack(home_info + [jnp.zeros_like(w_first)] * 4, axis=1).reshape(2, tiles, 8, TILE)
        home_plan = jnp.stack([begin, count, to], axis=1).reshape(24, 2 * tiles).T.reshape(2, tiles, 24)
        homes = 2 * chip + home_core

        onehot_in = (own_spot[:, None, :] == iota((1, cap, 1), 1)).astype(BF)

        def columns(w, axis, mine):
            parts = jnp.split(w, 2, axis=axis)
            return jnp.where((core == 0) == mine, parts[0], parts[1])

        w2_halves = [columns(w2, 1, m) for m in (True, False)]
        w2t = row_major(w2.T)
        w13t_halves = [[row_major(columns(w, 0, m).T) for w in (w1, w3)] for m in (True, False)]
        counts = jnp.sum((own_spot >= 0).astype(I32), axis=1)
        pad = jnp.zeros((group, toks), F32)
        own_info = jnp.stack([own_spot.astype(F32), own_gate] + [pad] * 6, axis=1)
        span = toks * 2 // 3
        s_first = jnp.min(jnp.where(own_spot >= 0, iota(own_spot.shape, 1), toks), axis=1)
        s_last = jnp.max(jnp.where(own_spot >= 0, iota(own_spot.shape, 1), 0), axis=1)
        froms = jnp.minimum(s_first // TILE * TILE, toks - span)
        froms = jnp.where(s_last < froms + span, froms, -1)
        plan = (state, list_cols, devs, segs, low_rows, home_info, home_plan, homes, onehot_in, counts, froms, own_info, w2_halves, w2t, w13t_halves)
        plan = lax.optimization_barrier(plan)
        all_x, plan = lax.optimization_barrier((all_x, plan))
        (state, list_cols, devs, segs, low_rows, home_info, home_plan, homes, onehot_in, counts, froms, own_info, w2_halves, w2t,
         w13t_halves) = plan

        def take(onehot, tok, gate=None):
            got = dot('gcs,gsd->gcd', onehot, tok)
            return (got if gate is None else gate.reshape(group, cap, 1) * got).astype(BF).reshape(rows, dim)

        def up_front(x):
            pre_a = dot('cd,df->cf', x, w1).astype(BF)
            pre_b = dot('cd,df->cf', x, w3).astype(BF)
            pre_a, pre_b = lax.optimization_barrier((pre_a, pre_b))
            a = pre_a.astype(F32)
            hid = (a * jax.nn.sigmoid(a) * pre_b.astype(F32)).astype(BF)
            return pre_a, pre_b, hid

        def inner_grads(pre_a, pre_b, dh):
            dh = dh.astype(BF).astype(F32)
            a = pre_a.astype(F32)
            sig = jax.nn.sigmoid(a)
            da = (dh * pre_b.astype(F32) * (sig * (1.0 + a * (1.0 - sig)))).astype(BF)
            db = (dh * (a * sig)).astype(BF)
            return da, db

        any_spec = pl.BlockSpec(memory_space=pl.ANY)

        def packed(tables, size, scaled):
            table_spec = pl.BlockSpec((1, cap, half), lambda g, dev, seg, low: (dev[g], 0, 0))
            res = pl.pallas_call(
                functools.partial(pack_kernel, scaled),
                grid_spec=pltpu.PrefetchScalarGridSpec(
                    num_scalar_prefetch=3, grid=(6,),
                    in_specs=[table_spec, table_spec, pl.BlockSpec((1, toks, 8), lambda g, dev, seg, low: (g, 0, 0))],
                    out_specs=[any_spec] * 4,
                    scratch_shapes=[pltpu.VMEM((2, TILE, half), BF), pltpu.SMEM((2,), I32),
                                    pltpu.SemaphoreType.DMA((2,))]),
                out_shape=[jax.ShapeDtypeStruct((size, half), BF)] * 4,
                compiler_params=pltpu.CompilerParams(vmem_limit_bytes=VMEM_LIMIT),
                cost_estimate=pl.CostEstimate(flops=2 * rows * cap * half, bytes_accessed=12 * rows * half, transcendentals=0),
                name='pack',
            )(devs, segs, low_rows, *tables, list_cols)
            return res[:2], res[2:]

        def arrived(which, tables, got_up, got_down, scaled):
            return pl.pallas_call(
                functools.partial(arrive_kernel, scaled),
                grid_spec=pltpu.PrefetchScalarGridSpec(
                    num_scalar_prefetch=2, grid=(tiles,),
                    in_specs=[pl.BlockSpec((1, 8, TILE), lambda t, homes, plan: (t, 0, 0))] + [any_spec] * 6,
                    out_specs=pl.BlockSpec((TILE, half), lambda t, homes, plan: (t, 0)),
                    scratch_shapes=[pltpu.VMEM((2, ROOM, half), BF), pltpu.SemaphoreType.DMA((2,))]),
                out_shape=jax.ShapeDtypeStruct((toks, half), BF),
                compiler_params=pltpu.CompilerParams(vmem_limit_bytes=VMEM_LIMIT),
                cost_estimate=pl.CostEstimate(flops=2 * rows * cap * half, bytes_accessed=6 * rows * half, transcendentals=0),
                name='arrive',
            )(homes[which], home_plan[which], home_info[which], *tables, *got_up, *got_down)

        def all_arrived(tables, got_up, got_down, scaled):
            theirs = arrived(0, tables, got_up, got_down, scaled)
            mine = arrived(1, after(tables, theirs), got_up, got_down, scaled)
            theirs = mate(theirs)
            return jnp.where(core == 0, jnp.concatenate([mine, theirs], axis=1), jnp.concatenate([theirs, mine], axis=1))

        def shift(up_rows, down_rows):
            got_up = lax.ppermute(up_rows, 'expert', to_next)
            got_down = lax.ppermute(down_rows, 'expert', to_prev)
            return got_up, got_down

        def second_rows(got, up_rows, down_rows):
            row = iota((up_rows.shape[0], 1), 0)
            return jnp.where(row < pass_up, got[0], up_rows), jnp.where(row < pass_down, got[1], down_rows)

        def table(v):
            return v.reshape(group, cap, half)

        x = take(onehot_in, all_x)
        pre_a, pre_b, hid = up_front(x)
        theirs = dot('cf,fd->cd', hid, w2_halves[1]).astype(BF)
        out_got = mate(theirs)
        ours = dot('cf,fd->cd', after(hid, theirs), w2_halves[0]).astype(BF)
        out_tables = (table(ours), table(out_got))
        out_up, out_down = packed(out_tables, stage, True)
        cut = [(out_up[0][:size], out_down[0][:size]) for size in tiers[:-1]] + [(out_up[0], out_down[0])]
        all_dy = after(all_dy, out_up, out_down, cut)

        def block_spec(rows, width):
            return pl.BlockSpec((1, rows, width), lambda e, *tables: (e, 0, 0))

        def fixed_spec(w):
            return pl.BlockSpec(w.shape, lambda e, *tables: (0, 0), pipeline_mode=pl.Buffered(1))

        def inner_grads_of(dy):
            f = pre_a.shape[1]
            return pl.pallas_call(
                inner_kernel,
                grid_spec=pltpu.PrefetchScalarGridSpec(
                    num_scalar_prefetch=2, grid=(group,),
                    in_specs=[block_spec(8, toks), block_spec(toks, dim), fixed_spec(w2t), block_spec(cap, f), block_spec(cap, f)],
                    out_specs=[block_spec(cap, dim), block_spec(cap, f), block_spec(cap, f)]),
                out_shape=[jax.ShapeDtypeStruct((group, cap, n), BF) for n in (dim, f, f)],
                compiler_params=pltpu.CompilerParams(vmem_limit_bytes=VMEM_LIMIT),
                cost_estimate=pl.CostEstimate(flops=2 * rows * dim * (toks + f), bytes_accessed=2 * rows * dim * 4, transcendentals=rows * f),
                name='inner',
            )(counts, froms, own_info, dy, w2t, pre_a.reshape(group, cap, f), pre_b.reshape(group, cap, f))

        def input_grad(da, db, k):
            w1t, w3t = w13t_halves[k]
            f = da.shape[2]
            return pl.pallas_call(
                input_kernel,
                grid_spec=pltpu.PrefetchScalarGridSpec(
                    num_scalar_prefetch=1, grid=(group,),
                    in_specs=[block_spec(cap, f), block_spec(cap, f), fixed_spec(w1t), fixed_spec(w3t)],
                    out_specs=block_spec(cap, half)),
                out_shape=jax.ShapeDtypeStruct((group, cap, half), BF),
                compiler_params=pltpu.CompilerParams(vmem_limit_bytes=VMEM_LIMIT),
                cost_estimate=pl.CostEstimate(flops=4 * rows * f * half, bytes_accessed=4 * rows * half, transcendentals=0),
                name='input_grad',
            )(counts, da, db, w1t, w3t)

        def rest(tier):
            size = tiers[tier]
            out_first = shift(*cut[tier])
            g, da, db = inner_grads_of(all_dy)
            out_second = second_rows(after(out_first, da), out_up[1][:size], out_down[1][:size])
            out_last = shift(*out_second)
            da, db = after((da, db), *out_second)
            theirs = input_grad(da, db, 1)
            dx_got = mate(theirs)
            ours = input_grad(after(da, theirs), db, 0)
            dx_tables = (ours, dx_got)
            dx_up, dx_down = packed(dx_tables, size, False)
            dx_first = shift(dx_up[0], dx_down[0])
            out_first, out_last, da, db, g = after((out_first, out_last, da, db, g), dx_up, dx_down)
            f = da.shape[2]
            da, db, g = da.reshape(rows, f), db.reshape(rows, f), g.reshape(rows, dim)
            dw1 = dot('cd,cf->df', x, da)
            out_first, out_last = after((out_first, out_last), dw1[:8, :TILE])
            y = all_arrived(out_tables, (out_first[0], out_last[0]), (out_first[1], out_last[1]), True)
            dx_second = second_rows(after(dx_first, y), dx_up[1], dx_down[1])
            dx_last = shift(*dx_second)
            db, hid_late = after((db, hid), *dx_second)
            dw3 = dot('cd,cf->df', x, db)
            dw2 = dot('cf,cd->fd', hid_late, g)
            gx = all_arrived(dx_tables, (dx_first[0], dx_last[0]), (dx_first[1], dx_last[1]), False)
            return y, gx, row_major(dw1)[None], row_major(dw3)[None], row_major(dw2)[None]

        def general():
            my_rank, my_taken = pick(rank, me), pick(taken.astype(I32), me) > 0
            my_idx = route_idx.T
            home_rank = pick(jnp.moveaxis(rank, 1, 0), me)
            out_rank = jnp.stack([jnp.sum(jnp.where(my_idx[j] == expert_id[:, 0], home_rank, 0), axis=0) for j in range(tops)])
            out_hot = my_idx % stride == 0

            def one_pass(first):
                ok = my_taken & (my_rank >= first) & (my_rank < first + cap)
                ok_out = (out_rank >= first) & (out_rank < first + cap)
                if first:
                    ok = ok & (me % stride == 0)
                    ok_out = ok_out & out_hot
                onehot = jnp.where(ok, my_rank - first, -1)[:, None, :] == iota((1, cap, 1), 1)
                gate = jnp.sum(jnp.where(onehot, own_gate[:, None, :], 0.0), axis=2)
                onehot = onehot.astype(BF)
                goal = jnp.where(ok_out, my_idx * cap + out_rank - first, -1)
                onehot_out = (goal[:, :, None] == iota((1, 1, rows), 2)).astype(BF)

                def swap(r):
                    return lax.all_to_all(r.reshape(group, cap, dim), 'expert', 0, 0).reshape(rows, dim)

                x = take(onehot, all_x)
                pre_a, pre_b, hid = up_front(x)
                back = swap(dot('cf,fd->cd', hid, w2).astype(BF))
                g = lax.optimization_barrier(take(onehot, all_dy, gate))
                da, db = lax.optimization_barrier(inner_grads(pre_a, pre_b, dot('cd,fd->cf', g, w2)))
                dx = (dot('cf,df->cd', da, w1) + dot('cf,df->cd', db, w3)).astype(BF)
                back_dx = swap(after(dx, back))
                slots = dot('jtr,rd->jtd', onehot_out, back)
                y = jnp.sum(route_gate.T[:, :, None] * slots, axis=0)
                gx = dot('tr,rd->td', jnp.sum(onehot_out, axis=0), back_dx)
                return y, gx, dot('cd,cf->df', x, da), dot('cd,cf->df', x, db), dot('cf,cd->fd', hid, g)

            first = one_pass(0)
            second = one_pass(cap)
            sums = [u + v for u, v in zip(first, second)]
            return sums[0].astype(BF), sums[1].astype(BF), *[v[None] for v in sums[2:]]

        branches = [functools.partial(rest, tier) for tier in range(len(tiers))]
        done = lax.switch(jnp.minimum(state, len(tiers) - 1), branches)
        return lax.cond(state == len(tiers), lambda done: general(), lambda done: done, done)

    return jax.shard_map(layer, mesh=mesh, in_specs=(tok_spec,) * 4 + (w_spec,) * 3, out_specs=(tok_spec,) * 5, check_vma=False)
```

```python
import functools

import jax
import jax.numpy as jnp
from jax import lax
from jax.experimental import pallas as pl
from jax.experimental.layout import Layout, with_layout_constraint
from jax.experimental.pallas import tpu as pltpu
from jax.sharding import PartitionSpec as P

BF = jnp.bfloat16
F32 = jnp.float32
I32 = jnp.int32
PIECE = 16
TILE = 128
SPAN = 256
ROOM = 512
VMEM_LIMIT = 50 * 2 ** 20


def dot(form, a, b):
    return jnp.einsum(form, a, b, preferred_element_type=F32)


def iota(shape, axis):
    return lax.broadcasted_iota(I32, shape, axis)


def count_before(mask):
    n = mask.shape[-1]
    earlier = iota((n, n), 0) < iota((n, n), 1)
    return dot('...u,us->...s', mask.astype(BF), earlier.astype(BF)).astype(I32)


def pick(table, index):
    sel = iota(table.shape, 0) == index
    return jnp.sum(jnp.where(sel, table, jnp.zeros_like(table)), axis=0)


def row_major(v):
    return with_layout_constraint(v, Layout(major_to_minor=tuple(range(v.ndim))))


def after(value, *others):
    return lax.optimization_barrier((value,) + others)[0]


def pack_kernel(scaled, dev_ref, seg_ref, low_ref, tab0, tab1, cols, *refs):
    outs, (buf, pend, sem) = (refs[0:2], refs[2:4]), refs[4:]
    g = pl.program_id(0)
    toks = cols.shape[1]
    length, start, extra, stage = [seg_ref[g, k] for k in range(4)]

    @pl.when(g == 0)
    def _():
        pend[0] = 0
        pend[1] = 0

    def drain(slot):
        def one(_, carry):
            pltpu.make_async_copy(buf.at[0, pl.ds(0, PIECE)], outs[0][0].at[pl.ds(0, PIECE)], sem.at[slot]).wait()
            return carry

        lax.fori_loop(0, pend[slot], one, 0)
        pend[slot] = 0

    def put(slot, p, side, at):
        for late, ref in enumerate(outs[side]):
            @pl.when((at >= stage) == bool(late))
            def _(ref=ref, late=late):
                spot = jnp.minimum(at - stage if late else at, ref.shape[0] - PIECE)
                src = buf.at[slot, pl.ds(pl.multiple_of(p * PIECE, PIECE), PIECE)]
                pltpu.make_async_copy(src, ref.at[pl.ds(pl.multiple_of(spot, PIECE), PIECE)], sem.at[slot]).start()
        pend[slot] = pend[slot] + 1

    def tile(i, carry):
        @pl.when(i * TILE < length)
        def _():
            slot = lax.rem(i, 2)
            drain(slot)
            vals = cols[0, pl.ds(pl.multiple_of(i * TILE, TILE), TILE)]
            lows = [low_ref[g, 2 * i + k] for k in range(2)]

            def part(k, tab):
                at = vals[:, k:k + 1] - lows[k].astype(F32)
                onehot = (at == iota((TILE, SPAN), 1).astype(F32)).astype(BF)
                got = jnp.dot(onehot, tab[0, pl.ds(pl.multiple_of(lows[k], PIECE), SPAN)], preferred_element_type=F32)
                return got * vals[:, 2 + k:3 + k] if scaled else got

            @pl.when((lows[0] >= 0) & (lows[1] < 0))
            def _():
                buf[slot] = part(0, tab0).astype(BF)

            @pl.when((lows[0] < 0) & (lows[1] >= 0))
            def _():
                buf[slot] = part(1, tab1).astype(BF)

            @pl.when((lows[0] >= 0) & (lows[1] >= 0))
            def _():
                buf[slot] = (part(0, tab0) + part(1, tab1)).astype(BF)

            def piece(p, carry):
                q = i * TILE + p * PIECE
                at = start + q
                near = jnp.where(at >= stage, at + extra, at)

                @pl.when((q < length) & (g < 2) & (at < extra))
                def _():
                    put(slot, p, 0, at)

                @pl.when((q < length) & (g < 2) & (at >= extra))
                def _():
                    put(slot, p, 1, at - extra)

                @pl.when((q < length) & (g >= 2) & (g < 4))
                def _():
                    put(slot, p, 0, near)

                @pl.when((q < length) & (g >= 4))
                def _():
                    put(slot, p, 1, near)

                return carry

            lax.fori_loop(0, TILE // PIECE, piece, 0)

        return carry

    lax.fori_loop(0, toks // TILE, tile, 0)

    @pl.when(g == pl.num_programs(0) - 1)
    def _():
        drain(0)
        drain(1)


def arrive_kernel(scaled, home_ref, plan_ref, info, tab0, tab1, up1, up2, down1, down2, out, wbuf, sem):
    t, last = pl.program_id(0), pl.num_programs(0) - 1
    sources = (tab0.at[home_ref[0]], tab1.at[home_ref[0]], up1, up2, up2, down1, down2, down2)

    def pieces(step, do):
        slot = lax.rem(step, 2)
        for w, ref in enumerate(sources):
            begin, count, to = [plan_ref[step, 3 * w + k] for k in range(3)]

            def one(p, carry, ref=ref, begin=begin, to=to):
                src = ref.at[pl.ds(pl.multiple_of(begin + p * PIECE, PIECE), PIECE)]
                do(pltpu.make_async_copy(src, wbuf.at[slot, pl.ds(pl.multiple_of(to + p * PIECE, PIECE), PIECE)], sem.at[slot]))
                return carry

            lax.fori_loop(0, count, one, 0)

    @pl.when(t == 0)
    def _():
        wbuf[...] = jnp.zeros_like(wbuf)
        pieces(0, lambda c: c.start())

    @pl.when(t < last)
    def _():
        pieces(t + 1, lambda c: c.start())

    vals = info[0]
    eye = iota((TILE, TILE), 0) == iota((TILE, TILE), 1)
    lane = iota((TILE, wbuf.shape[1]), 1).astype(F32)

    def column(k):
        return jnp.sum(jnp.where(eye, vals[k:k + 1, :], 0.0), axis=1, keepdims=True)

    first, second = column(0) == lane, column(1) == lane
    pieces(t, lambda c: c.wait())
    rows = wbuf.at[lax.rem(t, 2)]
    if scaled:
        total = column(2) * jnp.dot(first.astype(BF), rows[...], preferred_element_type=F32)
        total = total + column(3) * jnp.dot(second.astype(BF), rows[...], preferred_element_type=F32)
    else:
        total = jnp.dot((first | second).astype(BF), rows[...], preferred_element_type=F32)
    out[...] = total.astype(BF)


def by_count(count, cap, run):
    for n in range(0, cap + 1, TILE):
        @pl.when((count > n - TILE) & (count <= n))
        def _(n=n):
            run(n)


def inner_kernel(count_ref, from_ref, info, dy, w2t, a_ref, b_ref, g_ref, da_ref, db_ref):
    e = pl.program_id(0)
    cap, dim = g_ref.shape[1:]
    toks = dy.shape[1]
    step, narrow = dim // 4, da_ref.shape[2] // 4
    count, begin = count_ref[e], from_ref[e]

    def fill(n, begin, span):
        if n:
            vals = info[0, :, pl.ds(begin, span)]
            match = vals[0:1, :] == iota((n, span), 0).astype(F32)
            gate = jnp.sum(jnp.where(match, vals[1:2, :], 0.0), axis=1, keepdims=True)
            onehot = match.astype(BF)

            def outer(k, carry):
                at = pl.ds(pl.multiple_of(k * step, step), step)
                got = jnp.dot(onehot, dy[0, pl.ds(begin, span), at], preferred_element_type=F32)
                g_ref[0, :n, at] = (gate * got).astype(BF)
                return carry

            lax.fori_loop(0, dim // step, outer, 0)

            def hidden(k, carry):
                at = pl.ds(pl.multiple_of(k * narrow, narrow), narrow)
                dh = jnp.dot(g_ref[0, :n], w2t[:, at], preferred_element_type=F32).astype(BF).astype(F32)
                a, b = a_ref[0, :n, at].astype(F32), b_ref[0, :n, at].astype(F32)
                sig = jax.nn.sigmoid(a)
                da_ref[0, :n, at] = (dh * b * (sig * (1.0 + a * (1.0 - sig)))).astype(BF)
                db_ref[0, :n, at] = (dh * (a * sig)).astype(BF)
                return carry

            lax.fori_loop(0, da_ref.shape[2] // narrow, hidden, 0)
        if n < cap:
            for ref in (g_ref, da_ref, db_ref):
                ref[0, n:] = jnp.zeros((cap - n, ref.shape[2]), BF)

    @pl.when(begin >= 0)
    def _():
        by_count(count, cap, lambda n: fill(n, pl.multiple_of(begin, TILE), toks * 2 // 3))

    @pl.when(begin < 0)
    def _():
        fill(cap, 0, toks)


def input_kernel(count_ref, da, db, w1t, w3t, out):
    cap, width = out.shape[1:]
    step = width // 2

    def run(n):
        if n:
            for c in range(0, width, step):
                got = jnp.dot(da[0, :n], w1t[:, c:c + step], preferred_element_type=F32)
                got = got + jnp.dot(db[0, :n], w3t[:, c:c + step], preferred_element_type=F32)
                out[0, :n, c:c + step] = got.astype(BF)
        if n < cap:
            out[0, n:] = jnp.zeros((cap - n, width), BF)

    by_count(count_ref[pl.program_id(0)], cap, run)


def solution(mesh):
    group = mesh.shape['expert']
    chips = group // 2
    tok_spec = P(('data', 'expert'))
    w_spec = P('expert')
    to_mate = [(i, i ^ 1) for i in range(group)]
    to_next = [(i, (i + 2) % group) for i in range(group)]
    to_prev = [(i, (i - 2) % group) for i in range(group)]

    def layer(tok_x, route_idx, route_gate, grad_y, w_gate, w_up, w_down):
        toks, dim = tok_x.shape
        tops = route_idx.shape[1]
        experts = w_gate.shape[0] * group
        stride = experts // min(4, experts // 8)
        cap = max(4, 2 * toks * tops // experts)
        rows = group * cap
        half = dim // 2
        tiles = toks // TILE
        tiers = [toks * n // 48 for n in (49, 54, 60, 71)]
        stage = tiers[-1]
        place = 2 * stage
        me = lax.axis_index('expert')
        chip, core = me // 2, me % 2
        up, down, far = (chip + 1) % chips, (chip + chips - 1) % chips, (chip + 2) % chips
        w1, w3, w2 = w_gate[0], w_up[0], w_down[0]

        def mate(v):
            return lax.ppermute(v, 'expert', to_mate)

        all_x = lax.all_gather(tok_x, 'expert')
        all_dy = lax.all_gather(grad_y, 'expert')

        route = jnp.concatenate([route_idx.astype(F32).T, route_gate.T], axis=0)
        every = lax.all_gather(route, 'expert').swapaxes(0, 1)
        idx, gates = every[:tops].astype(I32), every[tops:]
        expert_id = iota((experts, 1, 1), 0)
        taken = jnp.any(idx[None] == expert_id[:, None], axis=1)
        rank = count_before(taken)
        hot_id = expert_id % stride == 0
        kept = taken & (hot_id | (rank < cap))
        spot = jnp.where(kept, rank, -1)
        need = jnp.any(kept.reshape(chips, 2, group, toks), axis=1)
        single = jnp.sum(need.astype(I32), axis=0) == 1
        listed = jnp.where(need, count_before(need), -1)
        sizes = (jnp.sum(need.astype(I32), axis=2) + PIECE - 1) // PIECE * PIECE
        total = jnp.sum(sizes.reshape(chips, chips, 2), axis=2)

        def turn(table, by):
            return jnp.roll(table, -by, axis=0)

        def hop(by):
            sel = (iota((chips, chips), 0) + by) % chips == iota((chips, chips), 1)
            return jnp.sum(jnp.where(sel, total, 0), axis=1)

        parts = 8
        tries = (parts + 1) ** chips
        share = (iota((chips, tries), 1) // ((parts + 1) ** iota((chips, tries), 0))) % (parts + 1)
        two_hops = hop(2)[:, None]
        go_up = two_hops * share // (parts * PIECE) * PIECE
        go_down = two_hops - go_up
        on_up = hop(1)[:, None] + go_up + turn(go_up, -1)
        on_down = hop(chips - 1)[:, None] + go_down + turn(go_down, 1)
        load = jnp.max(jnp.maximum(jnp.maximum(on_up, on_down), 2 * jnp.maximum(go_up, go_down)), axis=0)
        best = jnp.min(load)
        first_best = jnp.min(jnp.where(load == best, jnp.arange(tries, dtype=I32), tries))
        chosen = jnp.sum(jnp.where(iota((1, tries), 1) == first_best, go_up, 0), axis=1)
        other = hop(2) - chosen
        full = jnp.any(taken & hot_id & (rank >= cap))
        state = sum([(best > 2 * size).astype(I32) for size in tiers])
        state = lax.pmax(jnp.where(full, len(tiers), state), ('data', 'expert'))

        def gate_of(eid):
            return jnp.sum(jnp.where(idx == eid, gates, 0.0), axis=0)

        own_spot, mate_spot = pick(spot, me), pick(spot, me ^ 1)
        own_gate, mate_gate = gate_of(me), gate_of(me ^ 1)
        f_up, f_down = pick(chosen, chip), pick(other, chip)
        pass_up, pass_down = pick(chosen, down), pick(other, up)
        my_sizes = pick(sizes, chip)
        devs = jnp.stack([2 * to + k for to in (far, up, down) for k in range(2)])

        def lowest(at, ok):
            low = jnp.min(jnp.where(ok & (at >= 0), at, cap), axis=-1)
            return jnp.where(low < cap, jnp.minimum(low // PIECE * PIECE, cap - SPAN), -1)

        list_tile = (pick(listed, chip) // TILE)[None] == iota((tiles, 1, 1), 0)
        list_tile = list_tile & (pick(listed, chip) >= 0)[None]
        lows = jnp.stack([lowest(v[None], list_tile) for v in (own_spot, mate_spot)], axis=2)
        lows = lows.swapaxes(0, 1).reshape(group, 2 * tiles)
        low_rows = jnp.concatenate([lax.dynamic_slice_in_dim(lows, 2 * to, 2, 0) for to in (far, up, down)])

        def segments(size_of_stage):
            segs = []
            for to, lead, extra in ((far, 0, f_up), (up, f_up, pass_up), (down, f_down, pass_down)):
                for k in range(2):
                    size = pick(my_sizes, 2 * to + k)
                    segs.append(jnp.stack([size, jnp.asarray(lead, I32), extra, jnp.asarray(size_of_stage, I32)]))
                    lead = lead + size
            return jnp.stack(segs)

        def of_chips(v):
            return jnp.concatenate([lax.dynamic_slice_in_dim(v, 2 * to, 2, 0) for to in (far, up, down)])

        def thirds(v):
            high = v.astype(BF)
            middle = (v - high.astype(F32)).astype(BF)
            return [high, middle, (v - high.astype(F32) - middle.astype(F32)).astype(BF)]

        values = []
        for v in (own_spot, mate_spot):
            v = of_chips(v) + 1
            values += [(v // 256).astype(BF), (v % 256).astype(BF)]
        for v in (own_gate, mate_gate):
            values += thirds(of_chips(jnp.where(single, v, 1.0)))
        in_list = of_chips(pick(listed, chip))[:, None, :] == iota((1, toks, 1), 1)
        got = dot('gqs,gsk->gqk', in_list.astype(BF), jnp.stack(values, axis=2))
        list_cols = [got[:, :, 2 * k] * 256.0 + got[:, :, 2 * k + 1] - 1.0 for k in range(2)]
        list_cols += [got[:, :, 4 + 3 * k] + got[:, :, 5 + 3 * k] + got[:, :, 6 + 3 * k] for k in range(2)]
        list_cols = jnp.stack(list_cols + [jnp.zeros_like(list_cols[0])] * 4, axis=2)

        tier_stage = sum([jnp.where(state == k, size, 0) for k, size in enumerate(tiers)]) + jnp.where(state == len(tiers), stage, 0)
        segs = segments(tier_stage)

        def home(v):
            v = lax.dynamic_slice_in_dim(v, 2 * chip, 2, 0)
            return jnp.where(core == 0, v[::-1], v)

        home_core = jnp.where((core == 0) == (iota((2, 1), 0) == 0), 1, 0)
        home_idx = [home(idx[j]) for j in range(tops)]
        home_gates = [home(gates[j]) for j in range(tops)]
        home_kept = home(jnp.sum(kept.astype(I32) * (1 << expert_id), axis=0))
        home_single = home(single.astype(I32)) > 0

        def listed_at(c):
            at = home(pick(listed, c))
            first = pick(pick(sizes, c), 2 * chip)
            return at >= 0, at + jnp.where(home_core == 1, first, 0)

        def weight_of(c):
            w = 0.0
            for j in range(tops):
                held = (home_kept >> home_idx[j]) % 2 == 1
                w = w + jnp.where((home_idx[j] // 2 == c) & held, home_gates[j], 0.0)
            return jnp.where(home_single, 1.0, w)

        def near_spots(c, lead, passed):
            ok, at = listed_at(c)
            at = at + lead
            late = at >= tier_stage
            return [jnp.where(ok & jnp.logical_not(late), at, -1), jnp.where(ok & late, at + passed - tier_stage, -1)]

        far_ok, far_at = listed_at(far)
        far_cut = pick(chosen, far)
        spots = [home(own_spot), home(mate_spot)]
        spots += near_spots(down, pick(chosen, down), pick(chosen, far)) + [jnp.where(far_ok & (far_at < far_cut), far_at, -1)]
        spots += near_spots(up, pick(other, up), pick(other, far)) + [jnp.where(far_ok & (far_at >= far_cut), far_at - far_cut, -1)]
        w_down, w_up, w_far = [weight_of(c) for c in (down, up, far)]
        weights = [home(own_gate), home(mate_gate), w_down, w_down, w_far, w_up, w_up, w_far]
        spots = jnp.stack(spots).reshape(8, 2 * tiles, TILE)
        weights = jnp.stack(weights).reshape(8, 2 * tiles, TILE)
        there = spots >= 0
        begin = jnp.min(jnp.where(there, spots, place), axis=2) // PIECE * PIECE
        count = jnp.maximum(jnp.max(spots, axis=2) - begin + PIECE, 0) // PIECE
        to = jnp.cumsum(count, axis=0) * PIECE - count * PIECE
        at = jnp.where(there, spots + (to - begin)[:, :, None], -1)
        first = jnp.max(at, axis=0)
        second = jnp.sum(at + 1, axis=0) - first - 2
        w_first = jnp.sum(jnp.where(there & (at == first[None]), weights, 0.0), axis=0)
        w_second = jnp.sum(jnp.where(there & (at == second[None]), weights, 0.0), axis=0)
        home_info = [first.astype(F32), second.astype(F32), w_first, w_second]
        home_info = jnp.stack(home_info + [jnp.zeros_like(w_first)] * 4, axis=1).reshape(2, tiles, 8, TILE)
        home_plan = jnp.stack([begin, count, to], axis=1).reshape(24, 2 * tiles).T.reshape(2, tiles, 24)
        homes = 2 * chip + home_core

        onehot_in = (own_spot[:, None, :] == iota((1, cap, 1), 1)).astype(BF)

        def columns(w, axis, mine):
            parts = jnp.split(w, 2, axis=axis)
            return jnp.where((core == 0) == mine, parts[0], parts[1])

        w2_halves = [columns(w2, 1, m) for m in (True, False)]
        w2t = row_major(w2.T)
        w13t_halves = [[row_major(columns(w, 0, m).T) for w in (w1, w3)] for m in (True, False)]
        counts = jnp.sum((own_spot >= 0).astype(I32), axis=1)
        pad = jnp.zeros((group, toks), F32)
        own_info = jnp.stack([own_spot.astype(F32), own_gate] + [pad] * 6, axis=1)
        span = toks * 2 // 3
        s_first = jnp.min(jnp.where(own_spot >= 0, iota(own_spot.shape, 1), toks), axis=1)
        s_last = jnp.max(jnp.where(own_spot >= 0, iota(own_spot.shape, 1), 0), axis=1)
        froms = jnp.minimum(s_first // TILE * TILE, toks - span)
        froms = jnp.where(s_last < froms + span, froms, -1)
        plan = (state, list_cols, devs, segs, low_rows, home_info, home_plan, homes, onehot_in, counts, froms, own_info, w2_halves, w2t, w13t_halves)
        plan = lax.optimization_barrier(plan)
        all_x, plan = lax.optimization_barrier((all_x, plan))
        (state, list_cols, devs, segs, low_rows, home_info, home_plan, homes, onehot_in, counts, froms, own_info, w2_halves, w2t,
         w13t_halves) = plan

        def take(onehot, tok, gate=None):
            got = dot('gcs,gsd->gcd', onehot, tok)
            return (got if gate is None else gate.reshape(group, cap, 1) * got).astype(BF).reshape(rows, dim)

        def up_front(x):
            pre_a = dot('cd,df->cf', x, w1).astype(BF)
            pre_b = dot('cd,df->cf', x, w3).astype(BF)
            pre_a, pre_b = lax.optimization_barrier((pre_a, pre_b))
            a = pre_a.astype(F32)
            hid = (a * jax.nn.sigmoid(a) * pre_b.astype(F32)).astype(BF)
            return pre_a, pre_b, hid

        def inner_grads(pre_a, pre_b, dh):
            dh = dh.astype(BF).astype(F32)
            a = pre_a.astype(F32)
            sig = jax.nn.sigmoid(a)
            da = (dh * pre_b.astype(F32) * (sig * (1.0 + a * (1.0 - sig)))).astype(BF)
            db = (dh * (a * sig)).astype(BF)
            return da, db

        any_spec = pl.BlockSpec(memory_space=pl.ANY)

        def packed(tables, size, scaled):
            table_spec = pl.BlockSpec((1, cap, half), lambda g, dev, seg, low: (dev[g], 0, 0))
            res = pl.pallas_call(
                functools.partial(pack_kernel, scaled),
                grid_spec=pltpu.PrefetchScalarGridSpec(
                    num_scalar_prefetch=3, grid=(6,),
                    in_specs=[table_spec, table_spec, pl.BlockSpec((1, toks, 8), lambda g, dev, seg, low: (g, 0, 0))],
                    out_specs=[any_spec] * 4,
                    scratch_shapes=[pltpu.VMEM((2, TILE, half), BF), pltpu.SMEM((2,), I32),
                                    pltpu.SemaphoreType.DMA((2,))]),
                out_shape=[jax.ShapeDtypeStruct((size, half), BF)] * 4,
                compiler_params=pltpu.CompilerParams(vmem_limit_bytes=VMEM_LIMIT),
                cost_estimate=pl.CostEstimate(flops=2 * rows * cap * half, bytes_accessed=12 * rows * half, transcendentals=0),
                name='pack',
            )(devs, segs, low_rows, *tables, list_cols)
            return res[:2], res[2:]

        def arrived(which, tables, got_up, got_down, scaled):
            return pl.pallas_call(
                functools.partial(arrive_kernel, scaled),
                grid_spec=pltpu.PrefetchScalarGridSpec(
                    num_scalar_prefetch=2, grid=(tiles,),
                    in_specs=[pl.BlockSpec((1, 8, TILE), lambda t, homes, plan: (t, 0, 0))] + [any_spec] * 6,
                    out_specs=pl.BlockSpec((TILE, half), lambda t, homes, plan: (t, 0)),
                    scratch_shapes=[pltpu.VMEM((2, ROOM, half), BF), pltpu.SemaphoreType.DMA((2,))]),
                out_shape=jax.ShapeDtypeStruct((toks, half), BF),
                compiler_params=pltpu.CompilerParams(vmem_limit_bytes=VMEM_LIMIT),
                cost_estimate=pl.CostEstimate(flops=2 * rows * cap * half, bytes_accessed=6 * rows * half, transcendentals=0),
                name='arrive',
            )(homes[which], home_plan[which], home_info[which], *tables, *got_up, *got_down)

        def all_arrived(tables, got_up, got_down, scaled):
            theirs = arrived(0, tables, got_up, got_down, scaled)
            mine = arrived(1, after(tables, theirs), got_up, got_down, scaled)
            theirs = mate(theirs)
            return jnp.where(core == 0, jnp.concatenate([mine, theirs], axis=1), jnp.concatenate([theirs, mine], axis=1))

        def shift(up_rows, down_rows):
            got_up = lax.ppermute(up_rows, 'expert', to_next)
            got_down = lax.ppermute(down_rows, 'expert', to_prev)
            return got_up, got_down

        def second_rows(got, up_rows, down_rows):
            row = iota((up_rows.shape[0], 1), 0)
            return jnp.where(row < pass_up, got[0], up_rows), jnp.where(row < pass_down, got[1], down_rows)

        def table(v):
            return v.reshape(group, cap, half)

        x = take(onehot_in, all_x)
        pre_a, pre_b, hid = up_front(x)
        theirs = dot('cf,fd->cd', hid, w2_halves[1]).astype(BF)
        out_got = mate(theirs)
        ours = dot('cf,fd->cd', after(hid, theirs), w2_halves[0]).astype(BF)
        out_tables = (table(ours), table(out_got))
        out_up, out_down = packed(out_tables, stage, True)
        cut = [(out_up[0][:size], out_down[0][:size]) for size in tiers[:-1]] + [(out_up[0], out_down[0])]
        all_dy = after(all_dy, out_up, out_down, cut)

        def block_spec(rows, width):
            return pl.BlockSpec((1, rows, width), lambda e, *tables: (e, 0, 0))

        def fixed_spec(w):
            return pl.BlockSpec(w.shape, lambda e, *tables: (0, 0), pipeline_mode=pl.Buffered(1))

        def inner_grads_of(dy):
            f = pre_a.shape[1]
            return pl.pallas_call(
                inner_kernel,
                grid_spec=pltpu.PrefetchScalarGridSpec(
                    num_scalar_prefetch=2, grid=(group,),
                    in_specs=[block_spec(8, toks), block_spec(toks, dim), fixed_spec(w2t), block_spec(cap, f), block_spec(cap, f)],
                    out_specs=[block_spec(cap, dim), block_spec(cap, f), block_spec(cap, f)]),
                out_shape=[jax.ShapeDtypeStruct((group, cap, n), BF) for n in (dim, f, f)],
                compiler_params=pltpu.CompilerParams(vmem_limit_bytes=VMEM_LIMIT),
                cost_estimate=pl.CostEstimate(flops=2 * rows * dim * (toks + f), bytes_accessed=2 * rows * dim * 4, transcendentals=rows * f),
                name='inner',
            )(counts, froms, own_info, dy, w2t, pre_a.reshape(group, cap, f), pre_b.reshape(group, cap, f))

        def input_grad(da, db, k):
            w1t, w3t = w13t_halves[k]
            f = da.shape[2]
            return pl.pallas_call(
                input_kernel,
                grid_spec=pltpu.PrefetchScalarGridSpec(
                    num_scalar_prefetch=1, grid=(group,),
                    in_specs=[block_spec(cap, f), block_spec(cap, f), fixed_spec(w1t), fixed_spec(w3t)],
                    out_specs=block_spec(cap, half)),
                out_shape=jax.ShapeDtypeStruct((group, cap, half), BF),
                compiler_params=pltpu.CompilerParams(vmem_limit_bytes=VMEM_LIMIT),
                cost_estimate=pl.CostEstimate(flops=4 * rows * f * half, bytes_accessed=4 * rows * half, transcendentals=0),
                name='input_grad',
            )(counts, da, db, w1t, w3t)

        def rest(tier):
            size = tiers[tier]
            out_first = shift(*cut[tier])
            g, da, db = inner_grads_of(all_dy)
            out_second = second_rows(after(out_first, da), out_up[1][:size], out_down[1][:size])
            out_last = shift(*out_second)
            da, db = after((da, db), *out_second)
            theirs = input_grad(da, db, 1)
            dx_got = mate(theirs)
            ours = input_grad(after(da, theirs), db, 0)
            dx_tables = (ours, dx_got)
            dx_up, dx_down = packed(dx_tables, size, False)
            dx_first = shift(dx_up[0], dx_down[0])
            out_first, out_last, da, db, g = after((out_first, out_last, da, db, g), dx_up, dx_down)
            f = da.shape[2]
            da, db, g = da.reshape(rows, f), db.reshape(rows, f), g.reshape(rows, dim)
            dw1 = dot('cd,cf->df', x, da)
            out_first, out_last = after((out_first, out_last), dw1[:8, :TILE])
            y = all_arrived(out_tables, (out_first[0], out_last[0]), (out_first[1], out_last[1]), True)
            dx_second = second_rows(after(dx_first, y), dx_up[1], dx_down[1])
            dx_last = shift(*dx_second)
            db, hid_late = after((db, hid), *dx_second)
            dw3 = dot('cd,cf->df', x, db)
            dw2 = dot('cf,cd->fd', hid_late, g)
            gx = all_arrived(dx_tables, (dx_first[0], dx_last[0]), (dx_first[1], dx_last[1]), False)
            return y, gx, row_major(dw1)[None], row_major(dw3)[None], row_major(dw2)[None]

        def general():
            my_rank, my_taken = pick(rank, me), pick(taken.astype(I32), me) > 0
            my_idx = route_idx.T
            home_rank = pick(jnp.moveaxis(rank, 1, 0), me)
            out_rank = jnp.stack([jnp.sum(jnp.where(my_idx[j] == expert_id[:, 0], home_rank, 0), axis=0) for j in range(tops)])
            out_hot = my_idx % stride == 0

            def one_pass(first):
                ok = my_taken & (my_rank >= first) & (my_rank < first + cap)
                ok_out = (out_rank >= first) & (out_rank < first + cap)
                if first:
                    ok = ok & (me % stride == 0)
                    ok_out = ok_out & out_hot
                onehot = jnp.where(ok, my_rank - first, -1)[:, None, :] == iota((1, cap, 1), 1)
                gate = jnp.sum(jnp.where(onehot, own_gate[:, None, :], 0.0), axis=2)
                onehot = onehot.astype(BF)
                goal = jnp.where(ok_out, my_idx * cap + out_rank - first, -1)
                onehot_out = (goal[:, :, None] == iota((1, 1, rows), 2)).astype(BF)

                def swap(r):
                    blocks = r.reshape(group, cap, dim)
                    got = blocks
                    for by in range(1, group):
                        block = lax.dynamic_index_in_dim(blocks, (me + by) % group, 0)
                        block = lax.ppermute(block, 'expert', [(i, (i + by) % group) for i in range(group)])
                        got = lax.dynamic_update_slice_in_dim(got, block, (me + group - by) % group, 0)
                    return got.reshape(rows, dim)

                x = take(onehot, all_x)
                pre_a, pre_b, hid = up_front(x)
                back = swap(dot('cf,fd->cd', hid, w2).astype(BF))
                g = lax.optimization_barrier(take(onehot, all_dy, gate))
                da, db = lax.optimization_barrier(inner_grads(pre_a, pre_b, dot('cd,fd->cf', g, w2)))
                dx = (dot('cf,df->cd', da, w1) + dot('cf,df->cd', db, w3)).astype(BF)
                back_dx = swap(after(dx, back))
                slots = dot('jtr,rd->jtd', onehot_out, back)
                y = jnp.sum(route_gate.T[:, :, None] * slots, axis=0)
                gx = dot('tr,rd->td', jnp.sum(onehot_out, axis=0), back_dx)
                return y, gx, dot('cd,cf->df', x, da), dot('cd,cf->df', x, db), dot('cf,cd->fd', hid, g)

            first = one_pass(0)
            second = one_pass(cap)
            sums = [u + v for u, v in zip(first, second)]
            return sums[0].astype(BF), sums[1].astype(BF), *[v[None] for v in sums[2:]]

        branches = [functools.partial(rest, tier) for tier in range(len(tiers))] + [general]
        return lax.switch(state, branches)

    return jax.shard_map(layer, mesh=mesh, in_specs=(tok_spec,) * 4 + (w_spec,) * 3, out_specs=(tok_spec,) * 5, check_vma=False)
```
